32 devices in a mesh: batch: 8 (over z, x), mp: 4 (over y, core).
Axes of the slice: x: 2, y: 2, z: 4, core: 2. Of those that a mesh axis runs over, the one named last changes fastest.
Arguments:
- features: bfloat16 [1024, 65536], P('batch', 'mp'), may hold values from 0 to 4
- tiles: bfloat16 [2, 512, 3, 128, 128], P(None, 'mp', None, 'batch'), may hold values from -0.3125 to 0.3125
- biases: float32 [2, 65536], P(None, 'mp'), may hold values from -0.5 to 0
- in_block: int32 [2, 512, 3], replicated, may hold values from 0 to 511, as said below
Outputs:
- activations: bfloat16 [1024, 65536], P('batch', 'mp')
- row_means: float32 [1024], P('batch')
- grand: float32 [], replicated
The draws below stay inside these ranges and needn't reach their ends.
Inputs may be any that keep to these rules, and one draw needn't show every extreme that they name: `in_block`: number the 384 tiles of mp shard m (column blocks m * 128 to (m + 1) * 128 - 1) in order of column block, then tile slot; tile number s reads a block of shard s // 96, that is an id in [(s // 96) * 128, (s // 96 + 1) * 128).
All inputs are finite; a program needn't handle non-finite values.
Results may differ from the reference program's by a relative error of at most 0.0052.
Values may be sent and summed in bfloat16 or wider, within the bound.
A program may use at most 128 MiB of HBM per device.

```python
import math
import jax
import jax.numpy as jnp
from jax import lax

NEUR = 65536
BLOCK = 128
FAN_TILES = 3
LAYERS = 2
ROWS_DEV = 128
NB = 512
CB_DEV = 128
PER_PEER = 96
ROWS = 1024


def draw_in_block(key, part):
    shard_count = NB // CB_DEV
    slots = CB_DEV * FAN_TILES
    local = jax.random.randint(key, (LAYERS, shard_count, slots), 0, CB_DEV, dtype=jnp.int32)
    source = jnp.arange(slots, dtype=jnp.int32) // PER_PEER * CB_DEV
    ids = local + source[None, None, :]
    return ids.reshape(LAYERS, NB, FAN_TILES).astype(jnp.int32)


def draw_features(key, part):
    key_scale, key_base = jax.random.split(jax.random.fold_in(key, 17))
    groups = ROWS // ROWS_DEV
    logs = jax.random.uniform(key_scale, (groups, 1, 1), jnp.float32, math.log(0.25), math.log(2.0))
    scale = jnp.exp(logs)
    base = jax.random.uniform(key_base, (groups, ROWS_DEV, NEUR), jnp.float32, 0.0, 1.0)
    base = 2.0 * base
    values = jnp.clip(scale * base, 0.0, 4.0)
    return values.reshape(ROWS, NEUR).astype(jnp.bfloat16)


def levels(rng, extent, pieces, smallest, largest):
    def one(dim, blocks):
        steps = jax.random.uniform(jax.random.fold_in(jax.random.fold_in(rng, 6), dim), (blocks,), jnp.float32, smallest / len(pieces), largest / len(pieces))
        return jnp.repeat(jnp.exp(steps), extent[dim] // blocks).reshape((-1,) + (1,) * (len(extent) - dim - 1))

    level = one(*pieces[0])
    for cut in pieces[1:]:
        level = level * one(*cut)
    return level


def gaussian(stream_key, dims, spread, most, shards=(), kind=jnp.bfloat16):
    array = jax.random.normal(stream_key, dims, jnp.float32) * spread
    if len(shards) > 0:
        array = levels(stream_key, dims, shards, -0.22, 0.18) * array
    return jnp.clip(array, min=-most, max=most).astype(kind)


def setup_inputs(seed: int = 0) -> dict:
    seeds = jax.random.split(jax.random.key(seed), 5)
    return {
        "features": draw_features(jax.random.fold_in(seeds[4], 71), 0),
        "tiles": gaussian(seeds[1], (LAYERS, NB, FAN_TILES, BLOCK, BLOCK), (FAN_TILES * BLOCK) ** -0.5, 0.3125, ((1, 4), (3, 8))),
        "biases": jnp.clip(-0.5 + 0.5 * jax.random.uniform(seeds[2], (LAYERS, NEUR), jnp.float32) ** levels(seeds[2], (LAYERS, NEUR), ((1, 4),), -0.2, 0.2), -0.5, 0.0),
        "in_block": draw_in_block(jax.random.fold_in(seeds[4], 71), 0),
    }


def one_layer(current, tile_layer, bias_layer, ids_layer):
    group = math.gcd(NB, 32)
    blocks_all = current.reshape(ROWS, NB, BLOCK)
    ids_grouped = ids_layer.reshape(NB // group, group, FAN_TILES)
    tiles_grouped = tile_layer.reshape(NB // group, group, FAN_TILES, BLOCK, BLOCK)
    bias_grouped = bias_layer.reshape(NB // group, group, BLOCK)

    def per_group(packed):
        ids_here, tiles_here, bias_here = packed
        taken = jnp.take(blocks_all, ids_here.reshape(-1), axis=1)
        taken = taken.reshape(ROWS, group, FAN_TILES, BLOCK).astype(jnp.float32)
        total = jnp.einsum("rjki,jkio->rjo", taken, tiles_here.astype(jnp.float32))
        shifted = total + bias_here[None, :, :]
        return jnp.clip(shifted, 0.0, 32.0).astype(jnp.bfloat16)

    result = lax.map(per_group, (ids_grouped, tiles_grouped, bias_grouped))
    return jnp.transpose(result, (1, 0, 2, 3)).reshape(ROWS, NEUR)


def reference(features, tiles, biases, in_block):
    current = features
    for layer_no in range(LAYERS):
        current = one_layer(current, tiles[layer_no], biases[layer_no], in_block[layer_no])
    row_means = jnp.sum(current.astype(jnp.float32), axis=1) / NEUR
    grand = jnp.sum(row_means) / ROWS
    return current, row_means, grand
```

```python
import functools
import math

import jax
import jax.numpy as jnp
from jax import lax
from jax.experimental import pallas as pl
from jax.experimental.pallas import tpu as pltpu
from jax.sharding import PartitionSpec as P

MESH = pl.DeviceIdType.MESH
PIECES = 4


def geometry(mesh):
    groups, shards = mesh.devices.shape
    where = [getattr(d, "coords", None) for d in mesh.devices[:, 0]]
    if groups == 1 or where[0] is None or where[0] == where[1]:
        return groups, 1, True, 1
    moved = [i for i in range(len(where[0])) if where[0][i] != where[1][i]][0]
    minor = 1
    while minor < groups and all(
        where[minor][i] == where[0][i] for i in range(len(where[0])) if i != moved
    ):
        minor += 1
    major = groups // minor
    row = [d.coords for d in mesh.devices[0, :]]
    cores = sum(1 for c in row if c == row[0])
    if major >= minor:
        return major, minor, True, cores
    return minor, major, False, cores


def gather_kernel(
    geo, shards, layer, pieces,
    tiles, cur, wout, xout,
    wv, xv, lsem, wrecv, wup, wdn, wcross, whalf, xrecv, xfar, xcore,
):
    nl, nq, line_major, nc = geo
    ny = shards // nc
    bi = lax.axis_index("batch")
    mi = lax.axis_index("mp")
    if line_major:
        l, q = bi // nq, bi % nq
    else:
        l, q = bi % nl, bi // nl
    y, core = mi // nc, mi % nc
    step_w = tiles.shape[1] // pieces
    step_x = cur.shape[0] // pieces
    halves = nq == 2 and nl % 2 == 0
    first = pieces // 2

    def group(level, side):
        return level * nq + side if line_major else side * nl + level

    sides = [(q + d) % nq for d in range(1, nq)]
    fars = [((y + d) % ny) * nc + core for d in range(1, ny)]
    partners = [y * nc + (core + d) % nc for d in range(1, nc)]

    barrier = pltpu.get_barrier_semaphore()

    def greet(b, m):
        pl.semaphore_signal(barrier, inc=1, device_id=(b, m), device_id_type=MESH)

    @pl.when(l > 0)
    def _():
        greet(group(l - 1, q), mi)

    @pl.when(l < nl - 1)
    def _():
        greet(group(l + 1, q), mi)

    for side in sides:
        greet(group(l, side), mi)
    for m in fars + partners:
        greet(bi, m)
    near = jnp.where(l > 0, 1, 0) + jnp.where(l < nl - 1, 1, 0)
    pl.semaphore_wait(barrier, len(sides) + len(fars) + len(partners) + near)

    in_w = pltpu.make_async_copy(tiles.at[layer], wv, lsem.at[0])
    in_x = pltpu.make_async_copy(cur, xv, lsem.at[1])
    in_w.start()
    in_x.start()

    def wcopy(own, b, c, to, ssem):
        part = pl.ds(c * step_w, step_w)
        return pltpu.make_async_remote_copy(
            src_ref=tiles.at[layer, part] if own else wout.at[b, part],
            dst_ref=wout.at[b, part],
            send_sem=ssem,
            recv_sem=wrecv.at[b, c],
            device_id=(to, mi),
            device_id_type=MESH,
        )

    def xcopy(own, m, c, to, ssem):
        part = pl.ds(c * step_x, step_x)
        return pltpu.make_async_remote_copy(
            src_ref=cur.at[part] if own else xout.at[m, part],
            dst_ref=xout.at[m, part],
            send_sem=ssem,
            recv_sem=xrecv.at[m, c],
            device_id=(bi, to),
            device_id_type=MESH,
        )

    def phase(p, c, drain):
        def go(copy):
            copy.wait_send() if drain else copy.start()

        def arrived_w(b):
            if not drain:
                wcopy(False, b, c, bi, wup.at[0, c]).wait_recv()

        if p == 0:
            @pl.when(l < nl - 1)
            def _():
                go(wcopy(True, bi, c, group(l + 1, q), wup.at[0, c]))

            @pl.when(l > 0)
            def _():
                go(wcopy(True, bi, c, group(l - 1, q), wdn.at[0, c]))

            for i, side in enumerate(sides):
                go(wcopy(True, bi, c, group(l, side), wcross.at[i, l, c]))
            for i, m in enumerate(fars):
                go(xcopy(True, mi, c, m, xfar.at[i, c]))
            for i, m in enumerate(partners):
                go(xcopy(True, mi, c, m, xcore.at[i, y, c]))
        else:
            @pl.when(l - p >= 0)
            def _():
                b = group(l - p, q)
                arrived_w(b)

                @pl.when(l < nl - 1)
                def _():
                    go(wcopy(False, b, c, group(l + 1, q), wup.at[p, c]))

                def across():
                    for i, side in enumerate(sides):
                        go(wcopy(False, b, c, group(l, side), wcross.at[i, l - p, c]))

                if halves and p == 1:
                    pl.when((l < nl // 2) | (c < first))(across)
                else:
                    across()

            @pl.when(l + p <= nl - 1)
            def _():
                b = group(l + p, q)
                arrived_w(b)

                @pl.when(l > 0)
                def _():
                    go(wcopy(False, b, c, group(l - 1, q), wdn.at[p, c]))

                def across():
                    for i, side in enumerate(sides):
                        go(wcopy(False, b, c, group(l, side), wcross.at[i, l + p, c]))

                if halves and p == 1:
                    pl.when((l >= nl // 2) | (c < first))(across)
                else:
                    across()

            if halves and p == 1:
                @pl.when(c >= first)
                def _():
                    b = group(l, sides[0])
                    arrived_w(b)

                    @pl.when((l + 1 >= nl // 2) & (l < nl - 1))
                    def _():
                        go(wcopy(False, b, c, group(l + 1, q), whalf.at[0, c]))

                    @pl.when((l - 1 < nl // 2) & (l > 0))
                    def _():
                        go(wcopy(False, b, c, group(l - 1, q), whalf.at[1, c]))

        if p == nl - 1:
            for d, far in enumerate(fars):
                if not drain:
                    xcopy(False, far, c, mi, xfar.at[0, c]).wait_recv()
                for i, m in enumerate(partners):
                    go(xcopy(False, far, c, m, xcore.at[i, far // nc, c]))

    for p in range(nl):
        @pl.loop(0, pieces)
        def _(c, p=p):
            phase(p, c, False)

        if p == 0:
            in_w.wait()
            in_x.wait()
            out_w = pltpu.make_async_copy(wv, wout.at[bi], lsem.at[2])
            out_x = pltpu.make_async_copy(xv, xout.at[mi], lsem.at[3])
            out_w.start()
            out_x.start()

    @pl.loop(0, pieces)
    def _(c):
        for side in sides:
            for level in range(nl):
                b = group(level, side)

                def arrive(b=b):
                    wcopy(False, b, c, bi, wup.at[0, c]).wait_recv()

                if halves:
                    pl.when((l != level) | (c < first))(arrive)
                else:
                    arrive()
        for m in partners:
            for yy in range(ny):
                xcopy(False, yy * nc + m % nc, c, mi, xfar.at[0, c]).wait_recv()

    out_w.wait()
    out_x.wait()
    for p in range(nl):
        @pl.loop(0, pieces)
        def _(c, p=p):
            phase(p, c, True)


def gather(geo, shards, groups, layer, tiles, cur):
    nl, nq, _, nc = geo
    pieces = 8 if groups <= 8 else 2
    ny = shards // nc
    dma = pltpu.SemaphoreType.DMA
    return pl.pallas_call(
        functools.partial(gather_kernel, geo, shards, layer, pieces),
        out_shape=(
            jax.ShapeDtypeStruct((groups,) + tiles.shape[1:], tiles.dtype),
            jax.ShapeDtypeStruct((shards,) + cur.shape, cur.dtype),
        ),
        in_specs=[pl.BlockSpec(memory_space=pl.ANY)] * 2,
        out_specs=(pl.BlockSpec(memory_space=pl.ANY),) * 2,
        scratch_shapes=[
            pltpu.VMEM(tiles.shape[1:], tiles.dtype),
            pltpu.VMEM(cur.shape, cur.dtype),
            dma((4,)),
            dma((groups, pieces)),
            dma((nl, pieces)),
            dma((nl, pieces)),
            dma((max(nq - 1, 1), nl, pieces)),
            dma((2, pieces)),
            dma((shards, pieces)),
            dma((max(ny - 1, 1), pieces)),
            dma((max(nc - 1, 1), ny, pieces)),
        ],
        compiler_params=pltpu.CompilerParams(collective_id=layer, has_side_effects=True),
        name=f"gather_{layer}",
    )(tiles, cur)


def layer_kernel(ids, x_ref, w_ref, b_ref, o_ref, r_ref, xl, wl, s_ref, loads):
    shards, rows, _ = x_ref.shape
    _, cb, fan, _, side = w_ref.shape
    per_shard = cb // shards
    width = math.gcd(per_shard, 8)

    def pulls(s):
        part = pl.ds(s * per_shard, per_shard)
        return (
            pltpu.make_async_copy(x_ref.at[s], xl.at[s], loads.at[0, s]),
            pltpu.make_async_copy(w_ref.at[:, part], wl.at[:, part], loads.at[1, s]),
        )

    for s in range(min(2, shards)):
        for pull in pulls(s):
            pull.start()
    s_ref[...] = jnp.zeros_like(s_ref)
    for s in range(shards):
        for pull in pulls(s):
            pull.wait()
        if s + 2 < shards:
            for pull in pulls(s + 2):
                pull.start()

        @pl.loop(0, per_shard // width)
        def _(k, s=s):
            for jj in range(width):
                j = s * per_shard + k * width + jj
                xs, ws = [], []
                for t in range(fan):
                    at = ids[j * fan + t]
                    xs.append(xl[s, :, pl.ds(pl.multiple_of(at * side, side), side)])
                    ws.append(wl[:, j, t].reshape(side, side))
                total = jnp.dot(
                    jnp.concatenate(xs, axis=1),
                    jnp.concatenate(ws, axis=0),
                    preferred_element_type=jnp.float32,
                )
                cols = pl.ds(pl.multiple_of(j * side, side), side)
                out = jnp.clip(total + b_ref[:, cols], 0.0, 32.0).astype(o_ref.dtype)
                o_ref[:, cols] = out
                s_ref[...] += out.astype(jnp.float32)

    line = jnp.sum(s_ref[...].T, axis=0, keepdims=True)
    r_ref[...] = jnp.broadcast_to(line, r_ref.shape)


def apply_layer(ids, xall, wall, bias):
    shards, rows, width = xall.shape
    side = wall.shape[4]
    hbm = pl.BlockSpec(memory_space=pl.ANY)
    vmem = pl.BlockSpec(memory_space=pltpu.VMEM)
    return pl.pallas_call(
        layer_kernel,
        out_shape=(
            jax.ShapeDtypeStruct((rows, width), xall.dtype),
            jax.ShapeDtypeStruct((8, rows), jnp.float32),
        ),
        in_specs=[pl.BlockSpec(memory_space=pltpu.SMEM), hbm, hbm, vmem],
        out_specs=(vmem, vmem),
        scratch_shapes=[
            pltpu.VMEM(xall.shape, xall.dtype),
            pltpu.VMEM(wall.shape, wall.dtype),
            pltpu.VMEM((rows, side), jnp.float32),
            pltpu.SemaphoreType.DMA((2, shards)),
        ],
        compiler_params=pltpu.CompilerParams(vmem_limit_bytes=52 * 1024 * 1024),
        name="layer",
    )(ids, xall, wall, bias)


def means_kernel(groups, shards, neurons, x_ref, rows_ref, all_ref, slots, ssem, rsem):
    bi = lax.axis_index("batch")
    mi = lax.axis_index("mp")
    me = bi * shards + mi
    total = groups * shards
    barrier = pltpu.get_barrier_semaphore()

    def peer(d):
        to = (me + d) % total
        return to // shards, to % shards

    @pl.loop(1, total)
    def _(d):
        pl.semaphore_signal(barrier, inc=1, device_id=peer(d), device_id_type=MESH)

    pl.semaphore_wait(barrier, total - 1)

    def copy(d, slot):
        return pltpu.make_async_remote_copy(
            src_ref=x_ref,
            dst_ref=slots.at[slot],
            send_sem=ssem.at[d],
            recv_sem=rsem.at[slot],
            device_id=peer(d),
            device_id_type=MESH,
        )

    @pl.loop(1, total)
    def _(d):
        copy(d, me).start()

    slots[me] = x_ref[...]

    @pl.loop(1, total)
    def _(d):
        copy(d, (me + d) % total).wait_recv()

    whole = jnp.zeros(all_ref.shape, jnp.float32)
    for b in range(groups):
        one = slots[b * shards]
        for m in range(1, shards):
            one = one + slots[b * shards + m]
        whole = whole + one / neurons
    all_ref[...] = whole
    mine = slots[bi * shards]
    for m in range(1, shards):
        mine = mine + slots[bi * shards + m]
    rows_ref[...] = mine / neurons

    @pl.loop(1, total)
    def _(d):
        copy(d, me).wait_send()


def means(groups, shards, neurons, sums):
    total = groups * shards
    if total > 64:
        shard_sum = lax.psum(sums[0], "mp") / neurons
        return shard_sum, lax.psum(shard_sum, "batch")
    vmem = pl.BlockSpec(memory_space=pltpu.VMEM)
    like = jax.ShapeDtypeStruct(sums.shape, jnp.float32)
    mine, whole = pl.pallas_call(
        functools.partial(means_kernel, groups, shards, neurons),
        out_shape=(like, like),
        in_specs=[vmem],
        out_specs=(vmem, vmem),
        scratch_shapes=[
            pltpu.VMEM((total,) + sums.shape, jnp.float32),
            pltpu.SemaphoreType.DMA((total,)),
            pltpu.SemaphoreType.DMA((total,)),
        ],
        compiler_params=pltpu.CompilerParams(collective_id=20, has_side_effects=True),
        name="means",
    )(sums)
    return mine[0], whole[0]


def fused_kernel(
    geo, pieces, neurons, total_rows,
    ids, feats, tiles, biases, out, rows_ref, grand_ref,
    wl, bl, xin, x2, st, fin, sums, line, slots,
    lsem, qsend, qrecv, bsend, brecv, up, dn, xs, wrecv,
    osend, orecv, msend, mrecv,
):
    nl, nq, line_major, nc = geo
    layers, groups, shards, per, fan, _, side = wl.shape
    ny = shards // nc
    cb = per * shards
    n = per // pieces
    chunks = shards * pieces
    every = layers * chunks
    depth = nl
    bi = lax.axis_index("batch")
    mi = lax.axis_index("mp")
    if line_major:
        l, q = bi // nq, bi % nq
    else:
        l, q = bi % nl, bi // nl
    y, core = mi // nc, mi % nc
    side_q = (q + 1) % nq
    total = groups * shards
    me = bi * shards + mi

    def group(level, column):
        return level * nq + column if line_major else column * nl + level

    def source(k):
        return ((y + k // nc) % ny) * nc + (core + k % nc) % nc

    def spot(p):
        c = p % chunks
        return p // chunks, c // pieces, c % pieces

    def peer(d):
        to = (me + d) % total
        return to // shards, to % shards

    @pl.loop(0, cb)
    def _(j):
        pltpu.make_async_copy(
            feats.at[:, pl.ds(j * side, side)], xin.at[j], lsem.at[0]
        ).start()

    def own_quarter(layer):
        return pltpu.make_async_copy(
            tiles.at[layer, pl.ds(mi * per, per)], wl.at[layer, bi, mi], lsem.at[2 + layer]
        )

    for layer in range(layers):
        own_quarter(layer).start()
    mine_b = pl.ds(mi * per * side, per * side)
    in_b = pltpu.make_async_copy(biases.at[:, mine_b], bl.at[:, mine_b], lsem.at[1])
    in_b.start()

    barrier = pltpu.get_barrier_semaphore()

    @pl.loop(1, total)
    def _(d):
        pl.semaphore_signal(barrier, inc=1, device_id=peer(d), device_id_type=MESH)

    pl.semaphore_wait(barrier, total - 1)

    def quarter(layer, k):
        to = source(k)
        return pltpu.make_async_remote_copy(
            src_ref=tiles.at[layer, pl.ds(to * per, per)],
            dst_ref=wl.at[layer, bi, mi],
            send_sem=qsend.at[layer, k],
            recv_sem=qrecv.at[layer, mi],
            device_id=(bi, to),
            device_id_type=MESH,
        )

    def quarter_in(layer, k):
        m = source(k)
        return pltpu.make_async_remote_copy(
            src_ref=wl.at[layer, bi, m],
            dst_ref=wl.at[layer, bi, m],
            send_sem=qsend.at[layer, 0],
            recv_sem=qrecv.at[layer, m],
            device_id=(bi, m),
            device_id_type=MESH,
        )

    def bias_out(k):
        to = source(k)
        return pltpu.make_async_remote_copy(
            src_ref=biases.at[:, pl.ds(to * per * side, per * side)],
            dst_ref=bl.at[:, mine_b],
            send_sem=bsend.at[k],
            recv_sem=brecv.at[mi],
            device_id=(bi, to),
            device_id_type=MESH,
        )

    def bias_in(k):
        m = source(k)
        part = bl.at[:, pl.ds(m * per * side, per * side)]
        return pltpu.make_async_remote_copy(
            src_ref=part, dst_ref=part, send_sem=bsend.at[0], recv_sem=brecv.at[m],
            device_id=(bi, m), device_id_type=MESH,
        )

    for k in range(1, shards):
        quarter(0, k).start()
        bias_out(k).start()
    for layer in range(1, layers):
        for k in range(1, shards):
            quarter(layer, k).start()
    sums[...] = jnp.zeros_like(sums)

    def wcopy(p, b, to, ssem):
        layer, k, g = spot(p)
        part = wl.at[layer, b, source(k), pl.ds(g * n, n)]
        return pltpu.make_async_remote_copy(
            src_ref=part,
            dst_ref=part,
            send_sem=ssem,
            recv_sem=wrecv.at[b, p],
            device_id=(to, mi),
            device_id_type=MESH,
        )

    def relay(p, level, to):
        return (p % 2 == 1) & ((level // 2) == (to // 2)) & (level != to)

    def flow(t, drain):
        def go(cond, copy):
            @pl.when(cond)
            def _():
                copy.wait_send() if drain else copy.start()

        def arrive(p, b):
            if not drain:
                wcopy(p, b, bi, up.at[0, p]).wait_recv()

        def raise_(p, b, e):
            go(l < nl - 1, wcopy(p, b, group(jnp.minimum(l + 1, nl - 1), q), up.at[e, p]))

        def lower(p, b, e):
            go(l > 0, wcopy(p, b, group(jnp.maximum(l - 1, 0), q), dn.at[e, p]))

        def cross(p, b, level, cond):
            go(cond, wcopy(p, b, group(l, side_q), xs.at[level, p]))

        @pl.when(t < every)
        def _():
            if not drain:
                layer, k, g = spot(t)

                @pl.when((g == 0) & (k == 0))
                def _():
                    pltpu.make_async_copy(
                        tiles.at[layer, pl.ds(mi * per, per)],
                        wl.at[layer, bi, mi],
                        lsem.at[2 + layer],
                    ).wait()

                @pl.when((g == 0) & (k > 0))
                def _():
                    quarter_in(layer, k).wait_recv()

            raise_(t, bi, 0)
            lower(t, bi, 0)
            cross(t, bi, l, True)

        for d in range(1, nl):
            p = t - d

            @pl.when((p >= 0) & (p < every))
            def _(d=d, p=p):
                @pl.when(l - d >= 0)
                def _():
                    b = group(jnp.maximum(l - d, 0), q)
                    arrive(p, b)
                    raise_(p, b, d)
                    cross(p, b, jnp.maximum(l - d, 0), jnp.logical_not(relay(p, l - d, l)))

                @pl.when(l + d <= nl - 1)
                def _():
                    b = group(jnp.minimum(l + d, nl - 1), q)
                    arrive(p, b)
                    lower(p, b, d)
                    cross(p, b, jnp.minimum(l + d, nl - 1), jnp.logical_not(relay(p, l + d, l)))

                if d == 1:
                    @pl.when(p % 2 == 1)
                    def _():
                        b = group(l, side_q)
                        arrive(p, b)
                        go(l % 2 == 0, wcopy(p, b, group(jnp.minimum(l + 1, nl - 1), q), up.at[nl, p]))
                        go(l % 2 == 1, wcopy(p, b, group(jnp.maximum(l - 1, 0), q), dn.at[nl, p]))

    def landing(p):
        for level in range(nl):
            b = group(level, side_q)

            @pl.when((level != l) | (p % 2 == 0))
            def _(b=b):
                wcopy(p, b, bi, up.at[0, p]).wait_recv()

    def kept(layer, k, g):
        if layer < layers - 1:
            return st.at[k, pl.ds(g * n, n)]
        return fin.at[k, :, pl.ds(g * n * side, n * side)]

    def place(layer, m, g):
        if layer < layers - 1:
            return x2.at[pl.ds(m * per + g * n, n)]
        return out.at[:, pl.ds((m * per + g * n) * side, n * side)]

    def ocopy(layer, c):
        k, g = c // pieces, c % pieces
        return pltpu.make_async_remote_copy(
            src_ref=kept(layer, k, g),
            dst_ref=place(layer, mi, g),
            send_sem=osend.at[layer, c],
            recv_sem=orecv.at[layer, mi, g],
            device_id=(bi, source(k)),
            device_id_type=MESH,
        )

    def okeep(layer, g):
        return pltpu.make_async_copy(
            kept(layer, 0, g), place(layer, mi, g), osend.at[layer, g]
        )

    def ocopy_in(layer, m, g):
        part = place(layer, m, g)
        return pltpu.make_async_remote_copy(
            src_ref=part, dst_ref=part, send_sem=osend.at[layer, g],
            recv_sem=orecv.at[layer, m, g], device_id=(bi, m), device_id_type=MESH,
        )

    def hand_on(p):
        for layer in range(layers):
            c = p - layer * chunks

            @pl.when((c >= 0) & (c < pieces))
            def _(layer=layer, c=c):
                okeep(layer, c).start()

            @pl.when((c >= pieces) & (c < chunks))
            def _(layer=layer, c=c):
                ocopy(layer, c).start()

    def results_in(layer):
        @pl.loop(0, pieces)
        def _(g):
            okeep(layer, g).wait()
            for k in range(1, shards):
                ocopy_in(layer, source(k), g).wait_recv()

    def compute(layer, c):
        k, g = c // pieces, c % pieces
        m = source(k)
        src = xin if layer == 0 else x2
        for jj in range(n):
            j = g * n + jj
            base = ((layer * shards + m) * cb + mi * per + j) * fan
            xparts, wparts = [], []
            for t in range(fan):
                at = ids[base + t]
                xparts.append(src[at])
                wparts.append(wl[layer, :, m, j, t].reshape(side, side))
            whole = jnp.dot(
                jnp.concatenate(xparts, axis=1),
                jnp.concatenate(wparts, axis=0),
                preferred_element_type=jnp.float32,
            )
            bias = bl[layer : layer + 1, pl.ds(pl.multiple_of((m * per + j) * side, side), side)]
            res = jnp.clip(whole + bias, 0.0, 32.0).astype(out.dtype)
            if layer < layers - 1:
                st[k, j] = res
            else:
                fin[k, :, pl.ds(pl.multiple_of(j * side, side), side)] = res
                sums[...] += res.astype(jnp.float32)

    @pl.loop(0, every + depth + 1)
    def _(t):
        flow(t, False)
        p = t - depth

        @pl.when(p >= 1)
        def _():
            hand_on(p - 1)

        @pl.when(p == 0)
        def _():
            pltpu.make_async_copy(xin, xin, lsem.at[0]).wait()
            in_b.wait()
            for k in range(1, shards):
                bias_in(k).wait_recv()

        for layer in range(layers):
            if layer > 0:
                @pl.when(p == layer * chunks)
                def _(layer=layer):
                    results_in(layer - 1)

            @pl.when((p >= layer * chunks) & (p < (layer + 1) * chunks))
            def _(layer=layer):
                landing(p)
                compute(layer, p - layer * chunks)

    line[...] = jnp.broadcast_to(jnp.sum(sums[...].T, axis=0, keepdims=True), line.shape)

    @pl.loop(0, every + depth)
    def _(t):
        flow(t, True)

    for layer in range(layers):
        for k in range(1, shards):
            quarter(layer, k).wait_send()
    for k in range(1, shards):
        bias_out(k).wait_send()

    def mcopy(d, slot):
        return pltpu.make_async_remote_copy(
            src_ref=line,
            dst_ref=slots.at[slot],
            send_sem=msend.at[d],
            recv_sem=mrecv.at[slot],
            device_id=peer(d),
            device_id_type=MESH,
        )

    @pl.loop(1, total)
    def _(d):
        mcopy(d, me).start()

    slots[me] = line[...]
    for layer in range(layers):
        @pl.loop(pieces, chunks)
        def _(c, layer=layer):
            ocopy(layer, c).wait_send()

    @pl.loop(1, total)
    def _(d):
        mcopy(d, (me + d) % total).wait_recv()

    whole = jnp.zeros(line.shape, jnp.float32)
    for b in range(groups):
        one = slots[b * shards]
        for m in range(1, shards):
            one = one + slots[b * shards + m]
        whole = whole + one / neurons
    mine = slots[bi * shards]
    for m in range(1, shards):
        mine = mine + slots[bi * shards + m]
    rows_ref[...] = mine / neurons
    grand_ref[0, 0] = jnp.sum(whole[0:1]) / total_rows
    results_in(layers - 1)

    @pl.loop(1, total)
    def _(d):
        mcopy(d, me).wait_send()


def fused(geo, pieces, features, tiles, biases, in_block):
    nl, nq, _, nc = geo
    shards = lax.axis_size("mp")
    groups = lax.axis_size("batch")
    layers, cb, fan, depth, side = tiles.shape
    rows, width = features.shape
    per = cb // shards
    chunks = shards * pieces
    every = layers * chunks
    total = groups * shards
    dma = pltpu.SemaphoreType.DMA
    hbm = pl.BlockSpec(memory_space=pl.ANY)
    acts, row_means, grand = pl.pallas_call(
        functools.partial(
            fused_kernel, geo, pieces, cb * side * shards, rows * groups
        ),
        out_shape=(
            jax.ShapeDtypeStruct((rows, width), features.dtype),
            jax.ShapeDtypeStruct((8, rows), jnp.float32),
            jax.ShapeDtypeStruct((1, 1), jnp.float32),
        ),
        in_specs=[pl.BlockSpec(memory_space=pltpu.SMEM), hbm, hbm, hbm],
        out_specs=(
            hbm,
            pl.BlockSpec(memory_space=pltpu.VMEM),
            pl.BlockSpec(memory_space=pltpu.SMEM),
        ),
        scratch_shapes=[
            pltpu.VMEM((layers, groups, shards, per, fan, depth, side), tiles.dtype),
            pltpu.VMEM(biases.shape, biases.dtype),
            pltpu.VMEM((cb, rows, side), features.dtype),
            pltpu.VMEM((cb, rows, side), features.dtype),
            pltpu.VMEM((shards, per, rows, side), features.dtype),
            pltpu.VMEM((shards, rows, per * side), features.dtype),
            pltpu.VMEM((rows, side), jnp.float32),
            pltpu.VMEM((8, rows), jnp.float32),
            pltpu.VMEM((total, 8, rows), jnp.float32),
            dma((2 + layers,)),
            dma((layers, shards)),
            dma((layers, shards)),
            dma((shards,)),
            dma((shards,)),
            dma((nl + 1, every)),
            dma((nl + 1, every)),
            dma((nl, every)),
            dma((groups, every)),
            dma((layers, chunks)),
            dma((layers, shards, pieces)),
            dma((total,)),
            dma((total,)),
        ],
        compiler_params=pltpu.CompilerParams(
            collective_id=3,
            has_side_effects=True,
            vmem_limit_bytes=62 * 1024 * 1024,
        ),
        name="net",
    )((in_block % cb).reshape(-1), features, tiles, biases)
    return acts, row_means[0], grand[0, 0]


def suits(geo, shards, groups, features, tiles, biases):
    nl, nq, _, _ = geo
    kept = 2 * features.size + 2 * features.size + groups * tiles.size
    return (
        nq == 2
        and nl % 2 == 0
        and tiles.shape[0] == 2
        and tiles.shape[3] % 16 == 0
        and tiles.shape[1] // shards % PIECES == 0
        and groups * shards <= 64
        and 2 * kept < 56 * 1024 * 1024
    )


def on_device(geo, features, tiles, biases, in_block):
    shards = lax.axis_size("mp")
    groups = lax.axis_size("batch")
    me = lax.axis_index("mp")
    rows = features.shape[0]
    side = tiles.shape[4]
    cb = tiles.shape[1]
    fan = tiles.shape[2]
    if suits(geo, shards, groups, features, tiles, biases):
        return fused(geo, PIECES, features, tiles, biases, in_block)
    current = features
    mine = lax.dynamic_slice_in_dim(in_block, me * cb, cb, axis=1) % cb
    for layer in range(tiles.shape[0]):
        wall, xall = gather(geo, shards, groups, layer, tiles, current)
        current, sums = apply_layer(
            mine[layer].reshape(-1), xall, wall, biases[layer].reshape(1, -1)
        )
    row_means, whole = means(groups, shards, cb * side * shards, sums)
    grand = jnp.sum(whole) / (rows * groups)
    return (current, row_means, grand)


def solution(mesh):
    placed = (P("batch", "mp"), P(None, "mp", None, "batch", None), P(None, "mp"), P())
    return jax.shard_map(
        functools.partial(on_device, geometry(mesh)),
        mesh=mesh,
        in_specs=placed,
        out_specs=(P("batch", "mp"), P("batch"), P()),
        check_vma=False,
    )
```

```python
import functools
import math

import jax
import jax.numpy as jnp
from jax import lax
from jax.experimental import pallas as pl
from jax.experimental.pallas import tpu as pltpu
from jax.sharding import PartitionSpec as P

MESH = pl.DeviceIdType.MESH
PIECES = 4
HOP = 1


def geometry(mesh):
    groups, shards = mesh.devices.shape
    where = [getattr(d, "coords", None) for d in mesh.devices[:, 0]]
    if groups == 1 or where[0] is None or where[0] == where[1]:
        return groups, 1, True, 1
    moved = [i for i in range(len(where[0])) if where[0][i] != where[1][i]][0]
    minor = 1
    while minor < groups and all(
        where[minor][i] == where[0][i] for i in range(len(where[0])) if i != moved
    ):
        minor += 1
    major = groups // minor
    row = [d.coords for d in mesh.devices[0, :]]
    cores = sum(1 for c in row if c == row[0])
    if major >= minor:
        return major, minor, True, cores
    return minor, major, False, cores


def gather_kernel(
    geo, shards, layer, pieces,
    tiles, cur, wout, xout,
    wv, xv, lsem, wrecv, wup, wdn, wcross, whalf, xrecv, xfar, xcore,
):
    nl, nq, line_major, nc = geo
    ny = shards // nc
    bi = lax.axis_index("batch")
    mi = lax.axis_index("mp")
    if line_major:
        l, q = bi // nq, bi % nq
    else:
        l, q = bi % nl, bi // nl
    y, core = mi // nc, mi % nc
    step_w = tiles.shape[1] // pieces
    step_x = cur.shape[0] // pieces
    halves = nq == 2 and nl % 2 == 0
    first = pieces // 2

    def group(level, side):
        return level * nq + side if line_major else side * nl + level

    sides = [(q + d) % nq for d in range(1, nq)]
    fars = [((y + d) % ny) * nc + core for d in range(1, ny)]
    partners = [y * nc + (core + d) % nc for d in range(1, nc)]

    barrier = pltpu.get_barrier_semaphore()

    def greet(b, m):
        pl.semaphore_signal(barrier, inc=1, device_id=(b, m), device_id_type=MESH)

    @pl.when(l > 0)
    def _():
        greet(group(l - 1, q), mi)

    @pl.when(l < nl - 1)
    def _():
        greet(group(l + 1, q), mi)

    for side in sides:
        greet(group(l, side), mi)
    for m in fars + partners:
        greet(bi, m)
    near = jnp.where(l > 0, 1, 0) + jnp.where(l < nl - 1, 1, 0)
    pl.semaphore_wait(barrier, len(sides) + len(fars) + len(partners) + near)

    in_w = pltpu.make_async_copy(tiles.at[layer], wv, lsem.at[0])
    in_x = pltpu.make_async_copy(cur, xv, lsem.at[1])
    in_w.start()
    in_x.start()

    def wcopy(own, b, c, to, ssem):
        part = pl.ds(c * step_w, step_w)
        return pltpu.make_async_remote_copy(
            src_ref=tiles.at[layer, part] if own else wout.at[b, part],
            dst_ref=wout.at[b, part],
            send_sem=ssem,
            recv_sem=wrecv.at[b, c],
            device_id=(to, mi),
            device_id_type=MESH,
        )

    def xcopy(own, m, c, to, ssem):
        part = pl.ds(c * step_x, step_x)
        return pltpu.make_async_remote_copy(
            src_ref=cur.at[part] if own else xout.at[m, part],
            dst_ref=xout.at[m, part],
            send_sem=ssem,
            recv_sem=xrecv.at[m, c],
            device_id=(bi, to),
            device_id_type=MESH,
        )

    def phase(p, c, drain):
        def go(copy):
            copy.wait_send() if drain else copy.start()

        def arrived_w(b):
            if not drain:
                wcopy(False, b, c, bi, wup.at[0, c]).wait_recv()

        if p == 0:
            @pl.when(l < nl - 1)
            def _():
                go(wcopy(True, bi, c, group(l + 1, q), wup.at[0, c]))

            @pl.when(l > 0)
            def _():
                go(wcopy(True, bi, c, group(l - 1, q), wdn.at[0, c]))

            for i, side in enumerate(sides):
                go(wcopy(True, bi, c, group(l, side), wcross.at[i, l, c]))
            for i, m in enumerate(fars):
                go(xcopy(True, mi, c, m, xfar.at[i, c]))
            for i, m in enumerate(partners):
                go(xcopy(True, mi, c, m, xcore.at[i, y, c]))
        else:
            @pl.when(l - p >= 0)
            def _():
                b = group(l - p, q)
                arrived_w(b)

                @pl.when(l < nl - 1)
                def _():
                    go(wcopy(False, b, c, group(l + 1, q), wup.at[p, c]))

                def across():
                    for i, side in enumerate(sides):
                        go(wcopy(False, b, c, group(l, side), wcross.at[i, l - p, c]))

                if halves and p == 1:
                    pl.when((l < nl // 2) | (c < first))(across)
                else:
                    across()

            @pl.when(l + p <= nl - 1)
            def _():
                b = group(l + p, q)
                arrived_w(b)

                @pl.when(l > 0)
                def _():
                    go(wcopy(False, b, c, group(l - 1, q), wdn.at[p, c]))

                def across():
                    for i, side in enumerate(sides):
                        go(wcopy(False, b, c, group(l, side), wcross.at[i, l + p, c]))

                if halves and p == 1:
                    pl.when((l >= nl // 2) | (c < first))(across)
                else:
                    across()

            if halves and p == 1:
                @pl.when(c >= first)
                def _():
                    b = group(l, sides[0])
                    arrived_w(b)

                    @pl.when((l + 1 >= nl // 2) & (l < nl - 1))
                    def _():
                        go(wcopy(False, b, c, group(l + 1, q), whalf.at[0, c]))

                    @pl.when((l - 1 < nl // 2) & (l > 0))
                    def _():
                        go(wcopy(False, b, c, group(l - 1, q), whalf.at[1, c]))

        if p == nl - 1:
            for d, far in enumerate(fars):
                if not drain:
                    xcopy(False, far, c, mi, xfar.at[0, c]).wait_recv()
                for i, m in enumerate(partners):
                    go(xcopy(False, far, c, m, xcore.at[i, far // nc, c]))

    for p in range(nl):
        @pl.loop(0, pieces)
        def _(c, p=p):
            phase(p, c, False)

        if p == 0:
            in_w.wait()
            in_x.wait()
            out_w = pltpu.make_async_copy(wv, wout.at[bi], lsem.at[2])
            out_x = pltpu.make_async_copy(xv, xout.at[mi], lsem.at[3])
            out_w.start()
            out_x.start()

    @pl.loop(0, pieces)
    def _(c):
        for side in sides:
            for level in range(nl):
                b = group(level, side)

                def arrive(b=b):
                    wcopy(False, b, c, bi, wup.at[0, c]).wait_recv()

                if halves:
                    pl.when((l != level) | (c < first))(arrive)
                else:
                    arrive()
        for m in partners:
            for yy in range(ny):
                xcopy(False, yy * nc + m % nc, c, mi, xfar.at[0, c]).wait_recv()

    out_w.wait()
    out_x.wait()
    for p in range(nl):
        @pl.loop(0, pieces)
        def _(c, p=p):
            phase(p, c, True)


def gather(geo, shards, groups, layer, tiles, cur):
    nl, nq, _, nc = geo
    pieces = 8 if groups <= 8 else 2
    ny = shards // nc
    dma = pltpu.SemaphoreType.DMA
    return pl.pallas_call(
        functools.partial(gather_kernel, geo, shards, layer, pieces),
        out_shape=(
            jax.ShapeDtypeStruct((groups,) + tiles.shape[1:], tiles.dtype),
            jax.ShapeDtypeStruct((shards,) + cur.shape, cur.dtype),
        ),
        in_specs=[pl.BlockSpec(memory_space=pl.ANY)] * 2,
        out_specs=(pl.BlockSpec(memory_space=pl.ANY),) * 2,
        scratch_shapes=[
            pltpu.VMEM(tiles.shape[1:], tiles.dtype),
            pltpu.VMEM(cur.shape, cur.dtype),
            dma((4,)),
            dma((groups, pieces)),
            dma((nl, pieces)),
            dma((nl, pieces)),
            dma((max(nq - 1, 1), nl, pieces)),
            dma((2, pieces)),
            dma((shards, pieces)),
            dma((max(ny - 1, 1), pieces)),
            dma((max(nc - 1, 1), ny, pieces)),
        ],
        compiler_params=pltpu.CompilerParams(collective_id=layer, has_side_effects=True),
        name=f"gather_{layer}",
    )(tiles, cur)


def layer_kernel(ids, x_ref, w_ref, b_ref, o_ref, r_ref, xl, wl, s_ref, loads):
    shards, rows, _ = x_ref.shape
    _, cb, fan, _, side = w_ref.shape
    per_shard = cb // shards
    width = math.gcd(per_shard, 8)

    def pulls(s):
        part = pl.ds(s * per_shard, per_shard)
        return (
            pltpu.make_async_copy(x_ref.at[s], xl.at[s], loads.at[0, s]),
            pltpu.make_async_copy(w_ref.at[:, part], wl.at[:, part], loads.at[1, s]),
        )

    for s in range(min(2, shards)):
        for pull in pulls(s):
            pull.start()
    s_ref[...] = jnp.zeros_like(s_ref)
    for s in range(shards):
        for pull in pulls(s):
            pull.wait()
        if s + 2 < shards:
            for pull in pulls(s + 2):
                pull.start()

        @pl.loop(0, per_shard // width)
        def _(k, s=s):
            for jj in range(width):
                j = s * per_shard + k * width + jj
                xs, ws = [], []
                for t in range(fan):
                    at = ids[j * fan + t]
                    xs.append(xl[s, :, pl.ds(pl.multiple_of(at * side, side), side)])
                    ws.append(wl[:, j, t].reshape(side, side))
                total = jnp.dot(
                    jnp.concatenate(xs, axis=1),
                    jnp.concatenate(ws, axis=0),
                    preferred_element_type=jnp.float32,
                )
                cols = pl.ds(pl.multiple_of(j * side, side), side)
                out = jnp.clip(total + b_ref[:, cols], 0.0, 32.0).astype(o_ref.dtype)
                o_ref[:, cols] = out
                s_ref[...] += out.astype(jnp.float32)

    line = jnp.sum(s_ref[...].T, axis=0, keepdims=True)
    r_ref[...] = jnp.broadcast_to(line, r_ref.shape)


def apply_layer(ids, xall, wall, bias):
    shards, rows, width = xall.shape
    side = wall.shape[4]
    hbm = pl.BlockSpec(memory_space=pl.ANY)
    vmem = pl.BlockSpec(memory_space=pltpu.VMEM)
    return pl.pallas_call(
        layer_kernel,
        out_shape=(
            jax.ShapeDtypeStruct((rows, width), xall.dtype),
            jax.ShapeDtypeStruct((8, rows), jnp.float32),
        ),
        in_specs=[pl.BlockSpec(memory_space=pltpu.SMEM), hbm, hbm, vmem],
        out_specs=(vmem, vmem),
        scratch_shapes=[
            pltpu.VMEM(xall.shape, xall.dtype),
            pltpu.VMEM(wall.shape, wall.dtype),
            pltpu.VMEM((rows, side), jnp.float32),
            pltpu.SemaphoreType.DMA((2, shards)),
        ],
        compiler_params=pltpu.CompilerParams(vmem_limit_bytes=52 * 1024 * 1024),
        name="layer",
    )(ids, xall, wall, bias)


def means_kernel(groups, shards, neurons, x_ref, rows_ref, all_ref, slots, ssem, rsem):
    bi = lax.axis_index("batch")
    mi = lax.axis_index("mp")
    me = bi * shards + mi
    total = groups * shards
    barrier = pltpu.get_barrier_semaphore()

    def peer(d):
        to = (me + d) % total
        return to // shards, to % shards

    @pl.loop(1, total)
    def _(d):
        pl.semaphore_signal(barrier, inc=1, device_id=peer(d), device_id_type=MESH)

    pl.semaphore_wait(barrier, total - 1)

    def copy(d, slot):
        return pltpu.make_async_remote_copy(
            src_ref=x_ref,
            dst_ref=slots.at[slot],
            send_sem=ssem.at[d],
            recv_sem=rsem.at[slot],
            device_id=peer(d),
            device_id_type=MESH,
        )

    @pl.loop(1, total)
    def _(d):
        copy(d, me).start()

    slots[me] = x_ref[...]

    @pl.loop(1, total)
    def _(d):
        copy(d, (me + d) % total).wait_recv()

    whole = jnp.zeros(all_ref.shape, jnp.float32)
    for b in range(groups):
        one = slots[b * shards]
        for m in range(1, shards):
            one = one + slots[b * shards + m]
        whole = whole + one / neurons
    all_ref[...] = whole
    mine = slots[bi * shards]
    for m in range(1, shards):
        mine = mine + slots[bi * shards + m]
    rows_ref[...] = mine / neurons

    @pl.loop(1, total)
    def _(d):
        copy(d, me).wait_send()


def means(groups, shards, neurons, sums):
    total = groups * shards
    if total > 64:
        shard_sum = lax.psum(sums[0], "mp") / neurons
        return shard_sum, lax.psum(shard_sum, "batch")
    vmem = pl.BlockSpec(memory_space=pltpu.VMEM)
    like = jax.ShapeDtypeStruct(sums.shape, jnp.float32)
    mine, whole = pl.pallas_call(
        functools.partial(means_kernel, groups, shards, neurons),
        out_shape=(like, like),
        in_specs=[vmem],
        out_specs=(vmem, vmem),
        scratch_shapes=[
            pltpu.VMEM((total,) + sums.shape, jnp.float32),
            pltpu.SemaphoreType.DMA((total,)),
            pltpu.SemaphoreType.DMA((total,)),
        ],
        compiler_params=pltpu.CompilerParams(collective_id=20, has_side_effects=True),
        name="means",
    )(sums)
    return mine[0], whole[0]


def fused_kernel(
    geo, pieces, neurons, total_rows,
    ids, feats, tiles, biases, out, rows_ref, grand_ref,
    wl, bl, xin, x2, st, fin, sums, line, slots,
    lsem, qsend, qrecv, bsem, up, dn, xs, wrecv, xrecv, rrecv,
    osend, okept, orecv, msem,
):
    nl, nq, line_major, nc = geo
    layers, groups, shards, per, fan, _, side = wl.shape
    ny = shards // nc
    cb = per * shards
    n = per // pieces
    chunks = shards * pieces
    every = layers * chunks
    depth = HOP * nl
    half = every
    bi = lax.axis_index("batch")
    mi = lax.axis_index("mp")
    if line_major:
        l, q = bi // nq, bi % nq
    else:
        l, q = bi % nl, bi // nl
    y, core = mi // nc, mi % nc
    side_q = (q + 1) % nq
    total = groups * shards
    me = bi * shards + mi

    def group(level, column):
        return level * nq + column if line_major else column * nl + level

    def source(k):
        return ((y + k // nc) % ny) * nc + (core + k % nc) % nc

    def turn(layer, c):
        k = c // pieces
        return jnp.where(layer == layers - 1, shards - 1 - k, k) if layers > 1 else k

    def spot(p):
        c = p % chunks
        return p // chunks, turn(p // chunks, c), c % pieces

    def peer(d):
        to = (me + d) % total
        return to // shards, to % shards

    @pl.loop(0, cb)
    def _(j):
        pltpu.make_async_copy(
            feats.at[:, pl.ds(j * side, side)], xin.at[j], lsem.at[0]
        ).start()

    def own_quarter(layer):
        return pltpu.make_async_copy(
            tiles.at[layer, pl.ds(mi * per, per)], wl.at[layer, bi, mi], lsem.at[2 + layer]
        )

    for layer in range(layers):
        own_quarter(layer).start()
    mine_b = pl.ds(mi * per * side, per * side)
    in_b = pltpu.make_async_copy(biases.at[:, mine_b], bl.at[:, mine_b], lsem.at[1])
    in_b.start()

    barrier = pltpu.get_barrier_semaphore()

    def greet(b, m):
        pl.semaphore_signal(barrier, inc=1, device_id=(b, m), device_id_type=MESH)

    @pl.when(l > 0)
    def _():
        greet(group(l - 1, q), mi)

    @pl.when(l < nl - 1)
    def _():
        greet(group(l + 1, q), mi)

    greet(group(l, side_q), mi)
    for k in range(1, shards):
        greet(bi, source(k))
    near = jnp.where(l > 0, 1, 0) + jnp.where(l < nl - 1, 1, 0)
    pl.semaphore_wait(barrier, near + shards)

    def quarter(layer, k):
        to = source(k)
        return pltpu.make_async_remote_copy(
            src_ref=tiles.at[layer, pl.ds(to * per, per)],
            dst_ref=wl.at[layer, bi, mi],
            send_sem=qsend,
            recv_sem=qrecv.at[layer, mi],
            device_id=(bi, to),
            device_id_type=MESH,
        )

    def quarter_in(layer, k):
        m = source(k)
        return pltpu.make_async_remote_copy(
            src_ref=wl.at[layer, bi, m],
            dst_ref=wl.at[layer, bi, m],
            send_sem=qsend,
            recv_sem=qrecv.at[layer, m],
            device_id=(bi, m),
            device_id_type=MESH,
        )

    def bias_out(k):
        to = source(k)
        return pltpu.make_async_remote_copy(
            src_ref=biases.at[:, pl.ds(to * per * side, per * side)],
            dst_ref=bl.at[:, mine_b],
            send_sem=bsem.at[0],
            recv_sem=bsem.at[1],
            device_id=(bi, to),
            device_id_type=MESH,
        )

    def biases_of_others():
        part = bl.at[:, pl.ds(0, (shards - 1) * per * side)]
        return pltpu.make_async_remote_copy(
            src_ref=part, dst_ref=part, send_sem=bsem.at[0], recv_sem=bsem.at[1],
            device_id=(bi, mi), device_id_type=MESH,
        )

    for k in range(1, shards):
        quarter(0, k).start()
        bias_out(k).start()
    for layer in range(1, layers):
        for k in range(1, shards):
            quarter(layer, k).start()
    sums[...] = jnp.zeros_like(sums)

    def wcopy(p, b, to, ssem, rsem):
        layer, k, g = spot(p)
        part = wl.at[layer, b, source(k), pl.ds(g * n, n)]
        return pltpu.make_async_remote_copy(
            src_ref=part,
            dst_ref=part,
            send_sem=ssem,
            recv_sem=rsem,
            device_id=(to, mi),
            device_id_type=MESH,
        )

    def sent(part, ssem):
        pltpu.make_async_remote_copy(
            src_ref=part, dst_ref=part, send_sem=ssem, recv_sem=rrecv.at[0],
            device_id=(bi, mi), device_id_type=MESH,
        ).wait_send()

    def relay(p, level, to):
        return (p % 2 == 1) & ((level // 2) == (to // 2)) & (level != to)

    def flow(t):
        def go(cond, copy):
            @pl.when(cond)
            def _():
                copy.start()

        def arrive(p, level):
            wcopy(p, bi, bi, up.at[0], wrecv.at[level, p]).wait_recv()

        def raise_(p, b, level, e):
            to = group(jnp.minimum(l + 1, nl - 1), q)
            go(l < nl - 1, wcopy(p, b, to, up.at[e], wrecv.at[level, p]))

        def lower(p, b, level, e):
            to = group(jnp.maximum(l - 1, 0), q)
            go(l > 0, wcopy(p, b, to, dn.at[e], wrecv.at[level, p]))

        def cross(p, b, level, own):
            to = group(l, side_q)
            if own:
                go(p % 2 == 0, wcopy(p, b, to, xs.at[level], xrecv.at[p]))
                go(p % 2 == 1, wcopy(p, b, to, xs.at[level], rrecv.at[p]))
            else:
                cond = jnp.logical_not(relay(p, level, l))
                go(cond, wcopy(p, b, to, xs.at[level], xrecv.at[p]))

        def at(early, late):
            first, second = t - HOP * early, t - HOP * late
            p = jnp.where(first < half, first, second)
            return p, (p >= 0) & (p < every) & ((first < half) | (second >= half))

        below, above = l, nl - 1 - l
        turn_x = jnp.maximum(below, above) - 1

        @pl.when(t < every)
        def _():
            layer, k, g = spot(t)

            @pl.when((g == 0) & (k == 0))
            def _():
                own_quarter(layer).wait()

            @pl.when((g == 0) & (k > 0))
            def _():
                quarter_in(layer, k).wait_recv()

        p, ok = at(0, below)

        @pl.when(ok)
        def _(p=p):
            raise_(p, bi, l, 0)

        p, ok = at(0, above)

        @pl.when(ok)
        def _(p=p):
            lower(p, bi, l, 0)

        p, ok = at(0, turn_x)

        @pl.when(ok)
        def _(p=p):
            cross(p, bi, l, True)

        def across(p):
            b = group(l, side_q)
            wcopy(p, b, bi, up.at[0], rrecv.at[p]).wait_recv()
            upper = group(jnp.minimum(l + 1, nl - 1), q)
            under = group(jnp.maximum(l - 1, 0), q)
            go(l % 2 == 0, wcopy(p, b, upper, up.at[nl], xrecv.at[p]))
            go(l % 2 == 1, wcopy(p, b, under, dn.at[nl], xrecv.at[p]))

        for d in range(1, nl):
            p, ok = at(d, below)

            @pl.when(ok & (l - d >= 0))
            def _(d=d, p=p):
                level = jnp.maximum(l - d, 0)
                arrive(p, level)
                raise_(p, group(level, q), level, d)
                cross(p, group(level, q), level, False)

            p, ok = at(d, above)

            @pl.when(ok & (l + d <= nl - 1))
            def _(d=d, p=p):
                level = jnp.minimum(l + d, nl - 1)
                arrive(p, level)
                lower(p, group(level, q), level, d)
                cross(p, group(level, q), level, False)

            if d == 1:
                p, ok = at(1, turn_x + 1)

                @pl.when(ok & (p % 2 == 1))
                def _(p=p):
                    across(p)

    def landing(p):
        layer, k, g = spot(p)

        def wait(count):
            part = wl.at[layer, pl.ds(0, count), source(k), pl.ds(g * n, n)]
            pltpu.make_async_remote_copy(
                src_ref=part, dst_ref=part, send_sem=up.at[0], recv_sem=xrecv.at[p],
                device_id=(bi, mi), device_id_type=MESH,
            ).wait_recv()

        @pl.when(p % 2 == 0)
        def _():
            wait(nl)

        @pl.when(p % 2 == 1)
        def _():
            wait(nl - 1)

    def kept(layer, k, g):
        if layer < layers - 1:
            return st.at[k, pl.ds(g * n, n)]
        return fin.at[k, :, pl.ds(g * n * side, n * side)]

    def place(layer, m, g):
        if layer < layers - 1:
            return x2.at[pl.ds(m * per + g * n, n)]
        return out.at[:, pl.ds((m * per + g * n) * side, n * side)]

    def ocopy(layer, c):
        k, g = turn(layer, c), c % pieces
        return pltpu.make_async_remote_copy(
            src_ref=kept(layer, k, g),
            dst_ref=place(layer, mi, g),
            send_sem=osend.at[layer],
            recv_sem=orecv.at[layer],
            device_id=(bi, source(k)),
            device_id_type=MESH,
        )

    def okeep(layer, g):
        return pltpu.make_async_copy(
            kept(layer, 0, g), place(layer, mi, g), okept.at[layer]
        )

    def hand_on(p):
        for layer in range(layers):
            c = p - layer * chunks

            inside = (c >= 0) & (c < chunks)
            k = turn(layer, c)

            @pl.when(inside & (k == 0))
            def _(layer=layer, c=c):
                okeep(layer, c % pieces).start()

            @pl.when(inside & (k > 0))
            def _(layer=layer, c=c):
                ocopy(layer, c).start()

    def others(layer):
        if layer < layers - 1:
            return st.at[pl.ds(0, shards - 1)]
        return fin.at[pl.ds(0, shards - 1)]

    def results_in(layer):
        mine = st.at[0] if layer < layers - 1 else fin.at[0]
        pltpu.make_async_copy(mine, mine, okept.at[layer]).wait()
        part = others(layer)
        pltpu.make_async_remote_copy(
            src_ref=part, dst_ref=part, send_sem=osend.at[layer],
            recv_sem=orecv.at[layer], device_id=(bi, mi), device_id_type=MESH,
        ).wait_recv()

    def compute(layer, c):
        k, g = turn(layer, c), c % pieces
        m = source(k)
        src = xin if layer == 0 else x2
        for jj in range(n):
            j = g * n + jj
            column = m * cb + mi * per + j
            xparts, wparts = [], []
            for t in range(fan):
                at = lax.rem(ids[t, layer, column], cb)
                xparts.append(src[at])
                wparts.append(wl[layer, :, m, j, t].reshape(side, side))
            whole = jnp.dot(
                jnp.concatenate(xparts, axis=1),
                jnp.concatenate(wparts, axis=0),
                preferred_element_type=jnp.float32,
            )
            bias = bl[layer : layer + 1, pl.ds(pl.multiple_of((m * per + j) * side, side), side)]
            res = jnp.clip(whole + bias, 0.0, 32.0).astype(out.dtype)
            if layer < layers - 1:
                st[k, j] = res
            else:
                fin[k, :, pl.ds(pl.multiple_of(j * side, side), side)] = res
                sums[...] += res.astype(jnp.float32)

    @pl.loop(0, every + depth + 1)
    def _(t):
        flow(t)
        p = t - depth

        @pl.when(p >= 1)
        def _():
            hand_on(p - 1)

        @pl.when(p == 0)
        def _():
            pltpu.make_async_copy(xin, xin, lsem.at[0]).wait()
            in_b.wait()
            biases_of_others().wait_recv()

        for layer in range(layers):
            if layer > 0:
                @pl.when(p == layer * chunks)
                def _(layer=layer):
                    results_in(layer - 1)

            @pl.when((p >= layer * chunks) & (p < (layer + 1) * chunks))
            def _(layer=layer):
                landing(p)
                compute(layer, p - layer * chunks)

    line[...] = jnp.broadcast_to(jnp.sum(sums[...].T, axis=0, keepdims=True), line.shape)

    def mcopy(d, slot):
        return pltpu.make_async_remote_copy(
            src_ref=line,
            dst_ref=slots.at[slot],
            send_sem=msem.at[0],
            recv_sem=msem.at[1],
            device_id=peer(d),
            device_id_type=MESH,
        )

    @pl.when(l < nl - 1)
    def _():
        for d in range(nl):
            @pl.when(l - d >= 0)
            def _(d=d):
                sent(wl.at[:, bi], up.at[d])

    @pl.when(l > 0)
    def _():
        for d in range(nl):
            @pl.when(l + d <= nl - 1)
            def _(d=d):
                sent(wl.at[:, bi], dn.at[d])

    @pl.when(l % 2 == 0)
    def _():
        sent(wl.at[0, bi], up.at[nl])

    @pl.when(l % 2 == 1)
    def _():
        sent(wl.at[0, bi], dn.at[nl])

    for level in range(nl):
        paired = (l // 2 == level // 2) & (l != level)

        @pl.when(paired)
        def _(level=level):
            sent(wl.at[0, bi], xs.at[level])

        @pl.when(jnp.logical_not(paired))
        def _(level=level):
            sent(wl.at[:, bi], xs.at[level])

    sent(wl.at[:, bi, pl.ds(0, shards - 1)], qsend)
    biases_of_others().wait_send()

    @pl.loop(1, total)
    def _(d):
        mcopy(d, me).start()

    slots[me] = line[...]
    for layer in range(layers):
        sent(others(layer), osend.at[layer])
    lines = slots.at[pl.ds(0, total - 1)]
    exchanged = pltpu.make_async_remote_copy(
        src_ref=lines, dst_ref=lines, send_sem=msem.at[0], recv_sem=msem.at[1],
        device_id=(bi, mi), device_id_type=MESH,
    )
    exchanged.wait_recv()
    whole = jnp.zeros(line.shape, jnp.float32)
    for b in range(groups):
        one = slots[b * shards]
        for m in range(1, shards):
            one = one + slots[b * shards + m]
        whole = whole + one / neurons
    mine = slots[bi * shards]
    for m in range(1, shards):
        mine = mine + slots[bi * shards + m]
    rows_ref[...] = mine[0:1] / neurons
    grand_ref[0, 0] = jnp.sum(whole[0:1]) / total_rows
    results_in(layers - 1)
    exchanged.wait_send()


def fused(geo, pieces, features, tiles, biases, in_block):
    nl, nq, _, nc = geo
    shards = lax.axis_size("mp")
    groups = lax.axis_size("batch")
    layers, cb, fan, depth, side = tiles.shape
    rows, width = features.shape
    per = cb // shards
    chunks = shards * pieces
    every = layers * chunks
    total = groups * shards
    dma = pltpu.SemaphoreType.DMA
    hbm = pl.BlockSpec(memory_space=pltpu.HBM)
    acts, row_means, grand = pl.pallas_call(
        functools.partial(
            fused_kernel, geo, pieces, cb * side * shards, rows * groups
        ),
        out_shape=(
            jax.ShapeDtypeStruct((rows, width), features.dtype),
            jax.ShapeDtypeStruct((1, rows), jnp.float32),
            jax.ShapeDtypeStruct((1, 1), jnp.float32),
        ),
        in_specs=[pl.BlockSpec(memory_space=pltpu.SMEM), hbm, hbm, hbm],
        out_specs=(
            pl.BlockSpec(memory_space=pl.ANY),
            pl.BlockSpec(memory_space=pltpu.VMEM),
            pl.BlockSpec(memory_space=pltpu.SMEM),
        ),
        scratch_shapes=[
            pltpu.VMEM((layers, groups, shards, per, fan, depth, side), tiles.dtype),
            pltpu.VMEM(biases.shape, biases.dtype),
            pltpu.VMEM((cb, rows, side), features.dtype),
            pltpu.VMEM((cb, rows, side), features.dtype),
            pltpu.VMEM((shards, per, rows, side), features.dtype),
            pltpu.VMEM((shards, rows, per * side), features.dtype),
            pltpu.VMEM((rows, side), jnp.float32),
            pltpu.VMEM((8, rows), jnp.float32),
            pltpu.VMEM((total, 8, rows), jnp.float32),
            dma((2 + layers,)),
            dma(()),
            dma((layers, shards)),
            dma((2,)),
            dma((nl + 1,)),
            dma((nl + 1,)),
            dma((nl,)),
            dma((nl, every)),
            dma((every,)),
            dma((every,)),
            dma((layers,)),
            dma((layers,)),
            dma((layers,)),
            dma((2,)),
        ],
        compiler_params=pltpu.CompilerParams(
            collective_id=3,
            has_side_effects=True,
            vmem_limit_bytes=46 * 1024 * 1024,
        ),
        name="net",
    )(in_block.transpose(2, 0, 1), features, tiles, biases)
    return acts, row_means[0], grand[0, 0]


def suits(geo, shards, groups, features, tiles, biases):
    nl, nq, _, _ = geo
    kept = 2 * features.size + 2 * features.size + groups * tiles.size
    return (
        nq == 2
        and nl % 2 == 0
        and tiles.shape[0] == 2
        and tiles.shape[3] % 16 == 0
        and tiles.shape[1] // shards % PIECES == 0
        and groups * shards <= 64
        and 2 * kept < 56 * 1024 * 1024
    )


def on_device(geo, features, tiles, biases, in_block):
    shards = lax.axis_size("mp")
    groups = lax.axis_size("batch")
    me = lax.axis_index("mp")
    rows = features.shape[0]
    side = tiles.shape[4]
    cb = tiles.shape[1]
    fan = tiles.shape[2]
    if suits(geo, shards, groups, features, tiles, biases):
        return fused(geo, PIECES, features, tiles, biases, in_block)
    current = features
    mine = lax.dynamic_slice_in_dim(in_block, me * cb, cb, axis=1) % cb
    for layer in range(tiles.shape[0]):
        wall, xall = gather(geo, shards, groups, layer, tiles, current)
        current, sums = apply_layer(
            mine[layer].reshape(-1), xall, wall, biases[layer].reshape(1, -1)
        )
    row_means, whole = means(groups, shards, cb * side * shards, sums)
    grand = jnp.sum(whole) / (rows * groups)
    return (current, row_means, grand)


def solution(mesh):
    placed = (P("batch", "mp"), P(None, "mp", None, "batch", None), P(None, "mp"), P())
    return jax.shard_map(
        functools.partial(on_device, geometry(mesh)),
        mesh=mesh,
        in_specs=placed,
        out_specs=(P("batch", "mp"), P("batch"), P()),
        check_vma=False,
    )
```

```python
import functools
import math

import jax
import jax.numpy as jnp
from jax import lax
from jax.experimental import pallas as pl
from jax.experimental.pallas import tpu as pltpu
from jax.sharding import PartitionSpec as P

MESH = pl.DeviceIdType.MESH
PIECES = 4


def geometry(mesh):
    groups, shards = mesh.devices.shape
    where = [getattr(d, "coords", None) for d in mesh.devices[:, 0]]
    if groups == 1 or where[0] is None or where[0] == where[1]:
        return groups, 1, True, 1
    moved = [i for i in range(len(where[0])) if where[0][i] != where[1][i]][0]
    minor = 1
    while minor < groups and all(
        where[minor][i] == where[0][i] for i in range(len(where[0])) if i != moved
    ):
        minor += 1
    major = groups // minor
    row = [d.coords for d in mesh.devices[0, :]]
    cores = sum(1 for c in row if c == row[0])
    if major >= minor:
        return major, minor, True, cores
    return minor, major, False, cores


def gather_kernel(
    geo, shards, layer, pieces,
    tiles, cur, wout, xout,
    wv, xv, lsem, wrecv, wup, wdn, wcross, whalf, xrecv, xfar, xcore,
):
    nl, nq, line_major, nc = geo
    ny = shards // nc
    bi = lax.axis_index("batch")
    mi = lax.axis_index("mp")
    if line_major:
        l, q = bi // nq, bi % nq
    else:
        l, q = bi % nl, bi // nl
    y, core = mi // nc, mi % nc
    step_w = tiles.shape[1] // pieces
    step_x = cur.shape[0] // pieces
    halves = nq == 2 and nl % 2 == 0
    first = pieces // 2

    def group(level, side):
        return level * nq + side if line_major else side * nl + level

    sides = [(q + d) % nq for d in range(1, nq)]
    fars = [((y + d) % ny) * nc + core for d in range(1, ny)]
    partners = [y * nc + (core + d) % nc for d in range(1, nc)]

    barrier = pltpu.get_barrier_semaphore()

    def greet(b, m):
        pl.semaphore_signal(barrier, inc=1, device_id=(b, m), device_id_type=MESH)

    @pl.when(l > 0)
    def _():
        greet(group(l - 1, q), mi)

    @pl.when(l < nl - 1)
    def _():
        greet(group(l + 1, q), mi)

    for side in sides:
        greet(group(l, side), mi)
    for m in fars + partners:
        greet(bi, m)
    near = jnp.where(l > 0, 1, 0) + jnp.where(l < nl - 1, 1, 0)
    pl.semaphore_wait(barrier, len(sides) + len(fars) + len(partners) + near)

    in_w = pltpu.make_async_copy(tiles.at[layer], wv, lsem.at[0])
    in_x = pltpu.make_async_copy(cur, xv, lsem.at[1])
    in_w.start()
    in_x.start()

    def wcopy(own, b, c, to, ssem):
        part = pl.ds(c * step_w, step_w)
        return pltpu.make_async_remote_copy(
            src_ref=tiles.at[layer, part] if own else wout.at[b, part],
            dst_ref=wout.at[b, part],
            send_sem=ssem,
            recv_sem=wrecv.at[b, c],
            device_id=(to, mi),
            device_id_type=MESH,
        )

    def xcopy(own, m, c, to, ssem):
        part = pl.ds(c * step_x, step_x)
        return pltpu.make_async_remote_copy(
            src_ref=cur.at[part] if own else xout.at[m, part],
            dst_ref=xout.at[m, part],
            send_sem=ssem,
            recv_sem=xrecv.at[m, c],
            device_id=(bi, to),
            device_id_type=MESH,
        )

    def phase(p, c, drain):
        def go(copy):
            copy.wait_send() if drain else copy.start()

        def arrived_w(b):
            if not drain:
                wcopy(False, b, c, bi, wup.at[0, c]).wait_recv()

        if p == 0:
            @pl.when(l < nl - 1)
            def _():
                go(wcopy(True, bi, c, group(l + 1, q), wup.at[0, c]))

            @pl.when(l > 0)
            def _():
                go(wcopy(True, bi, c, group(l - 1, q), wdn.at[0, c]))

            for i, side in enumerate(sides):
                go(wcopy(True, bi, c, group(l, side), wcross.at[i, l, c]))
            for i, m in enumerate(fars):
                go(xcopy(True, mi, c, m, xfar.at[i, c]))
            for i, m in enumerate(partners):
                go(xcopy(True, mi, c, m, xcore.at[i, y, c]))
        else:
            @pl.when(l - p >= 0)
            def _():
                b = group(l - p, q)
                arrived_w(b)

                @pl.when(l < nl - 1)
                def _():
                    go(wcopy(False, b, c, group(l + 1, q), wup.at[p, c]))

                def across():
                    for i, side in enumerate(sides):
                        go(wcopy(False, b, c, group(l, side), wcross.at[i, l - p, c]))

                if halves and p == 1:
                    pl.when((l < nl // 2) | (c < first))(across)
                else:
                    across()

            @pl.when(l + p <= nl - 1)
            def _():
                b = group(l + p, q)
                arrived_w(b)

                @pl.when(l > 0)
                def _():
                    go(wcopy(False, b, c, group(l - 1, q), wdn.at[p, c]))

                def across():
                    for i, side in enumerate(sides):
                        go(wcopy(False, b, c, group(l, side), wcross.at[i, l + p, c]))

                if halves and p == 1:
                    pl.when((l >= nl // 2) | (c < first))(across)
                else:
                    across()

            if halves and p == 1:
                @pl.when(c >= first)
                def _():
                    b = group(l, sides[0])
                    arrived_w(b)

                    @pl.when((l + 1 >= nl // 2) & (l < nl - 1))
                    def _():
                        go(wcopy(False, b, c, group(l + 1, q), whalf.at[0, c]))

                    @pl.when((l - 1 < nl // 2) & (l > 0))
                    def _():
                        go(wcopy(False, b, c, group(l - 1, q), whalf.at[1, c]))

        if p == nl - 1:
            for d, far in enumerate(fars):
                if not drain:
                    xcopy(False, far, c, mi, xfar.at[0, c]).wait_recv()
                for i, m in enumerate(partners):
                    go(xcopy(False, far, c, m, xcore.at[i, far // nc, c]))

    for p in range(nl):
        @pl.loop(0, pieces)
        def _(c, p=p):
            phase(p, c, False)

        if p == 0:
            in_w.wait()
            in_x.wait()
            out_w = pltpu.make_async_copy(wv, wout.at[bi], lsem.at[2])
            out_x = pltpu.make_async_copy(xv, xout.at[mi], lsem.at[3])
            out_w.start()
            out_x.start()

    @pl.loop(0, pieces)
    def _(c):
        for side in sides:
            for level in range(nl):
                b = group(level, side)

                def arrive(b=b):
                    wcopy(False, b, c, bi, wup.at[0, c]).wait_recv()

                if halves:
                    pl.when((l != level) | (c < first))(arrive)
                else:
                    arrive()
        for m in partners:
            for yy in range(ny):
                xcopy(False, yy * nc + m % nc, c, mi, xfar.at[0, c]).wait_recv()

    out_w.wait()
    out_x.wait()
    for p in range(nl):
        @pl.loop(0, pieces)
        def _(c, p=p):
            phase(p, c, True)


def gather(geo, shards, groups, layer, tiles, cur):
    nl, nq, _, nc = geo
    pieces = 8 if groups <= 8 else 2
    ny = shards // nc
    dma = pltpu.SemaphoreType.DMA
    return pl.pallas_call(
        functools.partial(gather_kernel, geo, shards, layer, pieces),
        out_shape=(
            jax.ShapeDtypeStruct((groups,) + tiles.shape[1:], tiles.dtype),
            jax.ShapeDtypeStruct((shards,) + cur.shape, cur.dtype),
        ),
        in_specs=[pl.BlockSpec(memory_space=pl.ANY)] * 2,
        out_specs=(pl.BlockSpec(memory_space=pl.ANY),) * 2,
        scratch_shapes=[
            pltpu.VMEM(tiles.shape[1:], tiles.dtype),
            pltpu.VMEM(cur.shape, cur.dtype),
            dma((4,)),
            dma((groups, pieces)),
            dma((nl, pieces)),
            dma((nl, pieces)),
            dma((max(nq - 1, 1), nl, pieces)),
            dma((2, pieces)),
            dma((shards, pieces)),
            dma((max(ny - 1, 1), pieces)),
            dma((max(nc - 1, 1), ny, pieces)),
        ],
        compiler_params=pltpu.CompilerParams(collective_id=layer, has_side_effects=True),
        name=f"gather_{layer}",
    )(tiles, cur)


def layer_kernel(ids, x_ref, w_ref, b_ref, o_ref, r_ref, xl, wl, s_ref, loads):
    shards, rows, _ = x_ref.shape
    _, cb, fan, _, side = w_ref.shape
    per_shard = cb // shards
    width = math.gcd(per_shard, 8)

    def pulls(s):
        part = pl.ds(s * per_shard, per_shard)
        return (
            pltpu.make_async_copy(x_ref.at[s], xl.at[s], loads.at[0, s]),
            pltpu.make_async_copy(w_ref.at[:, part], wl.at[:, part], loads.at[1, s]),
        )

    for s in range(min(2, shards)):
        for pull in pulls(s):
            pull.start()
    s_ref[...] = jnp.zeros_like(s_ref)
    for s in range(shards):
        for pull in pulls(s):
            pull.wait()
        if s + 2 < shards:
            for pull in pulls(s + 2):
                pull.start()

        @pl.loop(0, per_shard // width)
        def _(k, s=s):
            for jj in range(width):
                j = s * per_shard + k * width + jj
                xs, ws = [], []
                for t in range(fan):
                    at = ids[j * fan + t]
                    xs.append(xl[s, :, pl.ds(pl.multiple_of(at * side, side), side)])
                    ws.append(wl[:, j, t].reshape(side, side))
                total = jnp.dot(
                    jnp.concatenate(xs, axis=1),
                    jnp.concatenate(ws, axis=0),
                    preferred_element_type=jnp.float32,
                )
                cols = pl.ds(pl.multiple_of(j * side, side), side)
                out = jnp.clip(total + b_ref[:, cols], 0.0, 32.0).astype(o_ref.dtype)
                o_ref[:, cols] = out
                s_ref[...] += out.astype(jnp.float32)

    line = jnp.sum(s_ref[...].T, axis=0, keepdims=True)
    r_ref[...] = jnp.broadcast_to(line, r_ref.shape)


def apply_layer(ids, xall, wall, bias):
    shards, rows, width = xall.shape
    side = wall.shape[4]
    hbm = pl.BlockSpec(memory_space=pl.ANY)
    vmem = pl.BlockSpec(memory_space=pltpu.VMEM)
    return pl.pallas_call(
        layer_kernel,
        out_shape=(
            jax.ShapeDtypeStruct((rows, width), xall.dtype),
            jax.ShapeDtypeStruct((8, rows), jnp.float32),
        ),
        in_specs=[pl.BlockSpec(memory_space=pltpu.SMEM), hbm, hbm, vmem],
        out_specs=(vmem, vmem),
        scratch_shapes=[
            pltpu.VMEM(xall.shape, xall.dtype),
            pltpu.VMEM(wall.shape, wall.dtype),
            pltpu.VMEM((rows, side), jnp.float32),
            pltpu.SemaphoreType.DMA((2, shards)),
        ],
        compiler_params=pltpu.CompilerParams(vmem_limit_bytes=52 * 1024 * 1024),
        name="layer",
    )(ids, xall, wall, bias)


def means_kernel(groups, shards, neurons, x_ref, rows_ref, all_ref, slots, ssem, rsem):
    bi = lax.axis_index("batch")
    mi = lax.axis_index("mp")
    me = bi * shards + mi
    total = groups * shards
    barrier = pltpu.get_barrier_semaphore()

    def peer(d):
        to = (me + d) % total
        return to // shards, to % shards

    @pl.loop(1, total)
    def _(d):
        pl.semaphore_signal(barrier, inc=1, device_id=peer(d), device_id_type=MESH)

    pl.semaphore_wait(barrier, total - 1)

    def copy(d, slot):
        return pltpu.make_async_remote_copy(
            src_ref=x_ref,
            dst_ref=slots.at[slot],
            send_sem=ssem.at[d],
            recv_sem=rsem.at[slot],
            device_id=peer(d),
            device_id_type=MESH,
        )

    @pl.loop(1, total)
    def _(d):
        copy(d, me).start()

    slots[me] = x_ref[...]

    @pl.loop(1, total)
    def _(d):
        copy(d, (me + d) % total).wait_recv()

    whole = jnp.zeros(all_ref.shape, jnp.float32)
    for b in range(groups):
        one = slots[b * shards]
        for m in range(1, shards):
            one = one + slots[b * shards + m]
        whole = whole + one / neurons
    all_ref[...] = whole
    mine = slots[bi * shards]
    for m in range(1, shards):
        mine = mine + slots[bi * shards + m]
    rows_ref[...] = mine / neurons

    @pl.loop(1, total)
    def _(d):
        copy(d, me).wait_send()


def means(groups, shards, neurons, sums):
    total = groups * shards
    if total > 64:
        shard_sum = lax.psum(sums[0], "mp") / neurons
        return shard_sum, lax.psum(shard_sum, "batch")
    vmem = pl.BlockSpec(memory_space=pltpu.VMEM)
    like = jax.ShapeDtypeStruct(sums.shape, jnp.float32)
    mine, whole = pl.pallas_call(
        functools.partial(means_kernel, groups, shards, neurons),
        out_shape=(like, like),
        in_specs=[vmem],
        out_specs=(vmem, vmem),
        scratch_shapes=[
            pltpu.VMEM((total,) + sums.shape, jnp.float32),
            pltpu.SemaphoreType.DMA((total,)),
            pltpu.SemaphoreType.DMA((total,)),
        ],
        compiler_params=pltpu.CompilerParams(collective_id=20, has_side_effects=True),
        name="means",
    )(sums)
    return mine[0], whole[0]


def fused_kernel(
    geo, pieces, neurons, total_rows,
    ids, feats, tiles, biases, out, rows_ref, grand_ref,
    wl, bl, xin, x2, x2g, st, fin, fing, sums, guests, line, slots,
    lsem, qsend, qrecv, bsem, up, dn, xs, wrecv, xrecv, rrecv,
    osend, okept, orecv, x2recv, fsem, gsend, msem,
):
    nl, nq, line_major, nc = geo
    layers, groups, shards, per, fan, _, side = wl.shape
    ny = shards // nc
    cb = per * shards
    n = per // pieces
    chunks = shards * pieces
    every = layers * chunks
    shared = chunks + pieces
    depth = nl
    bi = lax.axis_index("batch")
    mi = lax.axis_index("mp")
    if line_major:
        l, q = bi // nq, bi % nq
    else:
        l, q = bi % nl, bi // nl
    y, core = mi // nc, mi % nc
    side_q = (q + 1) % nq
    total = groups * shards
    me = bi * shards + mi
    edge = (l == 0) | (l == nl - 1)
    host = (l == 1) | (l == nl - 2)
    low = l < nl // 2

    def group(level, column):
        return level * nq + column if line_major else column * nl + level

    upper = group(jnp.minimum(l + 1, nl - 1), q)
    under = group(jnp.maximum(l - 1, 0), q)
    beside = group(l, side_q)
    hosted = group(jnp.where(low, 0, nl - 1), q)
    hosting = group(jnp.where(low, 1, nl - 2), q)

    def source(k):
        return ((y + k // nc) % ny) * nc + (core + k % nc) % nc

    def turn(layer, c):
        k = c // pieces
        return jnp.where(layer == layers - 1, shards - 1 - k, k)

    def spot(p):
        c = p % chunks
        return p // chunks, turn(p // chunks, c), c % pieces

    def peer(d):
        to = (me + d) % total
        return to // shards, to % shards

    def remote(src, dst, ssem, rsem, b, m):
        return pltpu.make_async_remote_copy(
            src_ref=src, dst_ref=dst, send_sem=ssem, recv_sem=rsem,
            device_id=(b, m), device_id_type=MESH,
        )

    def came(part, rsem):
        remote(part, part, msem.at[0], rsem, bi, mi).wait_recv()

    def left(part, ssem):
        remote(part, part, ssem, msem.at[1], bi, mi).wait_send()

    def own_quarter(layer):
        return pltpu.make_async_copy(
            tiles.at[layer, pl.ds(mi * per, per)], wl.at[layer, bi, mi], lsem.at[2 + layer]
        )

    for layer in range(layers):
        own_quarter(layer).start()
    mine_b = pl.ds(mi * per * side, per * side)
    in_b = pltpu.make_async_copy(biases.at[:, mine_b], bl.at[:, mine_b], lsem.at[1])
    in_b.start()

    barrier = pltpu.get_barrier_semaphore()

    def greet(b, m):
        pl.semaphore_signal(barrier, inc=1, device_id=(b, m), device_id_type=MESH)

    @pl.when(l > 0)
    def _():
        greet(under, mi)

    @pl.when(l < nl - 1)
    def _():
        greet(upper, mi)

    greet(beside, mi)
    for k in range(1, shards):
        greet(bi, source(k))

    @pl.loop(0, cb)
    def _(j):
        pltpu.make_async_copy(
            feats.at[:, pl.ds(j * side, side)], xin.at[j], lsem.at[0]
        ).start()

    near = jnp.where(l > 0, 1, 0) + jnp.where(l < nl - 1, 1, 0)
    pl.semaphore_wait(barrier, near + shards)

    def quarter(layer, k):
        to = source(k)
        return remote(
            tiles.at[layer, pl.ds(to * per, per)], wl.at[layer, bi, mi],
            qsend, qrecv.at[layer, mi], bi, to,
        )

    for k in range(1, shards):
        to = source(k)
        quarter(0, k).start()
        theirs = biases.at[:, pl.ds(to * per * side, per * side)]
        remote(theirs, bl.at[:, mine_b], bsem.at[0], bsem.at[1], bi, to).start()
    for layer in range(1, layers):
        for k in range(1, shards):
            quarter(layer, k).start()
    sums[...] = jnp.zeros_like(sums)
    guests[...] = jnp.zeros_like(guests)

    def piece(p, b):
        layer, k, g = spot(p)
        return wl.at[layer, b, source(k), pl.ds(g * n, n)]

    def inside(p):
        return p >= shared

    def top(p):
        return jnp.where(inside(p), nl - 2, nl - 1)

    def bottom(p):
        return jnp.where(inside(p), 1, 0)

    def relayed(p, level):
        outer = (level == 0) | (level == nl - 1)
        return (outer & inside(p)) | (jnp.logical_not(outer) & (p % 2 == 1))

    def go(cond, copy):
        @pl.when(cond)
        def _():
            copy.start()

    def along(p, b, level, e):
        part = piece(p, b)
        go(l < top(p), remote(part, part, up.at[e], wrecv.at[level, p], upper, mi))
        go(l > bottom(p), remote(part, part, dn.at[e], wrecv.at[level, p], under, mi))

    def flow(t):
        @pl.when(t < every)
        def _():
            layer, k, g = spot(t)

            @pl.when((g == 0) & (k == 0))
            def _():
                own_quarter(layer).wait()

            @pl.when((g == 0) & (k > 0))
            def _():
                m = source(k)
                came(wl.at[layer, bi, m], qrecv.at[layer, m])

            part = piece(t, bi)
            again = relayed(t, l)
            go(l < top(t), remote(part, part, up.at[0], wrecv.at[l, t], upper, mi))
            go(l > bottom(t), remote(part, part, dn.at[0], wrecv.at[l, t], under, mi))
            go(again, remote(part, part, xs.at[l], rrecv.at[t], beside, mi))
            go(jnp.logical_not(again), remote(part, part, xs.at[l], xrecv.at[t], beside, mi))

        for d in range(1, nl):
            p = t - d
            ok = (p >= 0) & (p < every)

            def step(p, level, onward, ssem, to):
                part = piece(p, group(level, q))
                came(part, wrecv.at[level, p])
                go(onward, remote(part, part, ssem, wrecv.at[level, p], to, mi))
                direct = jnp.logical_not((abs(level - l) == 1) & relayed(p, level))
                go(direct, remote(part, part, xs.at[level], xrecv.at[p], beside, mi))

            @pl.when(ok & (l - d >= 0) & (l <= top(p)))
            def _(d=d, p=p, step=step):
                step(p, jnp.maximum(l - d, 0), l < top(p), up.at[d], upper)

            @pl.when(ok & (l + d <= nl - 1) & (l >= bottom(p)))
            def _(d=d, p=p, step=step):
                step(p, jnp.minimum(l + d, nl - 1), l > bottom(p), dn.at[d], under)

            if d == 1:
                @pl.when(ok & relayed(p, l))
                def _(p=p):
                    part = piece(p, beside)
                    came(part, rrecv.at[p])
                    go(l < top(p), remote(part, part, up.at[nl], xrecv.at[p], upper, mi))
                    go(l > bottom(p), remote(part, part, dn.at[nl], xrecv.at[p], under, mi))

    def landing(p):
        layer, k, g = spot(p)
        early = relayed(p, l)

        def wait(count):
            came(wl.at[layer, pl.ds(0, count), source(k), pl.ds(g * n, n)], xrecv.at[p])

        @pl.when(early)
        def _():
            wait(nl - 1)

        @pl.when(jnp.logical_not(early))
        def _():
            wait(nl)

    def columns(m, g):
        return pl.ds((m * per + g * n) * side, n * side)

    def blocks(m, g):
        return pl.ds(m * per + g * n, n)

    def hand_on(p):
        c, k, g = p, turn(0, p), p % pieces
        first = p < chunks

        @pl.when(first & (k == 0))
        def _():
            pltpu.make_async_copy(
                st.at[0, pl.ds(g * n, n)], x2.at[blocks(mi, g)], okept.at[0]
            ).start()

        @pl.when(first & (k > 0))
        def _():
            remote(
                st.at[k, pl.ds(g * n, n)], x2.at[blocks(mi, g)],
                osend.at[0], x2recv.at[c], bi, source(k),
            ).start()

        @pl.when(jnp.logical_not(first))
        def _():
            k, g = turn(1, p - chunks), (p - chunks) % pieces
            here = jnp.logical_not(edge & inside(p))
            there = pl.ds(g * n * side, n * side)

            @pl.when(here & (k == 0))
            def _():
                pltpu.make_async_copy(
                    fin.at[0, :, there], out.at[:, columns(mi, g)], okept.at[1]
                ).start()

            @pl.when(here & (k > 0))
            def _():
                remote(
                    fin.at[k, :, there], out.at[:, columns(mi, g)],
                    osend.at[1], orecv, bi, source(k),
                ).start()

            @pl.when(host & inside(p))
            def _():
                remote(
                    fing.at[k, :, there], out.at[:, columns(mi, g)],
                    gsend, orecv, hosted, source(k),
                ).start()

    def pass_on(c):
        k, g = turn(0, c), c % pieces
        m = source(k)

        @pl.when(k == 0)
        def _():
            part = st.at[0, pl.ds(g * n, n)]
            go(edge, remote(part, x2g.at[blocks(mi, g)], fsem.at[0], fsem.at[1], hosting, mi))

        @pl.when(k > 0)
        def _():
            part = x2.at[blocks(m, g)]
            came(part, x2recv.at[c])
            go(edge, remote(part, x2g.at[blocks(m, g)], fsem.at[0], fsem.at[1], hosting, mi))

    def compute(layer, c, guest=False):
        k, g = turn(layer, c), c % pieces
        m = source(k)
        src = xin if layer == 0 else x2g if guest else x2
        for jj in range(n):
            j = g * n + jj
            column = m * cb + mi * per + j
            xparts, wparts = [], []
            for t in range(fan):
                at = lax.rem(ids[t, layer, column], cb)
                xparts.append(src[at])
                wparts.append(wl[layer, :, m, j, t].reshape(side, side))
            whole = jnp.dot(
                jnp.concatenate(xparts, axis=1),
                jnp.concatenate(wparts, axis=0),
                preferred_element_type=jnp.float32,
            )
            bias = bl[layer : layer + 1, pl.ds(pl.multiple_of((m * per + j) * side, side), side)]
            res = jnp.clip(whole + bias, 0.0, 32.0).astype(out.dtype)
            cols = pl.ds(pl.multiple_of(j * side, side), side)
            if layer == 0:
                st[k, j] = res
            elif guest:
                fing[k, :, cols] = res
                guests[...] += res.astype(jnp.float32)
            else:
                fin[k, :, cols] = res
                sums[...] += res.astype(jnp.float32)

    lag = 2

    @pl.loop(0, every + depth + 1)
    def _(t):
        flow(t)
        p = t - depth

        @pl.when(p >= 1)
        def _():
            hand_on(p - 1)

        @pl.when((p >= lag) & (p - lag < chunks - 1))
        def _():
            pass_on(p - lag)

        @pl.when(p == 0)
        def _():
            pltpu.make_async_copy(xin, xin, lsem.at[0]).wait()
            in_b.wait()
            came(bl.at[:, pl.ds(0, (shards - 1) * per * side)], bsem.at[1])

        @pl.when((p >= 0) & (p < chunks))
        def _():
            landing(p)
            compute(0, p)

        @pl.when(p == chunks)
        def _():
            pass_on(chunks - 1)
            pltpu.make_async_copy(st.at[0], st.at[0], okept.at[0]).wait()

        @pl.when((p == shared) & host)
        def _():
            came(x2g, fsem.at[1])

        @pl.when((p >= chunks) & (p < every) & jnp.logical_not(edge & inside(p)))
        def _():
            landing(p)

        @pl.when((p >= shared) & (p < every) & host)
        def _():
            compute(1, p - chunks, True)

        @pl.when((p >= chunks) & (p < every) & jnp.logical_not(edge & inside(p)))
        def _():
            compute(1, p - chunks)

    own_line = jnp.sum(sums[...].T, axis=0, keepdims=True)
    guest_line = jnp.sum(guests[...].T, axis=0, keepdims=True)
    at_row = lax.broadcasted_iota(jnp.int32, line.shape, 0)
    line[...] = jnp.where(at_row < line.shape[0] // 2, own_line, guest_line)

    def gone(halves, ssem):
        if halves % 2 == 0:
            left(wl.at[0, pl.ds(0, halves // 2), 0], ssem)
        else:
            left(wl.at[0, pl.ds(0, halves), 0, pl.ds(0, per // 2)], ssem)

    wide, narrow = 2 * (shards + 1), 2 * (shards - 1)
    full = wide + narrow
    for d in range(nl):
        @pl.when((l - d >= 0) & (l < nl - 2))
        def _(d=d):
            gone(full, up.at[d])

        @pl.when((l - d >= 0) & (l == nl - 2))
        def _(d=d):
            gone(wide, up.at[d])

        @pl.when((l + d <= nl - 1) & (l > 1))
        def _(d=d):
            gone(full, dn.at[d])

        @pl.when((l + d <= nl - 1) & (l == 1))
        def _(d=d):
            gone(wide, dn.at[d])

    @pl.when(l == 0)
    def _():
        gone(narrow, up.at[nl])

    @pl.when((l > 0) & (l < nl - 2))
    def _():
        gone(full // 2, up.at[nl])

    @pl.when(l == nl - 2)
    def _():
        gone(wide // 2, up.at[nl])

    @pl.when(l == nl - 1)
    def _():
        gone(narrow, dn.at[nl])

    @pl.when((l > 1) & (l < nl - 1))
    def _():
        gone(full // 2, dn.at[nl])

    @pl.when(l == 1)
    def _():
        gone(wide // 2, dn.at[nl])

    for level in range(nl):
        close = abs(l - level) == 1
        outer = level in (0, nl - 1)

        @pl.when(l == level)
        def _(level=level):
            gone(full, xs.at[level])

        @pl.when(edge & (l != level))
        def _(level=level, close=close):
            @pl.when(close)
            def _():
                gone(wide // 2, xs.at[level])

            @pl.when(jnp.logical_not(close))
            def _():
                gone(wide, xs.at[level])

        @pl.when(jnp.logical_not(edge) & (l != level))
        def _(level=level, close=close, outer=outer):
            @pl.when(close)
            def _():
                gone(wide if outer else full // 2, xs.at[level])

            @pl.when(jnp.logical_not(close))
            def _():
                gone(full, xs.at[level])

    left(wl.at[:, bi, pl.ds(0, shards - 1)], qsend)
    left(bl.at[:, pl.ds(0, (shards - 1) * per * side)], bsem.at[0])
    left(st.at[pl.ds(0, shards - 1)], osend.at[0])

    @pl.when(edge)
    def _():
        left(x2g, fsem.at[0])

    def mcopy(d, slot):
        return remote(line, slots.at[slot], msem.at[0], msem.at[1], *peer(d))

    @pl.loop(1, total)
    def _(d):
        mcopy(d, me).start()

    slots[me] = line[...]

    @pl.when(edge)
    def _():
        left(fin.at[0], osend.at[1])

    @pl.when(jnp.logical_not(edge))
    def _():
        left(fin.at[pl.ds(0, shards - 1)], osend.at[1])

    @pl.when(host)
    def _():
        left(fing, gsend)

    lines = slots.at[pl.ds(0, total - 1)]
    came(lines, msem.at[1])
    low_half = line.shape[0] // 2
    whole = jnp.zeros((1, line.shape[1]), jnp.float32)
    for b in range(groups):
        one = slots[b * shards]
        for m in range(1, shards):
            one = one + slots[b * shards + m]
        whole = whole + (one[0:1] + one[low_half : low_half + 1]) / neurons
    mine = slots[bi * shards]
    help_ = slots[hosting * shards]
    for m in range(1, shards):
        mine = mine + slots[bi * shards + m]
        help_ = help_ + slots[hosting * shards + m]
    extra = jnp.where(edge, help_[low_half : low_half + 1], 0.0)
    rows_ref[...] = (mine[0:1] + extra) / neurons
    grand_ref[0, 0] = jnp.sum(whole) / total_rows

    @pl.when(edge)
    def _():
        came(fin, orecv)

    @pl.when(jnp.logical_not(edge))
    def _():
        pltpu.make_async_copy(fin.at[0], fin.at[0], okept.at[1]).wait()
        came(fin.at[pl.ds(0, shards - 1)], orecv)

    left(lines, msem.at[0])


def fused(geo, pieces, features, tiles, biases, in_block):
    nl, nq, _, nc = geo
    shards = lax.axis_size("mp")
    groups = lax.axis_size("batch")
    layers, cb, fan, depth, side = tiles.shape
    rows, width = features.shape
    per = cb // shards
    chunks = shards * pieces
    every = layers * chunks
    total = groups * shards
    dma = pltpu.SemaphoreType.DMA
    hbm = pl.BlockSpec(memory_space=pltpu.HBM)
    vmem = pl.BlockSpec(memory_space=pltpu.VMEM)
    smem = pl.BlockSpec(memory_space=pltpu.SMEM)
    blocks = pltpu.VMEM((cb, rows, side), features.dtype)
    sums = pltpu.VMEM((rows, side), jnp.float32)
    acts, row_means, grand = pl.pallas_call(
        functools.partial(
            fused_kernel, geo, pieces, cb * side * shards, rows * groups
        ),
        out_shape=(
            jax.ShapeDtypeStruct((rows, width), features.dtype),
            jax.ShapeDtypeStruct((1, rows), jnp.float32),
            jax.ShapeDtypeStruct((1, 1), jnp.float32),
        ),
        in_specs=[smem, hbm, hbm, hbm],
        out_specs=(pl.BlockSpec(memory_space=pl.ANY), vmem, smem),
        scratch_shapes=[
            pltpu.VMEM((layers, groups, shards, per, fan, depth, side), tiles.dtype),
            pltpu.VMEM(biases.shape, biases.dtype),
            blocks,
            blocks,
            blocks,
            pltpu.VMEM((shards, per, rows, side), features.dtype),
            pltpu.VMEM((shards, rows, per * side), features.dtype),
            pltpu.VMEM((shards - 1, rows, per * side), features.dtype),
            sums,
            sums,
            pltpu.VMEM((8, rows), jnp.float32),
            pltpu.VMEM((total, 8, rows), jnp.float32),
            dma((2 + layers,)),
            dma(()),
            dma((layers, shards)),
            dma((2,)),
            dma((nl + 1,)),
            dma((nl + 1,)),
            dma((nl,)),
            dma((nl, every)),
            dma((every,)),
            dma((every,)),
            dma((2,)),
            dma((2,)),
            dma(()),
            dma((chunks,)),
            dma((2,)),
            dma(()),
            dma((2,)),
        ],
        compiler_params=pltpu.CompilerParams(
            collective_id=3,
            has_side_effects=True,
            vmem_limit_bytes=54 * 1024 * 1024,
        ),
        name="net",
    )(in_block.transpose(2, 0, 1), features, tiles, biases)
    return acts, row_means[0], grand[0, 0]


def suits(geo, shards, groups, features, tiles, biases):
    nl, nq, _, nc = geo
    kept = 6 * features.size + groups * tiles.size
    return (
        nq == 2
        and nl == 4
        and nc <= 2
        and shards == 2 * nc
        and groups >= 2 * shards
        and tiles.shape[0] == 2
        and tiles.shape[3] % 16 == 0
        and tiles.shape[1] // shards % PIECES == 0
        and 2 * kept < 54 * 1024 * 1024
    )


def on_device(geo, features, tiles, biases, in_block):
    shards = lax.axis_size("mp")
    groups = lax.axis_size("batch")
    me = lax.axis_index("mp")
    rows = features.shape[0]
    side = tiles.shape[4]
    cb = tiles.shape[1]
    fan = tiles.shape[2]
    if suits(geo, shards, groups, features, tiles, biases):
        return fused(geo, PIECES, features, tiles, biases, in_block)
    current = features
    mine = lax.dynamic_slice_in_dim(in_block, me * cb, cb, axis=1) % cb
    for layer in range(tiles.shape[0]):
        wall, xall = gather(geo, shards, groups, layer, tiles, current)
        current, sums = apply_layer(
            mine[layer].reshape(-1), xall, wall, biases[layer].reshape(1, -1)
        )
    row_means, whole = means(groups, shards, cb * side * shards, sums)
    grand = jnp.sum(whole) / (rows * groups)
    return (current, row_means, grand)


def solution(mesh):
    placed = (P("batch", "mp"), P(None, "mp", None, "batch", None), P(None, "mp"), P())
    return jax.shard_map(
        functools.partial(on_device, geometry(mesh)),
        mesh=mesh,
        in_specs=placed,
        out_specs=(P("batch", "mp"), P("batch"), P()),
        check_vma=False,
    )
```

```python
import functools
import math

import jax
import jax.numpy as jnp
from jax import lax
from jax.experimental import pallas as pl
from jax.experimental.pallas import tpu as pltpu
from jax.sharding import PartitionSpec as P

MESH = pl.DeviceIdType.MESH
PIECES = 4
KEPT = 2
FIRST = 2
LAG = 1
LATER = 0
SLACK = 2


def geometry(mesh):
    groups, shards = mesh.devices.shape
    where = [getattr(d, "coords", None) for d in mesh.devices[:, 0]]
    if groups == 1 or where[0] is None or where[0] == where[1]:
        return groups, 1, True, 1
    moved = [i for i in range(len(where[0])) if where[0][i] != where[1][i]][0]
    minor = 1
    while minor < groups and all(
        where[minor][i] == where[0][i] for i in range(len(where[0])) if i != moved
    ):
        minor += 1
    major = groups // minor
    row = [d.coords for d in mesh.devices[0, :]]
    cores = sum(1 for c in row if c == row[0])
    if major >= minor:
        return major, minor, True, cores
    return minor, major, False, cores


def gather_kernel(
    geo, shards, layer, pieces,
    tiles, cur, wout, xout,
    wv, xv, lsem, wrecv, wup, wdn, wcross, whalf, xrecv, xfar, xcore,
):
    nl, nq, line_major, nc = geo
    ny = shards // nc
    bi = lax.axis_index("batch")
    mi = lax.axis_index("mp")
    if line_major:
        l, q = bi // nq, bi % nq
    else:
        l, q = bi % nl, bi // nl
    y, core = mi // nc, mi % nc
    step_w = tiles.shape[1] // pieces
    step_x = cur.shape[0] // pieces
    halves = nq == 2 and nl % 2 == 0
    first = pieces // 2

    def group(level, side):
        return level * nq + side if line_major else side * nl + level

    sides = [(q + d) % nq for d in range(1, nq)]
    fars = [((y + d) % ny) * nc + core for d in range(1, ny)]
    partners = [y * nc + (core + d) % nc for d in range(1, nc)]

    barrier = pltpu.get_barrier_semaphore()

    def greet(b, m):
        pl.semaphore_signal(barrier, inc=1, device_id=(b, m), device_id_type=MESH)

    @pl.when(l > 0)
    def _():
        greet(group(l - 1, q), mi)

    @pl.when(l < nl - 1)
    def _():
        greet(group(l + 1, q), mi)

    for side in sides:
        greet(group(l, side), mi)
    for m in fars + partners:
        greet(bi, m)
    near = jnp.where(l > 0, 1, 0) + jnp.where(l < nl - 1, 1, 0)
    pl.semaphore_wait(barrier, len(sides) + len(fars) + len(partners) + near)

    in_w = pltpu.make_async_copy(tiles.at[layer], wv, lsem.at[0])
    in_x = pltpu.make_async_copy(cur, xv, lsem.at[1])
    in_w.start()
    in_x.start()

    def wcopy(own, b, c, to, ssem):
        part = pl.ds(c * step_w, step_w)
        return pltpu.make_async_remote_copy(
            src_ref=tiles.at[layer, part] if own else wout.at[b, part],
            dst_ref=wout.at[b, part],
            send_sem=ssem,
            recv_sem=wrecv.at[b, c],
            device_id=(to, mi),
            device_id_type=MESH,
        )

    def xcopy(own, m, c, to, ssem):
        part = pl.ds(c * step_x, step_x)
        return pltpu.make_async_remote_copy(
            src_ref=cur.at[part] if own else xout.at[m, part],
            dst_ref=xout.at[m, part],
            send_sem=ssem,
            recv_sem=xrecv.at[m, c],
            device_id=(bi, to),
            device_id_type=MESH,
        )

    def phase(p, c, drain):
        def go(copy):
            copy.wait_send() if drain else copy.start()

        def arrived_w(b):
            if not drain:
                wcopy(False, b, c, bi, wup.at[0, c]).wait_recv()

        if p == 0:
            @pl.when(l < nl - 1)
            def _():
                go(wcopy(True, bi, c, group(l + 1, q), wup.at[0, c]))

            @pl.when(l > 0)
            def _():
                go(wcopy(True, bi, c, group(l - 1, q), wdn.at[0, c]))

            for i, side in enumerate(sides):
                go(wcopy(True, bi, c, group(l, side), wcross.at[i, l, c]))
            for i, m in enumerate(fars):
                go(xcopy(True, mi, c, m, xfar.at[i, c]))
            for i, m in enumerate(partners):
                go(xcopy(True, mi, c, m, xcore.at[i, y, c]))
        else:
            @pl.when(l - p >= 0)
            def _():
                b = group(l - p, q)
                arrived_w(b)

                @pl.when(l < nl - 1)
                def _():
                    go(wcopy(False, b, c, group(l + 1, q), wup.at[p, c]))

                def across():
                    for i, side in enumerate(sides):
                        go(wcopy(False, b, c, group(l, side), wcross.at[i, l - p, c]))

                if halves and p == 1:
                    pl.when((l < nl // 2) | (c < first))(across)
                else:
                    across()

            @pl.when(l + p <= nl - 1)
            def _():
                b = group(l + p, q)
                arrived_w(b)

                @pl.when(l > 0)
                def _():
                    go(wcopy(False, b, c, group(l - 1, q), wdn.at[p, c]))

                def across():
                    for i, side in enumerate(sides):
                        go(wcopy(False, b, c, group(l, side), wcross.at[i, l + p, c]))

                if halves and p == 1:
                    pl.when((l >= nl // 2) | (c < first))(across)
                else:
                    across()

            if halves and p == 1:
                @pl.when(c >= first)
                def _():
                    b = group(l, sides[0])
                    arrived_w(b)

                    @pl.when((l + 1 >= nl // 2) & (l < nl - 1))
                    def _():
                        go(wcopy(False, b, c, group(l + 1, q), whalf.at[0, c]))

                    @pl.when((l - 1 < nl // 2) & (l > 0))
                    def _():
                        go(wcopy(False, b, c, group(l - 1, q), whalf.at[1, c]))

        if p == nl - 1:
            for d, far in enumerate(fars):
                if not drain:
                    xcopy(False, far, c, mi, xfar.at[0, c]).wait_recv()
                for i, m in enumerate(partners):
                    go(xcopy(False, far, c, m, xcore.at[i, far // nc, c]))

    for p in range(nl):
        @pl.loop(0, pieces)
        def _(c, p=p):
            phase(p, c, False)

        if p == 0:
            in_w.wait()
            in_x.wait()
            out_w = pltpu.make_async_copy(wv, wout.at[bi], lsem.at[2])
            out_x = pltpu.make_async_copy(xv, xout.at[mi], lsem.at[3])
            out_w.start()
            out_x.start()

    @pl.loop(0, pieces)
    def _(c):
        for side in sides:
            for level in range(nl):
                b = group(level, side)

                def arrive(b=b):
                    wcopy(False, b, c, bi, wup.at[0, c]).wait_recv()

                if halves:
                    pl.when((l != level) | (c < first))(arrive)
                else:
                    arrive()
        for m in partners:
            for yy in range(ny):
                xcopy(False, yy * nc + m % nc, c, mi, xfar.at[0, c]).wait_recv()

    out_w.wait()
    out_x.wait()
    for p in range(nl):
        @pl.loop(0, pieces)
        def _(c, p=p):
            phase(p, c, True)


def gather(geo, shards, groups, layer, tiles, cur):
    nl, nq, _, nc = geo
    pieces = 8 if groups <= 8 else 2
    ny = shards // nc
    dma = pltpu.SemaphoreType.DMA
    return pl.pallas_call(
        functools.partial(gather_kernel, geo, shards, layer, pieces),
        out_shape=(
            jax.ShapeDtypeStruct((groups,) + tiles.shape[1:], tiles.dtype),
            jax.ShapeDtypeStruct((shards,) + cur.shape, cur.dtype),
        ),
        in_specs=[pl.BlockSpec(memory_space=pl.ANY)] * 2,
        out_specs=(pl.BlockSpec(memory_space=pl.ANY),) * 2,
        scratch_shapes=[
            pltpu.VMEM(tiles.shape[1:], tiles.dtype),
            pltpu.VMEM(cur.shape, cur.dtype),
            dma((4,)),
            dma((groups, pieces)),
            dma((nl, pieces)),
            dma((nl, pieces)),
            dma((max(nq - 1, 1), nl, pieces)),
            dma((2, pieces)),
            dma((shards, pieces)),
            dma((max(ny - 1, 1), pieces)),
            dma((max(nc - 1, 1), ny, pieces)),
        ],
        compiler_params=pltpu.CompilerParams(collective_id=layer, has_side_effects=True),
        name=f"gather_{layer}",
    )(tiles, cur)


def layer_kernel(ids, x_ref, w_ref, b_ref, o_ref, r_ref, xl, wl, s_ref, loads):
    shards, rows, _ = x_ref.shape
    _, cb, fan, _, side = w_ref.shape
    per_shard = cb // shards
    width = math.gcd(per_shard, 8)

    def pulls(s):
        part = pl.ds(s * per_shard, per_shard)
        return (
            pltpu.make_async_copy(x_ref.at[s], xl.at[s], loads.at[0, s]),
            pltpu.make_async_copy(w_ref.at[:, part], wl.at[:, part], loads.at[1, s]),
        )

    for s in range(min(2, shards)):
        for pull in pulls(s):
            pull.start()
    s_ref[...] = jnp.zeros_like(s_ref)
    for s in range(shards):
        for pull in pulls(s):
            pull.wait()
        if s + 2 < shards:
            for pull in pulls(s + 2):
                pull.start()

        @pl.loop(0, per_shard // width)
        def _(k, s=s):
            for jj in range(width):
                j = s * per_shard + k * width + jj
                xs, ws = [], []
                for t in range(fan):
                    at = ids[j * fan + t]
                    xs.append(xl[s, :, pl.ds(pl.multiple_of(at * side, side), side)])
                    ws.append(wl[:, j, t].reshape(side, side))
                total = jnp.dot(
                    jnp.concatenate(xs, axis=1),
                    jnp.concatenate(ws, axis=0),
                    preferred_element_type=jnp.float32,
                )
                cols = pl.ds(pl.multiple_of(j * side, side), side)
                out = jnp.clip(total + b_ref[:, cols], 0.0, 32.0).astype(o_ref.dtype)
                o_ref[:, cols] = out
                s_ref[...] += out.astype(jnp.float32)

    line = jnp.sum(s_ref[...].T, axis=0, keepdims=True)
    r_ref[...] = jnp.broadcast_to(line, r_ref.shape)


def apply_layer(ids, xall, wall, bias):
    shards, rows, width = xall.shape
    side = wall.shape[4]
    hbm = pl.BlockSpec(memory_space=pl.ANY)
    vmem = pl.BlockSpec(memory_space=pltpu.VMEM)
    return pl.pallas_call(
        layer_kernel,
        out_shape=(
            jax.ShapeDtypeStruct((rows, width), xall.dtype),
            jax.ShapeDtypeStruct((8, rows), jnp.float32),
        ),
        in_specs=[pl.BlockSpec(memory_space=pltpu.SMEM), hbm, hbm, vmem],
        out_specs=(vmem, vmem),
        scratch_shapes=[
            pltpu.VMEM(xall.shape, xall.dtype),
            pltpu.VMEM(wall.shape, wall.dtype),
            pltpu.VMEM((rows, side), jnp.float32),
            pltpu.SemaphoreType.DMA((2, shards)),
        ],
        compiler_params=pltpu.CompilerParams(vmem_limit_bytes=52 * 1024 * 1024),
        name="layer",
    )(ids, xall, wall, bias)


def means_kernel(groups, shards, neurons, x_ref, rows_ref, all_ref, slots, ssem, rsem):
    bi = lax.axis_index("batch")
    mi = lax.axis_index("mp")
    me = bi * shards + mi
    total = groups * shards
    barrier = pltpu.get_barrier_semaphore()

    def peer(d):
        to = (me + d) % total
        return to // shards, to % shards

    @pl.loop(1, total)
    def _(d):
        pl.semaphore_signal(barrier, inc=1, device_id=peer(d), device_id_type=MESH)

    pl.semaphore_wait(barrier, total - 1)

    def copy(d, slot):
        return pltpu.make_async_remote_copy(
            src_ref=x_ref,
            dst_ref=slots.at[slot],
            send_sem=ssem.at[d],
            recv_sem=rsem.at[slot],
            device_id=peer(d),
            device_id_type=MESH,
        )

    @pl.loop(1, total)
    def _(d):
        copy(d, me).start()

    slots[me] = x_ref[...]

    @pl.loop(1, total)
    def _(d):
        copy(d, (me + d) % total).wait_recv()

    whole = jnp.zeros(all_ref.shape, jnp.float32)
    for b in range(groups):
        one = slots[b * shards]
        for m in range(1, shards):
            one = one + slots[b * shards + m]
        whole = whole + one / neurons
    all_ref[...] = whole
    mine = slots[bi * shards]
    for m in range(1, shards):
        mine = mine + slots[bi * shards + m]
    rows_ref[...] = mine / neurons

    @pl.loop(1, total)
    def _(d):
        copy(d, me).wait_send()


def means(groups, shards, neurons, sums):
    total = groups * shards
    if total > 64:
        shard_sum = lax.psum(sums[0], "mp") / neurons
        return shard_sum, lax.psum(shard_sum, "batch")
    vmem = pl.BlockSpec(memory_space=pltpu.VMEM)
    like = jax.ShapeDtypeStruct(sums.shape, jnp.float32)
    mine, whole = pl.pallas_call(
        functools.partial(means_kernel, groups, shards, neurons),
        out_shape=(like, like),
        in_specs=[vmem],
        out_specs=(vmem, vmem),
        scratch_shapes=[
            pltpu.VMEM((total,) + sums.shape, jnp.float32),
            pltpu.SemaphoreType.DMA((total,)),
            pltpu.SemaphoreType.DMA((total,)),
        ],
        compiler_params=pltpu.CompilerParams(collective_id=20, has_side_effects=True),
        name="means",
    )(sums)
    return mine[0], whole[0]


def fused_kernel(
    geo, pieces, neurons, total_rows,
    ids, feats, tiles, biases, out, rows_ref, grand_ref,
    wl, bl, xin, x2, x2g, st, fin, fing, sums, guests, line, slots,
    lsem, qsend, qrecv, bsem, up, dn, xs, wrecv, xrecv, rrecv,
    osend, okept, orecv, x2recv, fsem, gsend, msem,
):
    nl, nq, line_major, nc = geo
    layers, groups, shards, per, fan, _, side = wl.shape
    ny = shards // nc
    cb = per * shards
    n = per // pieces
    chunks = shards * pieces
    every = layers * chunks
    depth = nl
    edge_own = KEPT * pieces
    bi = lax.axis_index("batch")
    mi = lax.axis_index("mp")
    if line_major:
        l, q = bi // nq, bi % nq
    else:
        l, q = bi % nl, bi // nl
    y, core = mi // nc, mi % nc
    side_q = (q + 1) % nq
    total = groups * shards
    me = bi * shards + mi
    edge = (l == 0) | (l == nl - 1)
    host = (l == 1) | (l == nl - 2)
    low = l < nl // 2

    def group(level, column):
        return level * nq + column if line_major else column * nl + level

    upper = group(jnp.minimum(l + 1, nl - 1), q)
    under = group(jnp.maximum(l - 1, 0), q)
    beside = group(l, side_q)
    hosted = group(jnp.where(low, 0, nl - 1), q)
    hosting = group(jnp.where(low, 1, nl - 2), q)

    def source(k):
        return ((y + k // nc) % ny) * nc + (core + k % nc) % nc

    def turn(layer, c):
        k = c // pieces
        return (shards - k) % shards if layer == 0 else shards - 1 - k

    def place(p):
        r = p - chunks
        v = r - FIRST
        mixed = jnp.where(v % 2 == 1, FIRST + v // 2, edge_own + v // 2)
        later = jnp.where(v < 2 * (edge_own - FIRST), mixed, r)
        second = jnp.where(r < FIRST, r, later)
        return jnp.where(r >= 0, 1, 0), jnp.where(r >= 0, second, p)

    def spot(p):
        layer, c = place(p)
        return layer, jnp.where(layer == 0, turn(0, c), turn(1, c)), c % pieces

    def peer(d):
        to = (me + d) % total
        return to // shards, to % shards

    def remote(src, dst, ssem, rsem, b, m):
        return pltpu.make_async_remote_copy(
            src_ref=src, dst_ref=dst, send_sem=ssem, recv_sem=rsem,
            device_id=(b, m), device_id_type=MESH,
        )

    def came(part, rsem):
        remote(part, part, msem.at[0], rsem, bi, mi).wait_recv()

    def left(part, ssem):
        remote(part, part, ssem, msem.at[1], bi, mi).wait_send()

    def own_quarter(layer):
        return pltpu.make_async_copy(
            tiles.at[layer, pl.ds(mi * per, per)], wl.at[layer, bi, mi], lsem.at[2 + layer]
        )

    for layer in range(layers):
        own_quarter(layer).start()
    mine_b = pl.ds(mi * per * side, per * side)
    in_b = pltpu.make_async_copy(biases.at[:, mine_b], bl.at[:, mine_b], lsem.at[1])
    in_b.start()

    barrier = pltpu.get_barrier_semaphore()

    def greet(b, m):
        pl.semaphore_signal(barrier, inc=1, device_id=(b, m), device_id_type=MESH)

    @pl.when(l > 0)
    def _():
        greet(under, mi)

    @pl.when(l < nl - 1)
    def _():
        greet(upper, mi)

    greet(beside, mi)
    for k in range(1, shards):
        greet(bi, source(k))

    @pl.loop(0, cb)
    def _(j):
        pltpu.make_async_copy(
            feats.at[:, pl.ds(j * side, side)], xin.at[j], lsem.at[0]
        ).start()

    near = jnp.where(l > 0, 1, 0) + jnp.where(l < nl - 1, 1, 0)
    pl.semaphore_wait(barrier, near + shards)

    def quarter(layer, k):
        to = source(k)
        return remote(
            tiles.at[layer, pl.ds(to * per, per)], wl.at[layer, bi, mi],
            qsend, qrecv.at[layer, mi], bi, to,
        )

    for k in range(1, shards):
        to = source(k)
        quarter(0, k).start()
        theirs = biases.at[:, pl.ds(to * per * side, per * side)]
        remote(theirs, bl.at[:, mine_b], bsem.at[0], bsem.at[1], bi, to).start()
    for layer in range(1, layers):
        for k in range(1, shards):
            quarter(layer, k).start()
    sums[...] = jnp.zeros_like(sums)
    guests[...] = jnp.zeros_like(guests)

    def piece(p, b):
        layer, k, g = spot(p)
        return wl.at[layer, b, source(k), pl.ds(g * n, n)]

    def inside(p):
        layer, c = place(p)
        return (layer == 1) & (c >= edge_own)

    def top(p):
        return jnp.where(inside(p), nl - 2, nl - 1)

    def bottom(p):
        return jnp.where(inside(p), 1, 0)

    def relayed(p, level):
        outer = (level == 0) | (level == nl - 1)
        return jnp.where(outer, p >= chunks, place(p)[1] % 2 == 1)

    def carried(p, level, to):
        outer = (to == 0) | (to == nl - 1)
        across = (abs(level - to) == 1) & relayed(p, level)
        return across & jnp.logical_not(outer & (p >= chunks))

    def go(cond, copy):
        @pl.when(cond)
        def _():
            copy.start()

    def along(p, b, level, e):
        part = piece(p, b)
        go(l < top(p), remote(part, part, up.at[e], wrecv.at[level, p], upper, mi))
        go(l > bottom(p), remote(part, part, dn.at[e], wrecv.at[level, p], under, mi))

    def due(t, d):
        one, two = t - d, t - d - SLACK
        ok = ((one >= 0) & (one < chunks)) | ((two >= chunks) & (two < every))
        return jnp.where(one < chunks, one, two), ok

    def flow(t):
        def quarter_here(p):
            layer, k, g = spot(p)

            @pl.when((g == 0) & (k == 0))
            def _():
                own_quarter(layer).wait()

            @pl.when((g == 0) & (k > 0))
            def _():
                m = source(k)
                came(wl.at[layer, bi, m], qrecv.at[layer, m])

        def own(p, cond):
            part = piece(p, bi)
            go(cond & (l < top(p)), remote(part, part, up.at[0], wrecv.at[l, p], upper, mi))
            go(cond & (l > bottom(p)), remote(part, part, dn.at[0], wrecv.at[l, p], under, mi))

        hurried = pieces + 2 * (t - pieces)

        @pl.when((t < pieces) | ((t >= chunks) & (t < every)))
        def _():
            quarter_here(t)
            own(t, True)

        @pl.when((t >= pieces) & (hurried < chunks))
        def _():
            quarter_here(hurried)
            own(hurried, edge)
            own(hurried + 1, edge)

        @pl.when((t >= pieces) & (t < chunks))
        def _():
            own(t, jnp.logical_not(edge))

        @pl.when(t < every)
        def _():
            part = piece(t, bi)
            again = relayed(t, l)
            go(again, remote(part, part, xs.at[l], rrecv.at[t], beside, mi))
            go(jnp.logical_not(again), remote(part, part, xs.at[l], xrecv.at[t], beside, mi))

        for d in range(1, nl):
            p, ok = due(t, d)

            def step(p, level, onward, ssem, to):
                part = piece(p, group(level, q))
                came(part, wrecv.at[level, p])
                go(onward, remote(part, part, ssem, wrecv.at[level, p], to, mi))
                direct = jnp.logical_not(carried(p, level, l))
                go(direct, remote(part, part, xs.at[level], xrecv.at[p], beside, mi))

            @pl.when(ok & (l - d >= 0) & (l <= top(p)))
            def _(d=d, p=p, step=step):
                step(p, jnp.maximum(l - d, 0), l < top(p), up.at[d], upper)

            @pl.when(ok & (l + d <= nl - 1) & (l >= bottom(p)))
            def _(d=d, p=p, step=step):
                step(p, jnp.minimum(l + d, nl - 1), l > bottom(p), dn.at[d], under)

            if d == 1:
                @pl.when(ok & relayed(p, l))
                def _(p=p):
                    part = piece(p, beside)
                    came(part, rrecv.at[p])
                    more = (l < top(p)) & carried(p, l, l + 1)
                    go(more, remote(part, part, up.at[nl], xrecv.at[p], upper, mi))
                    more = (l > bottom(p)) & carried(p, l, l - 1)
                    go(more, remote(part, part, dn.at[nl], xrecv.at[p], under, mi))

    def landing(p):
        layer, k, g = spot(p)
        early = relayed(p, l)

        def wait(count):
            came(wl.at[layer, pl.ds(0, count), source(k), pl.ds(g * n, n)], xrecv.at[p])

        @pl.when(early)
        def _():
            wait(nl - 1)

        @pl.when(jnp.logical_not(early))
        def _():
            wait(nl)

    def columns(m, g):
        return pl.ds((m * per + g * n) * side, n * side)

    def blocks(m, g):
        return pl.ds(m * per + g * n, n)

    def hand_on(p):
        layer, c = place(p)
        g = c % pieces

        @pl.when(layer == 0)
        def _():
            k = turn(0, c)
            part = pl.ds(g * n, n)

            @pl.when(k == 0)
            def _():
                pltpu.make_async_copy(
                    st.at[0, part], x2.at[blocks(mi, g)], okept.at[0]
                ).start()

            @pl.when(k > 0)
            def _():
                remote(
                    st.at[k, part], x2.at[blocks(mi, g)],
                    osend.at[0], x2recv.at[c], bi, source(k),
                ).start()

        @pl.when((layer == 1) & jnp.logical_not(edge & inside(p)))
        def _():
            k = turn(1, c)
            part = pl.ds(g * n * side, n * side)

            @pl.when(k == 0)
            def _():
                pltpu.make_async_copy(
                    fin.at[0, :, part], out.at[:, columns(mi, g)], okept.at[1]
                ).start()

            @pl.when(k > 0)
            def _():
                remote(
                    fin.at[k, :, part], out.at[:, columns(mi, g)],
                    osend.at[1], orecv, bi, source(k),
                ).start()

    def give_back(p):
        _, c = place(p)
        k, g = turn(1, c), c % pieces
        remote(
            fing.at[k, :, pl.ds(g * n * side, n * side)], out.at[:, columns(mi, g)],
            gsend, orecv, hosted, source(k),
        ).start()

    def pass_on(c):
        k, g = turn(0, c), c % pieces
        m = source(k)

        @pl.when(k == 0)
        def _():
            part = st.at[0, pl.ds(g * n, n)]
            go(edge, remote(part, x2g.at[blocks(mi, g)], fsem.at[0], fsem.at[1], hosting, mi))

        @pl.when(k > 0)
        def _():
            part = x2.at[blocks(m, g)]
            came(part, x2recv.at[c])
            go(edge, remote(part, x2g.at[blocks(m, g)], fsem.at[0], fsem.at[1], hosting, mi))

    def compute(layer, c, guest=False):
        k, g = turn(layer, c), c % pieces
        m = source(k)
        src = xin if layer == 0 else x2g if guest else x2
        for jj in range(n):
            j = g * n + jj
            column = m * cb + mi * per + j
            xparts, wparts = [], []
            for t in range(fan):
                at = lax.rem(ids[t, layer, column], cb)
                xparts.append(src[at])
                wparts.append(wl[layer, :, m, j, t].reshape(side, side))
            whole = jnp.dot(
                jnp.concatenate(xparts, axis=1),
                jnp.concatenate(wparts, axis=0),
                preferred_element_type=jnp.float32,
            )
            bias = bl[layer : layer + 1, pl.ds(pl.multiple_of((m * per + j) * side, side), side)]
            res = jnp.clip(whole + bias, 0.0, 32.0).astype(out.dtype)
            cols = pl.ds(pl.multiple_of(j * side, side), side)
            if layer == 0:
                st[k, j] = res
            elif guest:
                fing[k, :, cols] = res
                guests[...] += res.astype(jnp.float32)
            else:
                fin[k, :, cols] = res
                sums[...] += res.astype(jnp.float32)

    @pl.loop(0, every + depth + SLACK + LATER + 1)
    def _(t):
        flow(t)
        p = t - depth
        r = p - SLACK
        h = r - LATER

        @pl.when((p >= 1) & (p <= chunks))
        def _():
            hand_on(p - 1)

        @pl.when((r > chunks) & (r <= every))
        def _():
            hand_on(r - 1)

        @pl.when(host & (h > chunks))
        def _():
            pl.when(inside(h - 1))(lambda: give_back(h - 1))

        @pl.when((p >= LAG) & (p - LAG < chunks))
        def _():
            pass_on(p - LAG)

        @pl.when(p == 0)
        def _():
            pltpu.make_async_copy(xin, xin, lsem.at[0]).wait()
            in_b.wait()
            came(bl.at[:, pl.ds(0, (shards - 1) * per * side)], bsem.at[1])

        @pl.when((p >= 0) & (p < chunks))
        def _():
            landing(p)
            compute(0, p)

        @pl.when(r == chunks)
        def _():
            pltpu.make_async_copy(st.at[0], st.at[0], okept.at[0]).wait()

        needed = (r >= chunks) & (r < every) & jnp.logical_not(edge & inside(r))

        @pl.when(needed)
        def _():
            landing(r)

        @pl.when(host & (h == chunks + FIRST))
        def _():
            came(x2g, fsem.at[1])

        @pl.when(host & (h >= chunks) & (h < every))
        def _():
            pl.when(inside(h))(lambda: compute(1, place(h)[1], True))

        @pl.when(needed)
        def _():
            compute(1, place(r)[1])

    own_line = jnp.sum(sums[...].T, axis=0, keepdims=True)
    guest_line = jnp.sum(guests[...].T, axis=0, keepdims=True)
    at_row = lax.broadcasted_iota(jnp.int32, line.shape, 0)
    line[...] = jnp.where(at_row < line.shape[0] // 2, own_line, guest_line)

    def gone(halves, ssem):
        if halves % 2 == 0:
            left(wl.at[0, pl.ds(0, halves // 2), 0], ssem)
        else:
            left(wl.at[0, pl.ds(0, halves), 0, pl.ds(0, per // 2)], ssem)

    wide, narrow = 2 * (shards + KEPT), 2 * (shards - KEPT)
    full = wide + narrow
    for d in range(nl):
        @pl.when((l - d >= 0) & (l < nl - 2))
        def _(d=d):
            gone(full, up.at[d])

        @pl.when((l - d >= 0) & (l == nl - 2))
        def _(d=d):
            gone(wide, up.at[d])

        @pl.when((l + d <= nl - 1) & (l > 1))
        def _(d=d):
            gone(full, dn.at[d])

        @pl.when((l + d <= nl - 1) & (l == 1))
        def _(d=d):
            gone(wide, dn.at[d])

    @pl.when(l == 0)
    def _():
        gone(full // 2, up.at[nl])

    @pl.when((l > 0) & (l < nl - 2))
    def _():
        gone(full // 2, up.at[nl])

    @pl.when(l == nl - 2)
    def _():
        gone(shards, up.at[nl])

    @pl.when(l == nl - 1)
    def _():
        gone(full // 2, dn.at[nl])

    @pl.when((l > 1) & (l < nl - 1))
    def _():
        gone(full // 2, dn.at[nl])

    @pl.when(l == 1)
    def _():
        gone(shards, dn.at[nl])

    for level in range(nl):
        close = abs(l - level) == 1
        outer = level in (0, nl - 1)

        @pl.when(l == level)
        def _(level=level):
            gone(full, xs.at[level])

        @pl.when(edge & (l != level))
        def _(level=level, close=close):
            @pl.when(close)
            def _():
                gone(wide - shards, xs.at[level])

            @pl.when(jnp.logical_not(close))
            def _():
                gone(wide, xs.at[level])

        @pl.when(jnp.logical_not(edge) & (l != level))
        def _(level=level, close=close, outer=outer):
            @pl.when(close)
            def _():
                gone(full // 2, xs.at[level])

            @pl.when(jnp.logical_not(close))
            def _():
                gone(full, xs.at[level])

    left(wl.at[:, bi, pl.ds(0, shards - 1)], qsend)
    left(bl.at[:, pl.ds(0, (shards - 1) * per * side)], bsem.at[0])
    left(st.at[pl.ds(0, shards - 1)], osend.at[0])

    @pl.when(edge)
    def _():
        left(x2g, fsem.at[0])

    def mcopy(d, slot):
        return remote(line, slots.at[slot], msem.at[0], msem.at[1], *peer(d))

    @pl.loop(1, total)
    def _(d):
        mcopy(d, me).start()

    slots[me] = line[...]

    @pl.when(edge)
    def _():
        left(fin.at[pl.ds(0, KEPT)], osend.at[1])

    @pl.when(jnp.logical_not(edge))
    def _():
        left(fin.at[pl.ds(0, shards - 1)], osend.at[1])

    @pl.when(host)
    def _():
        left(fing, gsend)

    lines = slots.at[pl.ds(0, total - 1)]
    came(lines, msem.at[1])
    low_half = line.shape[0] // 2
    whole = jnp.zeros((1, line.shape[1]), jnp.float32)
    for b in range(groups):
        one = slots[b * shards]
        for m in range(1, shards):
            one = one + slots[b * shards + m]
        whole = whole + (one[0:1] + one[low_half : low_half + 1]) / neurons
    mine = slots[bi * shards]
    help_ = slots[hosting * shards]
    for m in range(1, shards):
        mine = mine + slots[bi * shards + m]
        help_ = help_ + slots[hosting * shards + m]
    extra = jnp.where(edge, help_[low_half : low_half + 1], 0.0)
    rows_ref[...] = (mine[0:1] + extra) / neurons
    grand_ref[0, 0] = jnp.sum(whole) / total_rows

    @pl.when(edge)
    def _():
        came(fin, orecv)

    @pl.when(jnp.logical_not(edge))
    def _():
        pltpu.make_async_copy(fin.at[0], fin.at[0], okept.at[1]).wait()
        came(fin.at[pl.ds(0, shards - 1)], orecv)

    left(lines, msem.at[0])


def fused(geo, pieces, features, tiles, biases, in_block):
    nl, nq, _, nc = geo
    shards = lax.axis_size("mp")
    groups = lax.axis_size("batch")
    layers, cb, fan, depth, side = tiles.shape
    rows, width = features.shape
    per = cb // shards
    chunks = shards * pieces
    every = layers * chunks
    total = groups * shards
    dma = pltpu.SemaphoreType.DMA
    hbm = pl.BlockSpec(memory_space=pltpu.HBM)
    vmem = pl.BlockSpec(memory_space=pltpu.VMEM)
    smem = pl.BlockSpec(memory_space=pltpu.SMEM)
    blocks = pltpu.VMEM((cb, rows, side), features.dtype)
    sums = pltpu.VMEM((rows, side), jnp.float32)
    acts, row_means, grand = pl.pallas_call(
        functools.partial(
            fused_kernel, geo, pieces, cb * side * shards, rows * groups
        ),
        out_shape=(
            jax.ShapeDtypeStruct((rows, width), features.dtype),
            jax.ShapeDtypeStruct((1, rows), jnp.float32),
            jax.ShapeDtypeStruct((1, 1), jnp.float32),
        ),
        in_specs=[smem, hbm, hbm, hbm],
        out_specs=(pl.BlockSpec(memory_space=pl.ANY), vmem, smem),
        scratch_shapes=[
            pltpu.VMEM((layers, groups, shards, per, fan, depth, side), tiles.dtype),
            pltpu.VMEM(biases.shape, biases.dtype),
            blocks,
            blocks,
            blocks,
            pltpu.VMEM((shards, per, rows, side), features.dtype),
            pltpu.VMEM((shards, rows, per * side), features.dtype),
            pltpu.VMEM((shards - KEPT, rows, per * side), features.dtype),
            sums,
            sums,
            pltpu.VMEM((8, rows), jnp.float32),
            pltpu.VMEM((total, 8, rows), jnp.float32),
            dma((2 + layers,)),
            dma(()),
            dma((layers, shards)),
            dma((2,)),
            dma((nl + 1,)),
            dma((nl + 1,)),
            dma((nl,)),
            dma((nl, every)),
            dma((every,)),
            dma((every,)),
            dma((2,)),
            dma((2,)),
            dma(()),
            dma((chunks,)),
            dma((2,)),
            dma(()),
            dma((2,)),
        ],
        compiler_params=pltpu.CompilerParams(
            collective_id=3,
            has_side_effects=True,
            vmem_limit_bytes=54 * 1024 * 1024,
        ),
        name="net",
    )(in_block.transpose(2, 0, 1), features, tiles, biases)
    return acts, row_means[0], grand[0, 0]


def suits(geo, shards, groups, features, tiles, biases):
    nl, nq, _, nc = geo
    kept = 6 * features.size + groups * tiles.size
    return (
        nq == 2
        and nl == 4
        and nc <= 2
        and shards == 2 * nc
        and groups >= 2 * shards
        and tiles.shape[0] == 2
        and tiles.shape[3] % 16 == 0
        and tiles.shape[1] // shards % PIECES == 0
        and 2 * kept < 54 * 1024 * 1024
    )


def on_device(geo, features, tiles, biases, in_block):
    shards = lax.axis_size("mp")
    groups = lax.axis_size("batch")
    me = lax.axis_index("mp")
    rows = features.shape[0]
    side = tiles.shape[4]
    cb = tiles.shape[1]
    fan = tiles.shape[2]
    if suits(geo, shards, groups, features, tiles, biases):
        return fused(geo, PIECES, features, tiles, biases, in_block)
    current = features
    mine = lax.dynamic_slice_in_dim(in_block, me * cb, cb, axis=1) % cb
    for layer in range(tiles.shape[0]):
        wall, xall = gather(geo, shards, groups, layer, tiles, current)
        current, sums = apply_layer(
            mine[layer].reshape(-1), xall, wall, biases[layer].reshape(1, -1)
        )
    row_means, whole = means(groups, shards, cb * side * shards, sums)
    grand = jnp.sum(whole) / (rows * groups)
    return (current, row_means, grand)


def solution(mesh):
    placed = (P("batch", "mp"), P(None, "mp", None, "batch", None), P(None, "mp"), P())
    return jax.shard_map(
        functools.partial(on_device, geometry(mesh)),
        mesh=mesh,
        in_specs=placed,
        out_specs=(P("batch", "mp"), P("batch"), P()),
        check_vma=False,
    )
```

```python
import functools
import math

import jax
import jax.numpy as jnp
from jax import lax
from jax.experimental import pallas as pl
from jax.experimental.pallas import tpu as pltpu
from jax.sharding import PartitionSpec as P

MESH = pl.DeviceIdType.MESH
PIECES = 4
KEPT = 2
FIRST = 3
LAG = 2
LATER = 0
SLACK = 2


def geometry(mesh):
    groups, shards = mesh.devices.shape
    where = [getattr(d, "coords", None) for d in mesh.devices[:, 0]]
    if groups == 1 or where[0] is None or where[0] == where[1]:
        return groups, 1, True, 1
    moved = [i for i in range(len(where[0])) if where[0][i] != where[1][i]][0]
    minor = 1
    while minor < groups and all(
        where[minor][i] == where[0][i] for i in range(len(where[0])) if i != moved
    ):
        minor += 1
    major = groups // minor
    row = [d.coords for d in mesh.devices[0, :]]
    cores = sum(1 for c in row if c == row[0])
    if major >= minor:
        return major, minor, True, cores
    return minor, major, False, cores


def gather_kernel(
    geo, shards, layer, pieces,
    tiles, cur, wout, xout,
    wv, xv, lsem, wrecv, wup, wdn, wcross, whalf, xrecv, xfar, xcore,
):
    nl, nq, line_major, nc = geo
    ny = shards // nc
    bi = lax.axis_index("batch")
    mi = lax.axis_index("mp")
    if line_major:
        l, q = bi // nq, bi % nq
    else:
        l, q = bi % nl, bi // nl
    y, core = mi // nc, mi % nc
    step_w = tiles.shape[1] // pieces
    step_x = cur.shape[0] // pieces
    halves = nq == 2 and nl % 2 == 0
    first = pieces // 2

    def group(level, side):
        return level * nq + side if line_major else side * nl + level

    sides = [(q + d) % nq for d in range(1, nq)]
    fars = [((y + d) % ny) * nc + core for d in range(1, ny)]
    partners = [y * nc + (core + d) % nc for d in range(1, nc)]

    barrier = pltpu.get_barrier_semaphore()

    def greet(b, m):
        pl.semaphore_signal(barrier, inc=1, device_id=(b, m), device_id_type=MESH)

    @pl.when(l > 0)
    def _():
        greet(group(l - 1, q), mi)

    @pl.when(l < nl - 1)
    def _():
        greet(group(l + 1, q), mi)

    for side in sides:
        greet(group(l, side), mi)
    for m in fars + partners:
        greet(bi, m)
    near = jnp.where(l > 0, 1, 0) + jnp.where(l < nl - 1, 1, 0)
    pl.semaphore_wait(barrier, len(sides) + len(fars) + len(partners) + near)

    in_w = pltpu.make_async_copy(tiles.at[layer], wv, lsem.at[0])
    in_x = pltpu.make_async_copy(cur, xv, lsem.at[1])
    in_w.start()
    in_x.start()

    def wcopy(own, b, c, to, ssem):
        part = pl.ds(c * step_w, step_w)
        return pltpu.make_async_remote_copy(
            src_ref=tiles.at[layer, part] if own else wout.at[b, part],
            dst_ref=wout.at[b, part],
            send_sem=ssem,
            recv_sem=wrecv.at[b, c],
            device_id=(to, mi),
            device_id_type=MESH,
        )

    def xcopy(own, m, c, to, ssem):
        part = pl.ds(c * step_x, step_x)
        return pltpu.make_async_remote_copy(
            src_ref=cur.at[part] if own else xout.at[m, part],
            dst_ref=xout.at[m, part],
            send_sem=ssem,
            recv_sem=xrecv.at[m, c],
            device_id=(bi, to),
            device_id_type=MESH,
        )

    def phase(p, c, drain):
        def go(copy):
            copy.wait_send() if drain else copy.start()

        def arrived_w(b):
            if not drain:
                wcopy(False, b, c, bi, wup.at[0, c]).wait_recv()

        if p == 0:
            @pl.when(l < nl - 1)
            def _():
                go(wcopy(True, bi, c, group(l + 1, q), wup.at[0, c]))

            @pl.when(l > 0)
            def _():
                go(wcopy(True, bi, c, group(l - 1, q), wdn.at[0, c]))

            for i, side in enumerate(sides):
                go(wcopy(True, bi, c, group(l, side), wcross.at[i, l, c]))
            for i, m in enumerate(fars):
                go(xcopy(True, mi, c, m, xfar.at[i, c]))
            for i, m in enumerate(partners):
                go(xcopy(True, mi, c, m, xcore.at[i, y, c]))
        else:
            @pl.when(l - p >= 0)
            def _():
                b = group(l - p, q)
                arrived_w(b)

                @pl.when(l < nl - 1)
                def _():
                    go(wcopy(False, b, c, group(l + 1, q), wup.at[p, c]))

                def across():
                    for i, side in enumerate(sides):
                        go(wcopy(False, b, c, group(l, side), wcross.at[i, l - p, c]))

                if halves and p == 1:
                    pl.when((l < nl // 2) | (c < first))(across)
                else:
                    across()

            @pl.when(l + p <= nl - 1)
            def _():
                b = group(l + p, q)
                arrived_w(b)

                @pl.when(l > 0)
                def _():
                    go(wcopy(False, b, c, group(l - 1, q), wdn.at[p, c]))

                def across():
                    for i, side in enumerate(sides):
                        go(wcopy(False, b, c, group(l, side), wcross.at[i, l + p, c]))

                if halves and p == 1:
                    pl.when((l >= nl // 2) | (c < first))(across)
                else:
                    across()

            if halves and p == 1:
                @pl.when(c >= first)
                def _():
                    b = group(l, sides[0])
                    arrived_w(b)

                    @pl.when((l + 1 >= nl // 2) & (l < nl - 1))
                    def _():
                        go(wcopy(False, b, c, group(l + 1, q), whalf.at[0, c]))

                    @pl.when((l - 1 < nl // 2) & (l > 0))
                    def _():
                        go(wcopy(False, b, c, group(l - 1, q), whalf.at[1, c]))

        if p == nl - 1:
            for d, far in enumerate(fars):
                if not drain:
                    xcopy(False, far, c, mi, xfar.at[0, c]).wait_recv()
                for i, m in enumerate(partners):
                    go(xcopy(False, far, c, m, xcore.at[i, far // nc, c]))

    for p in range(nl):
        @pl.loop(0, pieces)
        def _(c, p=p):
            phase(p, c, False)

        if p == 0:
            in_w.wait()
            in_x.wait()
            out_w = pltpu.make_async_copy(wv, wout.at[bi], lsem.at[2])
            out_x = pltpu.make_async_copy(xv, xout.at[mi], lsem.at[3])
            out_w.start()
            out_x.start()

    @pl.loop(0, pieces)
    def _(c):
        for side in sides:
            for level in range(nl):
                b = group(level, side)

                def arrive(b=b):
                    wcopy(False, b, c, bi, wup.at[0, c]).wait_recv()

                if halves:
                    pl.when((l != level) | (c < first))(arrive)
                else:
                    arrive()
        for m in partners:
            for yy in range(ny):
                xcopy(False, yy * nc + m % nc, c, mi, xfar.at[0, c]).wait_recv()

    out_w.wait()
    out_x.wait()
    for p in range(nl):
        @pl.loop(0, pieces)
        def _(c, p=p):
            phase(p, c, True)


def gather(geo, shards, groups, layer, tiles, cur):
    nl, nq, _, nc = geo
    pieces = 8 if groups <= 8 else 2
    ny = shards // nc
    dma = pltpu.SemaphoreType.DMA
    return pl.pallas_call(
        functools.partial(gather_kernel, geo, shards, layer, pieces),
        out_shape=(
            jax.ShapeDtypeStruct((groups,) + tiles.shape[1:], tiles.dtype),
            jax.ShapeDtypeStruct((shards,) + cur.shape, cur.dtype),
        ),
        in_specs=[pl.BlockSpec(memory_space=pl.ANY)] * 2,
        out_specs=(pl.BlockSpec(memory_space=pl.ANY),) * 2,
        scratch_shapes=[
            pltpu.VMEM(tiles.shape[1:], tiles.dtype),
            pltpu.VMEM(cur.shape, cur.dtype),
            dma((4,)),
            dma((groups, pieces)),
            dma((nl, pieces)),
            dma((nl, pieces)),
            dma((max(nq - 1, 1), nl, pieces)),
            dma((2, pieces)),
            dma((shards, pieces)),
            dma((max(ny - 1, 1), pieces)),
            dma((max(nc - 1, 1), ny, pieces)),
        ],
        compiler_params=pltpu.CompilerParams(collective_id=layer, has_side_effects=True),
        name=f"gather_{layer}",
    )(tiles, cur)


def layer_kernel(ids, x_ref, w_ref, b_ref, o_ref, r_ref, xl, wl, s_ref, loads):
    shards, rows, _ = x_ref.shape
    _, cb, fan, _, side = w_ref.shape
    per_shard = cb // shards
    width = math.gcd(per_shard, 8)

    def pulls(s):
        part = pl.ds(s * per_shard, per_shard)
        return (
            pltpu.make_async_copy(x_ref.at[s], xl.at[s], loads.at[0, s]),
            pltpu.make_async_copy(w_ref.at[:, part], wl.at[:, part], loads.at[1, s]),
        )

    for s in range(min(2, shards)):
        for pull in pulls(s):
            pull.start()
    s_ref[...] = jnp.zeros_like(s_ref)
    for s in range(shards):
        for pull in pulls(s):
            pull.wait()
        if s + 2 < shards:
            for pull in pulls(s + 2):
                pull.start()

        @pl.loop(0, per_shard // width)
        def _(k, s=s):
            for jj in range(width):
                j = s * per_shard + k * width + jj
                xs, ws = [], []
                for t in range(fan):
                    at = ids[j * fan + t]
                    xs.append(xl[s, :, pl.ds(pl.multiple_of(at * side, side), side)])
                    ws.append(wl[:, j, t].reshape(side, side))
                total = jnp.dot(
                    jnp.concatenate(xs, axis=1),
                    jnp.concatenate(ws, axis=0),
                    preferred_element_type=jnp.float32,
                )
                cols = pl.ds(pl.multiple_of(j * side, side), side)
                out = jnp.clip(total + b_ref[:, cols], 0.0, 32.0).astype(o_ref.dtype)
                o_ref[:, cols] = out
                s_ref[...] += out.astype(jnp.float32)

    line = jnp.sum(s_ref[...].T, axis=0, keepdims=True)
    r_ref[...] = jnp.broadcast_to(line, r_ref.shape)


def apply_layer(ids, xall, wall, bias):
    shards, rows, width = xall.shape
    side = wall.shape[4]
    hbm = pl.BlockSpec(memory_space=pl.ANY)
    vmem = pl.BlockSpec(memory_space=pltpu.VMEM)
    return pl.pallas_call(
        layer_kernel,
        out_shape=(
            jax.ShapeDtypeStruct((rows, width), xall.dtype),
            jax.ShapeDtypeStruct((8, rows), jnp.float32),
        ),
        in_specs=[pl.BlockSpec(memory_space=pltpu.SMEM), hbm, hbm, vmem],
        out_specs=(vmem, vmem),
        scratch_shapes=[
            pltpu.VMEM(xall.shape, xall.dtype),
            pltpu.VMEM(wall.shape, wall.dtype),
            pltpu.VMEM((rows, side), jnp.float32),
            pltpu.SemaphoreType.DMA((2, shards)),
        ],
        compiler_params=pltpu.CompilerParams(vmem_limit_bytes=52 * 1024 * 1024),
        name="layer",
    )(ids, xall, wall, bias)


def means_kernel(groups, shards, neurons, x_ref, rows_ref, all_ref, slots, ssem, rsem):
    bi = lax.axis_index("batch")
    mi = lax.axis_index("mp")
    me = bi * shards + mi
    total = groups * shards
    barrier = pltpu.get_barrier_semaphore()

    def peer(d):
        to = (me + d) % total
        return to // shards, to % shards

    @pl.loop(1, total)
    def _(d):
        pl.semaphore_signal(barrier, inc=1, device_id=peer(d), device_id_type=MESH)

    pl.semaphore_wait(barrier, total - 1)

    def copy(d, slot):
        return pltpu.make_async_remote_copy(
            src_ref=x_ref,
            dst_ref=slots.at[slot],
            send_sem=ssem.at[d],
            recv_sem=rsem.at[slot],
            device_id=peer(d),
            device_id_type=MESH,
        )

    @pl.loop(1, total)
    def _(d):
        copy(d, me).start()

    slots[me] = x_ref[...]

    @pl.loop(1, total)
    def _(d):
        copy(d, (me + d) % total).wait_recv()

    whole = jnp.zeros(all_ref.shape, jnp.float32)
    for b in range(groups):
        one = slots[b * shards]
        for m in range(1, shards):
            one = one + slots[b * shards + m]
        whole = whole + one / neurons
    all_ref[...] = whole
    mine = slots[bi * shards]
    for m in range(1, shards):
        mine = mine + slots[bi * shards + m]
    rows_ref[...] = mine / neurons

    @pl.loop(1, total)
    def _(d):
        copy(d, me).wait_send()


def means(groups, shards, neurons, sums):
    total = groups * shards
    if total > 64:
        shard_sum = lax.psum(sums[0], "mp") / neurons
        return shard_sum, lax.psum(shard_sum, "batch")
    vmem = pl.BlockSpec(memory_space=pltpu.VMEM)
    like = jax.ShapeDtypeStruct(sums.shape, jnp.float32)
    mine, whole = pl.pallas_call(
        functools.partial(means_kernel, groups, shards, neurons),
        out_shape=(like, like),
        in_specs=[vmem],
        out_specs=(vmem, vmem),
        scratch_shapes=[
            pltpu.VMEM((total,) + sums.shape, jnp.float32),
            pltpu.SemaphoreType.DMA((total,)),
            pltpu.SemaphoreType.DMA((total,)),
        ],
        compiler_params=pltpu.CompilerParams(collective_id=20, has_side_effects=True),
        name="means",
    )(sums)
    return mine[0], whole[0]


def fused_kernel(
    geo, pieces, neurons, total_rows,
    ids, feats, tiles, biases, out, rows_ref, grand_ref,
    wl, bl, xin, x2, x2g, st, fin, fing, sums, guests, line, slots,
    lsem, qsend, qrecv, bsem, up, dn, xs, wrecv, xrecv, rrecv,
    osend, okept, orecv, x2recv, fsem, gsend, msem,
):
    nl, nq, line_major, nc = geo
    layers, groups, shards, per, fan, _, side = wl.shape
    ny = shards // nc
    cb = per * shards
    n = per // pieces
    chunks = shards * pieces
    every = layers * chunks
    depth = nl
    edge_own = KEPT * pieces
    bi = lax.axis_index("batch")
    mi = lax.axis_index("mp")
    if line_major:
        l, q = bi // nq, bi % nq
    else:
        l, q = bi % nl, bi // nl
    y, core = mi // nc, mi % nc
    side_q = (q + 1) % nq
    total = groups * shards
    me = bi * shards + mi
    edge = (l == 0) | (l == nl - 1)
    host = (l == 1) | (l == nl - 2)
    low = l < nl // 2

    def group(level, column):
        return level * nq + column if line_major else column * nl + level

    upper = group(jnp.minimum(l + 1, nl - 1), q)
    under = group(jnp.maximum(l - 1, 0), q)
    beside = group(l, side_q)
    hosted = group(jnp.where(low, 0, nl - 1), q)
    hosting = group(jnp.where(low, 1, nl - 2), q)

    def source(k):
        return ((y + k // nc) % ny) * nc + (core + k % nc) % nc

    def turn(layer, c):
        k = c // pieces
        return (shards - k) % shards if layer == 0 else shards - 1 - k

    def place(p):
        r = p - chunks
        v = r - FIRST
        mixed = jnp.where(v % 2 == 1, FIRST + v // 2, edge_own + v // 2)
        later = jnp.where(v < 2 * (edge_own - FIRST), mixed, r)
        second = jnp.where(r < FIRST, r, later)
        return jnp.where(r >= 0, 1, 0), jnp.where(r >= 0, second, p)

    def spot(p):
        layer, c = place(p)
        return layer, jnp.where(layer == 0, turn(0, c), turn(1, c)), c % pieces

    def peer(d):
        to = (me + d) % total
        return to // shards, to % shards

    def remote(src, dst, ssem, rsem, b, m):
        return pltpu.make_async_remote_copy(
            src_ref=src, dst_ref=dst, send_sem=ssem, recv_sem=rsem,
            device_id=(b, m), device_id_type=MESH,
        )

    def came(part, rsem):
        remote(part, part, msem.at[0], rsem, bi, mi).wait_recv()

    def left(part, ssem):
        remote(part, part, ssem, msem.at[1], bi, mi).wait_send()

    def own_quarter(layer):
        return pltpu.make_async_copy(
            tiles.at[layer, pl.ds(mi * per, per)], wl.at[layer, bi, mi], lsem.at[2 + layer]
        )

    for layer in range(layers):
        own_quarter(layer).start()
    mine_b = pl.ds(mi * per * side, per * side)
    in_b = pltpu.make_async_copy(biases.at[:, mine_b], bl.at[:, mine_b], lsem.at[1])
    in_b.start()

    barrier = pltpu.get_barrier_semaphore()

    def greet(b, m):
        pl.semaphore_signal(barrier, inc=1, device_id=(b, m), device_id_type=MESH)

    @pl.when(l > 0)
    def _():
        greet(under, mi)

    @pl.when(l < nl - 1)
    def _():
        greet(upper, mi)

    greet(beside, mi)
    for k in range(1, shards):
        greet(bi, source(k))

    @pl.loop(0, cb)
    def _(j):
        pltpu.make_async_copy(
            feats.at[:, pl.ds(j * side, side)], xin.at[j], lsem.at[0]
        ).start()

    near = jnp.where(l > 0, 1, 0) + jnp.where(l < nl - 1, 1, 0)
    pl.semaphore_wait(barrier, near + shards)

    def quarter(layer, k):
        to = source(k)
        return remote(
            tiles.at[layer, pl.ds(to * per, per)], wl.at[layer, bi, mi],
            qsend, qrecv.at[layer, mi], bi, to,
        )

    for k in range(1, shards):
        to = source(k)
        quarter(0, k).start()
        theirs = biases.at[:, pl.ds(to * per * side, per * side)]
        remote(theirs, bl.at[:, mine_b], bsem.at[0], bsem.at[1], bi, to).start()
    for layer in range(1, layers):
        for k in range(1, shards):
            quarter(layer, k).start()
    sums[...] = jnp.zeros_like(sums)
    guests[...] = jnp.zeros_like(guests)

    def piece(p, b):
        layer, k, g = spot(p)
        return wl.at[layer, b, source(k), pl.ds(g * n, n)]

    def inside(p):
        layer, c = place(p)
        return (layer == 1) & (c >= edge_own)

    def top(p):
        return jnp.where(inside(p), nl - 2, nl - 1)

    def bottom(p):
        return jnp.where(inside(p), 1, 0)

    def relayed(p, level):
        outer = (level == 0) | (level == nl - 1)
        return jnp.where(outer, p >= chunks, place(p)[1] % 2 == 1)

    def carried(p, level, to):
        outer = (to == 0) | (to == nl - 1)
        across = (abs(level - to) == 1) & relayed(p, level)
        return across & jnp.logical_not(outer & (p >= chunks))

    def go(cond, copy):
        @pl.when(cond)
        def _():
            copy.start()

    def along(p, b, level, e):
        part = piece(p, b)
        go(l < top(p), remote(part, part, up.at[e], wrecv.at[level, p], upper, mi))
        go(l > bottom(p), remote(part, part, dn.at[e], wrecv.at[level, p], under, mi))

    def due(t, d):
        one, two = t - d, t - d - SLACK
        ok = ((one >= 0) & (one < chunks)) | ((two >= chunks) & (two < every))
        return jnp.where(one < chunks, one, two), ok

    def flow(t):
        def quarter_here(p):
            layer, k, g = spot(p)

            @pl.when((g == 0) & (k == 0))
            def _():
                own_quarter(layer).wait()

            @pl.when((g == 0) & (k > 0))
            def _():
                m = source(k)
                came(wl.at[layer, bi, m], qrecv.at[layer, m])

        def own(p, cond):
            part = piece(p, bi)
            go(cond & (l < top(p)), remote(part, part, up.at[0], wrecv.at[l, p], upper, mi))
            go(cond & (l > bottom(p)), remote(part, part, dn.at[0], wrecv.at[l, p], under, mi))

        hurried = pieces + 2 * (t - pieces)

        @pl.when((t < pieces) | ((t >= chunks) & (t < every)))
        def _():
            quarter_here(t)
            own(t, True)

        @pl.when((t >= pieces) & (hurried < chunks))
        def _():
            quarter_here(hurried)
            own(hurried, edge)
            own(hurried + 1, edge)

        @pl.when((t >= pieces) & (t < chunks))
        def _():
            own(t, jnp.logical_not(edge))

        @pl.when(t < every)
        def _():
            part = piece(t, bi)
            again = relayed(t, l)
            go(again, remote(part, part, xs.at[l], rrecv.at[t], beside, mi))
            go(jnp.logical_not(again), remote(part, part, xs.at[l], xrecv.at[t], beside, mi))

    def steps(t):
        for d in range(1, nl):
            p, ok = due(t, d)

            def step(p, level, onward, ssem, to):
                part = piece(p, group(level, q))
                came(part, wrecv.at[level, p])
                go(onward, remote(part, part, ssem, wrecv.at[level, p], to, mi))
                direct = jnp.logical_not(carried(p, level, l))
                go(direct, remote(part, part, xs.at[level], xrecv.at[p], beside, mi))

            @pl.when(ok & (l - d >= 0) & (l <= top(p)))
            def _(d=d, p=p, step=step):
                step(p, jnp.maximum(l - d, 0), l < top(p), up.at[d], upper)

            @pl.when(ok & (l + d <= nl - 1) & (l >= bottom(p)))
            def _(d=d, p=p, step=step):
                step(p, jnp.minimum(l + d, nl - 1), l > bottom(p), dn.at[d], under)

            if d == 1:
                @pl.when(ok & relayed(p, l))
                def _(p=p):
                    part = piece(p, beside)
                    came(part, rrecv.at[p])
                    more = (l < top(p)) & carried(p, l, l + 1)
                    go(more, remote(part, part, up.at[nl], xrecv.at[p], upper, mi))
                    more = (l > bottom(p)) & carried(p, l, l - 1)
                    go(more, remote(part, part, dn.at[nl], xrecv.at[p], under, mi))

    def landing(p):
        layer, k, g = spot(p)
        early = relayed(p, l)

        def wait(count):
            came(wl.at[layer, pl.ds(0, count), source(k), pl.ds(g * n, n)], xrecv.at[p])

        @pl.when(early)
        def _():
            wait(nl - 1)

        @pl.when(jnp.logical_not(early))
        def _():
            wait(nl)

    def columns(m, g):
        return pl.ds((m * per + g * n) * side, n * side)

    def blocks(m, g):
        return pl.ds(m * per + g * n, n)

    def hand_on(p):
        layer, c = place(p)
        g = c % pieces

        @pl.when(layer == 0)
        def _():
            k = turn(0, c)
            part = pl.ds(g * n, n)

            @pl.when(k == 0)
            def _():
                pltpu.make_async_copy(
                    st.at[0, part], x2.at[blocks(mi, g)], okept.at[0]
                ).start()

            @pl.when(k > 0)
            def _():
                remote(
                    st.at[k, part], x2.at[blocks(mi, g)],
                    osend.at[0], x2recv.at[c], bi, source(k),
                ).start()

        @pl.when((layer == 1) & jnp.logical_not(edge & inside(p)))
        def _():
            k = turn(1, c)
            part = pl.ds(g * n * side, n * side)

            @pl.when(k == 0)
            def _():
                pltpu.make_async_copy(
                    fin.at[0, :, part], out.at[:, columns(mi, g)], okept.at[1]
                ).start()

            @pl.when(k > 0)
            def _():
                remote(
                    fin.at[k, :, part], out.at[:, columns(mi, g)],
                    osend.at[1], orecv, bi, source(k),
                ).start()

    def give_back(p):
        _, c = place(p)
        k, g = turn(1, c), c % pieces
        remote(
            fing.at[k, :, pl.ds(g * n * side, n * side)], out.at[:, columns(mi, g)],
            gsend, orecv, hosted, source(k),
        ).start()

    def pass_on(c):
        k, g = turn(0, c), c % pieces
        m = source(k)

        @pl.when(k == 0)
        def _():
            part = st.at[0, pl.ds(g * n, n)]
            go(edge, remote(part, x2g.at[blocks(mi, g)], fsem.at[0], fsem.at[1], hosting, mi))

        @pl.when(k > 0)
        def _():
            part = x2.at[blocks(m, g)]
            came(part, x2recv.at[c])
            go(edge, remote(part, x2g.at[blocks(m, g)], fsem.at[0], fsem.at[1], hosting, mi))

    def compute(layer, c, guest=False):
        k, g = turn(layer, c), c % pieces
        m = source(k)
        src = xin if layer == 0 else x2g if guest else x2
        for jj in range(n):
            j = g * n + jj
            column = m * cb + mi * per + j
            xparts, wparts = [], []
            for t in range(fan):
                at = lax.rem(ids[t, layer, column], cb)
                xparts.append(src[at])
                wparts.append(wl[layer, :, m, j, t].reshape(side, side))
            whole = jnp.dot(
                jnp.concatenate(xparts, axis=1),
                jnp.concatenate(wparts, axis=0),
                preferred_element_type=jnp.float32,
            )
            bias = bl[layer : layer + 1, pl.ds(pl.multiple_of((m * per + j) * side, side), side)]
            res = jnp.clip(whole + bias, 0.0, 32.0).astype(out.dtype)
            cols = pl.ds(pl.multiple_of(j * side, side), side)
            if layer == 0:
                st[k, j] = res
            elif guest:
                fing[k, :, cols] = res
                guests[...] += res.astype(jnp.float32)
            else:
                fin[k, :, cols] = res
                sums[...] += res.astype(jnp.float32)

    @pl.loop(0, every + depth + SLACK + LATER + 1)
    def _(t):
        flow(t)
        p = t - depth
        r = p - SLACK
        h = r - LATER

        @pl.when((p >= 1) & (p <= chunks))
        def _():
            hand_on(p - 1)

        @pl.when((r > chunks) & (r <= every))
        def _():
            hand_on(r - 1)

        @pl.when(host & (h > chunks))
        def _():
            pl.when(inside(h - 1))(lambda: give_back(h - 1))

        @pl.when((p >= LAG) & (p - LAG < chunks))
        def _():
            pass_on(p - LAG)

        steps(t)

        @pl.when(p == 0)
        def _():
            pltpu.make_async_copy(xin, xin, lsem.at[0]).wait()
            in_b.wait()
            came(bl.at[:, pl.ds(0, (shards - 1) * per * side)], bsem.at[1])

        @pl.when((p >= 0) & (p < chunks))
        def _():
            landing(p)
            compute(0, p)

        @pl.when(r == chunks)
        def _():
            pltpu.make_async_copy(st.at[0], st.at[0], okept.at[0]).wait()

        needed = (r >= chunks) & (r < every) & jnp.logical_not(edge & inside(r))

        @pl.when(needed)
        def _():
            landing(r)

        @pl.when(host & (h == chunks + FIRST))
        def _():
            came(x2g, fsem.at[1])

        @pl.when(host & (h >= chunks) & (h < every))
        def _():
            pl.when(inside(h))(lambda: compute(1, place(h)[1], True))

        @pl.when(needed)
        def _():
            compute(1, place(r)[1])

    own_line = jnp.sum(sums[...].T, axis=0, keepdims=True)
    guest_line = jnp.sum(guests[...].T, axis=0, keepdims=True)
    at_row = lax.broadcasted_iota(jnp.int32, line.shape, 0)
    line[...] = jnp.where(at_row < line.shape[0] // 2, own_line, guest_line)

    def gone(halves, ssem):
        if halves % 2 == 0:
            left(wl.at[0, pl.ds(0, halves // 2), 0], ssem)
        else:
            left(wl.at[0, pl.ds(0, halves), 0, pl.ds(0, per // 2)], ssem)

    wide, narrow = 2 * (shards + KEPT), 2 * (shards - KEPT)
    full = wide + narrow
    for d in range(nl):
        @pl.when((l - d >= 0) & (l < nl - 2))
        def _(d=d):
            gone(full, up.at[d])

        @pl.when((l - d >= 0) & (l == nl - 2))
        def _(d=d):
            gone(wide, up.at[d])

        @pl.when((l + d <= nl - 1) & (l > 1))
        def _(d=d):
            gone(full, dn.at[d])

        @pl.when((l + d <= nl - 1) & (l == 1))
        def _(d=d):
            gone(wide, dn.at[d])

    @pl.when(l == 0)
    def _():
        gone(full // 2, up.at[nl])

    @pl.when((l > 0) & (l < nl - 2))
    def _():
        gone(full // 2, up.at[nl])

    @pl.when(l == nl - 2)
    def _():
        gone(shards, up.at[nl])

    @pl.when(l == nl - 1)
    def _():
        gone(full // 2, dn.at[nl])

    @pl.when((l > 1) & (l < nl - 1))
    def _():
        gone(full // 2, dn.at[nl])

    @pl.when(l == 1)
    def _():
        gone(shards, dn.at[nl])

    for level in range(nl):
        close = abs(l - level) == 1
        outer = level in (0, nl - 1)

        @pl.when(l == level)
        def _(level=level):
            gone(full, xs.at[level])

        @pl.when(edge & (l != level))
        def _(level=level, close=close):
            @pl.when(close)
            def _():
                gone(wide - shards, xs.at[level])

            @pl.when(jnp.logical_not(close))
            def _():
                gone(wide, xs.at[level])

        @pl.when(jnp.logical_not(edge) & (l != level))
        def _(level=level, close=close, outer=outer):
            @pl.when(close)
            def _():
                gone(full // 2, xs.at[level])

            @pl.when(jnp.logical_not(close))
            def _():
                gone(full, xs.at[level])

    left(wl.at[:, bi, pl.ds(0, shards - 1)], qsend)
    left(bl.at[:, pl.ds(0, (shards - 1) * per * side)], bsem.at[0])
    left(st.at[pl.ds(0, shards - 1)], osend.at[0])

    @pl.when(edge)
    def _():
        left(x2g, fsem.at[0])

    def mcopy(d, slot):
        return remote(line, slots.at[slot], msem.at[0], msem.at[1], *peer(d))

    @pl.loop(1, total)
    def _(d):
        mcopy(d, me).start()

    slots[me] = line[...]

    @pl.when(edge)
    def _():
        left(fin.at[pl.ds(0, KEPT)], osend.at[1])

    @pl.when(jnp.logical_not(edge))
    def _():
        left(fin.at[pl.ds(0, shards - 1)], osend.at[1])

    @pl.when(host)
    def _():
        left(fing, gsend)

    lines = slots.at[pl.ds(0, total - 1)]
    came(lines, msem.at[1])
    low_half = line.shape[0] // 2
    whole = jnp.zeros((1, line.shape[1]), jnp.float32)
    for b in range(groups):
        one = slots[b * shards]
        for m in range(1, shards):
            one = one + slots[b * shards + m]
        whole = whole + (one[0:1] + one[low_half : low_half + 1]) / neurons
    mine = slots[bi * shards]
    help_ = slots[hosting * shards]
    for m in range(1, shards):
        mine = mine + slots[bi * shards + m]
        help_ = help_ + slots[hosting * shards + m]
    extra = jnp.where(edge, help_[low_half : low_half + 1], 0.0)
    rows_ref[...] = (mine[0:1] + extra) / neurons
    grand_ref[0, 0] = jnp.sum(whole) / total_rows

    @pl.when(edge)
    def _():
        came(fin, orecv)

    @pl.when(jnp.logical_not(edge))
    def _():
        pltpu.make_async_copy(fin.at[0], fin.at[0], okept.at[1]).wait()
        came(fin.at[pl.ds(0, shards - 1)], orecv)

    left(lines, msem.at[0])


def fused(geo, pieces, features, tiles, biases, in_block):
    nl, nq, _, nc = geo
    shards = lax.axis_size("mp")
    groups = lax.axis_size("batch")
    layers, cb, fan, depth, side = tiles.shape
    rows, width = features.shape
    per = cb // shards
    chunks = shards * pieces
    every = layers * chunks
    total = groups * shards
    dma = pltpu.SemaphoreType.DMA
    hbm = pl.BlockSpec(memory_space=pltpu.HBM)
    vmem = pl.BlockSpec(memory_space=pltpu.VMEM)
    smem = pl.BlockSpec(memory_space=pltpu.SMEM)
    blocks = pltpu.VMEM((cb, rows, side), features.dtype)
    sums = pltpu.VMEM((rows, side), jnp.float32)
    acts, row_means, grand = pl.pallas_call(
        functools.partial(
            fused_kernel, geo, pieces, cb * side * shards, rows * groups
        ),
        out_shape=(
            jax.ShapeDtypeStruct((rows, width), features.dtype),
            jax.ShapeDtypeStruct((1, rows), jnp.float32),
            jax.ShapeDtypeStruct((1, 1), jnp.float32),
        ),
        in_specs=[smem, hbm, hbm, hbm],
        out_specs=(pl.BlockSpec(memory_space=pl.ANY), vmem, smem),
        scratch_shapes=[
            pltpu.VMEM((layers, groups, shards, per, fan, depth, side), tiles.dtype),
            pltpu.VMEM(biases.shape, biases.dtype),
            blocks,
            blocks,
            blocks,
            pltpu.VMEM((shards, per, rows, side), features.dtype),
            pltpu.VMEM((shards, rows, per * side), features.dtype),
            pltpu.VMEM((shards - KEPT, rows, per * side), features.dtype),
            sums,
            sums,
            pltpu.VMEM((8, rows), jnp.float32),
            pltpu.VMEM((total, 8, rows), jnp.float32),
            dma((2 + layers,)),
            dma(()),
            dma((layers, shards)),
            dma((2,)),
            dma((nl + 1,)),
            dma((nl + 1,)),
            dma((nl,)),
            dma((nl, every)),
            dma((every,)),
            dma((every,)),
            dma((2,)),
            dma((2,)),
            dma(()),
            dma((chunks,)),
            dma((2,)),
            dma(()),
            dma((2,)),
        ],
        compiler_params=pltpu.CompilerParams(
            collective_id=3,
            has_side_effects=True,
            vmem_limit_bytes=54 * 1024 * 1024,
        ),
        name="net",
    )(in_block.transpose(2, 0, 1), features, tiles, biases)
    return acts, row_means[0], grand[0, 0]


def suits(geo, shards, groups, features, tiles, biases):
    nl, nq, _, nc = geo
    kept = 6 * features.size + groups * tiles.size
    return (
        nq == 2
        and nl == 4
        and nc <= 2
        and shards == 2 * nc
        and groups >= 2 * shards
        and tiles.shape[0] == 2
        and tiles.shape[3] % 16 == 0
        and tiles.shape[1] // shards % PIECES == 0
        and 2 * kept < 54 * 1024 * 1024
    )


def on_device(geo, features, tiles, biases, in_block):
    shards = lax.axis_size("mp")
    groups = lax.axis_size("batch")
    me = lax.axis_index("mp")
    rows = features.shape[0]
    side = tiles.shape[4]
    cb = tiles.shape[1]
    fan = tiles.shape[2]
    if suits(geo, shards, groups, features, tiles, biases):
        return fused(geo, PIECES, features, tiles, biases, in_block)
    current = features
    mine = lax.dynamic_slice_in_dim(in_block, me * cb, cb, axis=1) % cb
    for layer in range(tiles.shape[0]):
        wall, xall = gather(geo, shards, groups, layer, tiles, current)
        current, sums = apply_layer(
            mine[layer].reshape(-1), xall, wall, biases[layer].reshape(1, -1)
        )
    row_means, whole = means(groups, shards, cb * side * shards, sums)
    grand = jnp.sum(whole) / (rows * groups)
    return (current, row_means, grand)


def solution(mesh):
    placed = (P("batch", "mp"), P(None, "mp", None, "batch", None), P(None, "mp"), P())
    return jax.shard_map(
        functools.partial(on_device, geometry(mesh)),
        mesh=mesh,
        in_specs=placed,
        out_specs=(P("batch", "mp"), P("batch"), P()),
        check_vma=False,
    )
```

```python
import functools
import math

import jax
import jax.numpy as jnp
from jax import lax
from jax.experimental import pallas as pl
from jax.experimental.pallas import tpu as pltpu
from jax.sharding import PartitionSpec as P

MESH = pl.DeviceIdType.MESH
PIECES = 4
KEPT = 2
FIRST = 3
LAG = 2
LATER = 0
SLACK = 2


def geometry(mesh):
    groups, shards = mesh.devices.shape
    where = [getattr(d, "coords", None) for d in mesh.devices[:, 0]]
    if groups == 1 or where[0] is None or where[0] == where[1]:
        return groups, 1, True, 1
    moved = [i for i in range(len(where[0])) if where[0][i] != where[1][i]][0]
    minor = 1
    while minor < groups and all(
        where[minor][i] == where[0][i] for i in range(len(where[0])) if i != moved
    ):
        minor += 1
    major = groups // minor
    row = [d.coords for d in mesh.devices[0, :]]
    cores = sum(1 for c in row if c == row[0])
    if major >= minor:
        return major, minor, True, cores
    return minor, major, False, cores


def gather_kernel(
    geo, shards, layer, pieces,
    tiles, cur, wout, xout,
    wv, xv, lsem, wrecv, wup, wdn, wcross, whalf, xrecv, xfar, xcore,
):
    nl, nq, line_major, nc = geo
    ny = shards // nc
    bi = lax.axis_index("batch")
    mi = lax.axis_index("mp")
    if line_major:
        l, q = bi // nq, bi % nq
    else:
        l, q = bi % nl, bi // nl
    y, core = mi // nc, mi % nc
    step_w = tiles.shape[1] // pieces
    step_x = cur.shape[0] // pieces
    halves = nq == 2 and nl % 2 == 0
    first = pieces // 2

    def group(level, side):
        return level * nq + side if line_major else side * nl + level

    sides = [(q + d) % nq for d in range(1, nq)]
    fars = [((y + d) % ny) * nc + core for d in range(1, ny)]
    partners = [y * nc + (core + d) % nc for d in range(1, nc)]

    barrier = pltpu.get_barrier_semaphore()

    def greet(b, m):
        pl.semaphore_signal(barrier, inc=1, device_id=(b, m), device_id_type=MESH)

    @pl.when(l > 0)
    def _():
        greet(group(l - 1, q), mi)

    @pl.when(l < nl - 1)
    def _():
        greet(group(l + 1, q), mi)

    for side in sides:
        greet(group(l, side), mi)
    for m in fars + partners:
        greet(bi, m)
    near = jnp.where(l > 0, 1, 0) + jnp.where(l < nl - 1, 1, 0)
    pl.semaphore_wait(barrier, len(sides) + len(fars) + len(partners) + near)

    in_w = pltpu.make_async_copy(tiles.at[layer], wv, lsem.at[0])
    in_x = pltpu.make_async_copy(cur, xv, lsem.at[1])
    in_w.start()
    in_x.start()

    def wcopy(own, b, c, to, ssem):
        part = pl.ds(c * step_w, step_w)
        return pltpu.make_async_remote_copy(
            src_ref=tiles.at[layer, part] if own else wout.at[b, part],
            dst_ref=wout.at[b, part],
            send_sem=ssem,
            recv_sem=wrecv.at[b, c],
            device_id=(to, mi),
            device_id_type=MESH,
        )

    def xcopy(own, m, c, to, ssem):
        part = pl.ds(c * step_x, step_x)
        return pltpu.make_async_remote_copy(
            src_ref=cur.at[part] if own else xout.at[m, part],
            dst_ref=xout.at[m, part],
            send_sem=ssem,
            recv_sem=xrecv.at[m, c],
            device_id=(bi, to),
            device_id_type=MESH,
        )

    def phase(p, c, drain):
        def go(copy):
            copy.wait_send() if drain else copy.start()

        def arrived_w(b):
            if not drain:
                wcopy(False, b, c, bi, wup.at[0, c]).wait_recv()

        if p == 0:
            @pl.when(l < nl - 1)
            def _():
                go(wcopy(True, bi, c, group(l + 1, q), wup.at[0, c]))

            @pl.when(l > 0)
            def _():
                go(wcopy(True, bi, c, group(l - 1, q), wdn.at[0, c]))

            for i, side in enumerate(sides):
                go(wcopy(True, bi, c, group(l, side), wcross.at[i, l, c]))
            for i, m in enumerate(fars):
                go(xcopy(True, mi, c, m, xfar.at[i, c]))
            for i, m in enumerate(partners):
                go(xcopy(True, mi, c, m, xcore.at[i, y, c]))
        else:
            @pl.when(l - p >= 0)
            def _():
                b = group(l - p, q)
                arrived_w(b)

                @pl.when(l < nl - 1)
                def _():
                    go(wcopy(False, b, c, group(l + 1, q), wup.at[p, c]))

                def across():
                    for i, side in enumerate(sides):
                        go(wcopy(False, b, c, group(l, side), wcross.at[i, l - p, c]))

                if halves and p == 1:
                    pl.when((l < nl // 2) | (c < first))(across)
                else:
                    across()

            @pl.when(l + p <= nl - 1)
            def _():
                b = group(l + p, q)
                arrived_w(b)

                @pl.when(l > 0)
                def _():
                    go(wcopy(False, b, c, group(l - 1, q), wdn.at[p, c]))

                def across():
                    for i, side in enumerate(sides):
                        go(wcopy(False, b, c, group(l, side), wcross.at[i, l + p, c]))

                if halves and p == 1:
                    pl.when((l >= nl // 2) | (c < first))(across)
                else:
                    across()

            if halves and p == 1:
                @pl.when(c >= first)
                def _():
                    b = group(l, sides[0])
                    arrived_w(b)

                    @pl.when((l + 1 >= nl // 2) & (l < nl - 1))
                    def _():
                        go(wcopy(False, b, c, group(l + 1, q), whalf.at[0, c]))

                    @pl.when((l - 1 < nl // 2) & (l > 0))
                    def _():
                        go(wcopy(False, b, c, group(l - 1, q), whalf.at[1, c]))

        if p == nl - 1:
            for d, far in enumerate(fars):
                if not drain:
                    xcopy(False, far, c, mi, xfar.at[0, c]).wait_recv()
                for i, m in enumerate(partners):
                    go(xcopy(False, far, c, m, xcore.at[i, far // nc, c]))

    for p in range(nl):
        @pl.loop(0, pieces)
        def _(c, p=p):
            phase(p, c, False)

        if p == 0:
            in_w.wait()
            in_x.wait()
            out_w = pltpu.make_async_copy(wv, wout.at[bi], lsem.at[2])
            out_x = pltpu.make_async_copy(xv, xout.at[mi], lsem.at[3])
            out_w.start()
            out_x.start()

    @pl.loop(0, pieces)
    def _(c):
        for side in sides:
            for level in range(nl):
                b = group(level, side)

                def arrive(b=b):
                    wcopy(False, b, c, bi, wup.at[0, c]).wait_recv()

                if halves:
                    pl.when((l != level) | (c < first))(arrive)
                else:
                    arrive()
        for m in partners:
            for yy in range(ny):
                xcopy(False, yy * nc + m % nc, c, mi, xfar.at[0, c]).wait_recv()

    out_w.wait()
    out_x.wait()
    for p in range(nl):
        @pl.loop(0, pieces)
        def _(c, p=p):
            phase(p, c, True)


def gather(geo, shards, groups, layer, tiles, cur):
    nl, nq, _, nc = geo
    pieces = 8 if groups <= 8 else 2
    ny = shards // nc
    dma = pltpu.SemaphoreType.DMA
    return pl.pallas_call(
        functools.partial(gather_kernel, geo, shards, layer, pieces),
        out_shape=(
            jax.ShapeDtypeStruct((groups,) + tiles.shape[1:], tiles.dtype),
            jax.ShapeDtypeStruct((shards,) + cur.shape, cur.dtype),
        ),
        in_specs=[pl.BlockSpec(memory_space=pl.ANY)] * 2,
        out_specs=(pl.BlockSpec(memory_space=pl.ANY),) * 2,
        scratch_shapes=[
            pltpu.VMEM(tiles.shape[1:], tiles.dtype),
            pltpu.VMEM(cur.shape, cur.dtype),
            dma((4,)),
            dma((groups, pieces)),
            dma((nl, pieces)),
            dma((nl, pieces)),
            dma((max(nq - 1, 1), nl, pieces)),
            dma((2, pieces)),
            dma((shards, pieces)),
            dma((max(ny - 1, 1), pieces)),
            dma((max(nc - 1, 1), ny, pieces)),
        ],
        compiler_params=pltpu.CompilerParams(collective_id=layer, has_side_effects=True),
        name=f"gather_{layer}",
    )(tiles, cur)


def layer_kernel(ids, x_ref, w_ref, b_ref, o_ref, r_ref, xl, wl, s_ref, loads):
    shards, rows, _ = x_ref.shape
    _, cb, fan, _, side = w_ref.shape
    per_shard = cb // shards
    width = math.gcd(per_shard, 8)

    def pulls(s):
        part = pl.ds(s * per_shard, per_shard)
        return (
            pltpu.make_async_copy(x_ref.at[s], xl.at[s], loads.at[0, s]),
            pltpu.make_async_copy(w_ref.at[:, part], wl.at[:, part], loads.at[1, s]),
        )

    for s in range(min(2, shards)):
        for pull in pulls(s):
            pull.start()
    s_ref[...] = jnp.zeros_like(s_ref)
    for s in range(shards):
        for pull in pulls(s):
            pull.wait()
        if s + 2 < shards:
            for pull in pulls(s + 2):
                pull.start()

        @pl.loop(0, per_shard // width)
        def _(k, s=s):
            for jj in range(width):
                j = s * per_shard + k * width + jj
                xs, ws = [], []
                for t in range(fan):
                    at = ids[j * fan + t]
                    xs.append(xl[s, :, pl.ds(pl.multiple_of(at * side, side), side)])
                    ws.append(wl[:, j, t].reshape(side, side))
                total = jnp.dot(
                    jnp.concatenate(xs, axis=1),
                    jnp.concatenate(ws, axis=0),
                    preferred_element_type=jnp.float32,
                )
                cols = pl.ds(pl.multiple_of(j * side, side), side)
                out = jnp.clip(total + b_ref[:, cols], 0.0, 32.0).astype(o_ref.dtype)
                o_ref[:, cols] = out
                s_ref[...] += out.astype(jnp.float32)

    line = jnp.sum(s_ref[...].T, axis=0, keepdims=True)
    r_ref[...] = jnp.broadcast_to(line, r_ref.shape)


def apply_layer(ids, xall, wall, bias):
    shards, rows, width = xall.shape
    side = wall.shape[4]
    hbm = pl.BlockSpec(memory_space=pl.ANY)
    vmem = pl.BlockSpec(memory_space=pltpu.VMEM)
    return pl.pallas_call(
        layer_kernel,
        out_shape=(
            jax.ShapeDtypeStruct((rows, width), xall.dtype),
            jax.ShapeDtypeStruct((8, rows), jnp.float32),
        ),
        in_specs=[pl.BlockSpec(memory_space=pltpu.SMEM), hbm, hbm, vmem],
        out_specs=(vmem, vmem),
        scratch_shapes=[
            pltpu.VMEM(xall.shape, xall.dtype),
            pltpu.VMEM(wall.shape, wall.dtype),
            pltpu.VMEM((rows, side), jnp.float32),
            pltpu.SemaphoreType.DMA((2, shards)),
        ],
        compiler_params=pltpu.CompilerParams(vmem_limit_bytes=52 * 1024 * 1024),
        name="layer",
    )(ids, xall, wall, bias)


def means_kernel(groups, shards, neurons, x_ref, rows_ref, all_ref, slots, ssem, rsem):
    bi = lax.axis_index("batch")
    mi = lax.axis_index("mp")
    me = bi * shards + mi
    total = groups * shards
    barrier = pltpu.get_barrier_semaphore()

    def peer(d):
        to = (me + d) % total
        return to // shards, to % shards

    @pl.loop(1, total)
    def _(d):
        pl.semaphore_signal(barrier, inc=1, device_id=peer(d), device_id_type=MESH)

    pl.semaphore_wait(barrier, total - 1)

    def copy(d, slot):
        return pltpu.make_async_remote_copy(
            src_ref=x_ref,
            dst_ref=slots.at[slot],
            send_sem=ssem.at[d],
            recv_sem=rsem.at[slot],
            device_id=peer(d),
            device_id_type=MESH,
        )

    @pl.loop(1, total)
    def _(d):
        copy(d, me).start()

    slots[me] = x_ref[...]

    @pl.loop(1, total)
    def _(d):
        copy(d, (me + d) % total).wait_recv()

    whole = jnp.zeros(all_ref.shape, jnp.float32)
    for b in range(groups):
        one = slots[b * shards]
        for m in range(1, shards):
            one = one + slots[b * shards + m]
        whole = whole + one / neurons
    all_ref[...] = whole
    mine = slots[bi * shards]
    for m in range(1, shards):
        mine = mine + slots[bi * shards + m]
    rows_ref[...] = mine / neurons

    @pl.loop(1, total)
    def _(d):
        copy(d, me).wait_send()


def means(groups, shards, neurons, sums):
    total = groups * shards
    if total > 64:
        shard_sum = lax.psum(sums[0], "mp") / neurons
        return shard_sum, lax.psum(shard_sum, "batch")
    vmem = pl.BlockSpec(memory_space=pltpu.VMEM)
    like = jax.ShapeDtypeStruct(sums.shape, jnp.float32)
    mine, whole = pl.pallas_call(
        functools.partial(means_kernel, groups, shards, neurons),
        out_shape=(like, like),
        in_specs=[vmem],
        out_specs=(vmem, vmem),
        scratch_shapes=[
            pltpu.VMEM((total,) + sums.shape, jnp.float32),
            pltpu.SemaphoreType.DMA((total,)),
            pltpu.SemaphoreType.DMA((total,)),
        ],
        compiler_params=pltpu.CompilerParams(collective_id=20, has_side_effects=True),
        name="means",
    )(sums)
    return mine[0], whole[0]


def fused_kernel(
    geo, pieces, neurons, total_rows,
    ids, feats, tiles, biases, out, rows_ref, grand_ref,
    wl, bl, xin, x2, x2g, st, fin, fing, sums, guests, line, slots,
    lsem, qsend, qrecv, bsem, up, dn, xs, wrecv, xrecv, rrecv,
    osend, okept, orecv, x2recv, fsem, gsend, msem,
):
    nl, nq, line_major, nc = geo
    layers, groups, shards, per, fan, _, side = wl.shape
    ny = shards // nc
    cb = per * shards
    n = per // pieces
    chunks = shards * pieces
    every = layers * chunks
    depth = nl
    edge_own = KEPT * pieces
    bi = lax.axis_index("batch")
    mi = lax.axis_index("mp")
    if line_major:
        l, q = bi // nq, bi % nq
    else:
        l, q = bi % nl, bi // nl
    y, core = mi // nc, mi % nc
    side_q = (q + 1) % nq
    total = groups * shards
    me = bi * shards + mi
    edge = (l == 0) | (l == nl - 1)
    host = (l == 1) | (l == nl - 2)
    low = l < nl // 2

    def group(level, column):
        return level * nq + column if line_major else column * nl + level

    upper = group(jnp.minimum(l + 1, nl - 1), q)
    under = group(jnp.maximum(l - 1, 0), q)
    beside = group(l, side_q)
    hosted = group(jnp.where(low, 0, nl - 1), q)
    hosting = group(jnp.where(low, 1, nl - 2), q)

    def source(k):
        return ((y + k // nc) % ny) * nc + (core + k % nc) % nc

    def turn(layer, c):
        k = c // pieces
        return (shards - k) % shards if layer == 0 else shards - 1 - k

    def place(p):
        r = p - chunks
        v = r - FIRST
        mixed = jnp.where(v % 2 == 1, FIRST + v // 2, edge_own + v // 2)
        later = jnp.where(v < 2 * (edge_own - FIRST), mixed, r)
        second = jnp.where(r < FIRST, r, later)
        return jnp.where(r >= 0, 1, 0), jnp.where(r >= 0, second, p)

    def spot(p):
        layer, c = place(p)
        return layer, jnp.where(layer == 0, turn(0, c), turn(1, c)), c % pieces

    def peer(d):
        to = (me + d) % total
        return to // shards, to % shards

    def remote(src, dst, ssem, rsem, b, m):
        return pltpu.make_async_remote_copy(
            src_ref=src, dst_ref=dst, send_sem=ssem, recv_sem=rsem,
            device_id=(b, m), device_id_type=MESH,
        )

    def came(part, rsem):
        remote(part, part, msem.at[0], rsem, bi, mi).wait_recv()

    def left(part, ssem):
        remote(part, part, ssem, msem.at[1], bi, mi).wait_send()

    def own_quarter(layer):
        return pltpu.make_async_copy(
            tiles.at[layer, pl.ds(mi * per, per)], wl.at[layer, bi, mi], lsem.at[2 + layer]
        )

    for layer in range(layers):
        own_quarter(layer).start()
    mine_b = pl.ds(mi * per * side, per * side)
    in_b = pltpu.make_async_copy(biases.at[:, mine_b], bl.at[:, mine_b], lsem.at[1])
    in_b.start()

    barrier = pltpu.get_barrier_semaphore()

    def greet(b, m):
        pl.semaphore_signal(barrier, inc=1, device_id=(b, m), device_id_type=MESH)

    @pl.when(l > 0)
    def _():
        greet(under, mi)

    @pl.when(l < nl - 1)
    def _():
        greet(upper, mi)

    greet(beside, mi)
    for k in range(1, shards):
        greet(bi, source(k))

    @pl.loop(0, cb)
    def _(j):
        pltpu.make_async_copy(
            feats.at[:, pl.ds(j * side, side)], xin.at[j], lsem.at[0]
        ).start()

    near = jnp.where(l > 0, 1, 0) + jnp.where(l < nl - 1, 1, 0)
    pl.semaphore_wait(barrier, near + shards)

    def quarter(layer, k):
        to = source(k)
        return remote(
            tiles.at[layer, pl.ds(to * per, per)], wl.at[layer, bi, mi],
            qsend, qrecv.at[layer, mi], bi, to,
        )

    for k in range(1, shards):
        to = source(k)
        quarter(0, k).start()
        theirs = biases.at[:, pl.ds(to * per * side, per * side)]
        remote(theirs, bl.at[:, mine_b], bsem.at[0], bsem.at[1], bi, to).start()
    for layer in range(1, layers):
        for k in range(1, shards):
            quarter(layer, k).start()
    sums[...] = jnp.zeros_like(sums)
    guests[...] = jnp.zeros_like(guests)

    def piece(p, b):
        layer, k, g = spot(p)
        return wl.at[layer, b, source(k), pl.ds(g * n, n)]

    def inside(p):
        layer, c = place(p)
        return (layer == 1) & (c >= edge_own)

    def top(p):
        return jnp.where(inside(p), nl - 2, nl - 1)

    def bottom(p):
        return jnp.where(inside(p), 1, 0)

    def relayed(p, level):
        outer = (level == 0) | (level == nl - 1)
        return jnp.where(outer, p >= chunks, place(p)[1] % 2 == 1)

    def carried(p, level, to):
        outer = (to == 0) | (to == nl - 1)
        across = (abs(level - to) == 1) & relayed(p, level)
        return across & jnp.logical_not(outer & (p >= chunks))

    def go(cond, copy):
        @pl.when(cond)
        def _():
            copy.start()

    def along(p, b, level, e):
        part = piece(p, b)
        go(l < top(p), remote(part, part, up.at[e], wrecv.at[level, p], upper, mi))
        go(l > bottom(p), remote(part, part, dn.at[e], wrecv.at[level, p], under, mi))

    def due(t, d):
        one, two = t - d, t - d - SLACK
        ok = ((one >= 0) & (one < chunks)) | ((two >= chunks) & (two < every))
        return jnp.where(one < chunks, one, two), ok

    def flow(t):
        def quarter_here(p):
            layer, k, g = spot(p)

            @pl.when((g == 0) & (k == 0))
            def _():
                own_quarter(layer).wait()

            @pl.when((g == 0) & (k > 0))
            def _():
                m = source(k)
                came(wl.at[layer, bi, m], qrecv.at[layer, m])

        def own(p, cond):
            part = piece(p, bi)
            go(cond & (l < top(p)), remote(part, part, up.at[0], wrecv.at[l, p], upper, mi))
            go(cond & (l > bottom(p)), remote(part, part, dn.at[0], wrecv.at[l, p], under, mi))

        hurried = pieces + 2 * (t - pieces)

        @pl.when((t < pieces) | ((t >= chunks) & (t < every)))
        def _():
            quarter_here(t)
            own(t, True)

        @pl.when((t >= pieces) & (hurried < chunks))
        def _():
            quarter_here(hurried)
            own(hurried, edge)
            own(hurried + 1, edge)

        @pl.when((t >= pieces) & (t < chunks))
        def _():
            own(t, jnp.logical_not(edge))

        @pl.when(t < every)
        def _():
            part = piece(t, bi)
            again = relayed(t, l)
            go(again, remote(part, part, xs.at[l], rrecv.at[t], beside, mi))
            go(jnp.logical_not(again), remote(part, part, xs.at[l], xrecv.at[t], beside, mi))

    def steps(t):
        for d in range(1, nl):
            p, ok = due(t, d)

            def step(p, level, onward, ssem, to):
                part = piece(p, group(level, q))
                came(part, wrecv.at[level, p])
                go(onward, remote(part, part, ssem, wrecv.at[level, p], to, mi))
                direct = jnp.logical_not(carried(p, level, l))
                go(direct, remote(part, part, xs.at[level], xrecv.at[p], beside, mi))

            @pl.when(ok & (l - d >= 0) & (l <= top(p)))
            def _(d=d, p=p, step=step):
                step(p, jnp.maximum(l - d, 0), l < top(p), up.at[d], upper)

            @pl.when(ok & (l + d <= nl - 1) & (l >= bottom(p)))
            def _(d=d, p=p, step=step):
                step(p, jnp.minimum(l + d, nl - 1), l > bottom(p), dn.at[d], under)

            if d == 1:
                @pl.when(ok & relayed(p, l))
                def _(p=p):
                    part = piece(p, beside)
                    came(part, rrecv.at[p])
                    more = (l < top(p)) & carried(p, l, l + 1)
                    go(more, remote(part, part, up.at[nl], xrecv.at[p], upper, mi))
                    more = (l > bottom(p)) & carried(p, l, l - 1)
                    go(more, remote(part, part, dn.at[nl], xrecv.at[p], under, mi))

    def landing(p):
        layer, k, g = spot(p)
        early = relayed(p, l)

        def wait(count):
            came(wl.at[layer, pl.ds(0, count), source(k), pl.ds(g * n, n)], xrecv.at[p])

        @pl.when(early)
        def _():
            wait(nl - 1)

        @pl.when(jnp.logical_not(early))
        def _():
            wait(nl)

    def columns(m, g):
        return pl.ds((m * per + g * n) * side, n * side)

    def blocks(m, g):
        return pl.ds(m * per + g * n, n)

    def hand_on(p):
        layer, c = place(p)
        g = c % pieces

        @pl.when(layer == 0)
        def _():
            k = turn(0, c)
            part = pl.ds(g * n, n)

            @pl.when(k == 0)
            def _():
                pltpu.make_async_copy(
                    st.at[0, part], x2.at[blocks(mi, g)], okept.at[0]
                ).start()

            @pl.when(k > 0)
            def _():
                remote(
                    st.at[k, part], x2.at[blocks(mi, g)],
                    osend.at[0], x2recv.at[c], bi, source(k),
                ).start()

        @pl.when((layer == 1) & jnp.logical_not(edge & inside(p)))
        def _():
            k = turn(1, c)
            part = pl.ds(g * n * side, n * side)

            @pl.when(k == 0)
            def _():
                pltpu.make_async_copy(
                    fin.at[0, :, part], out.at[:, columns(mi, g)], okept.at[1]
                ).start()

            @pl.when(k > 0)
            def _():
                remote(
                    fin.at[k, :, part], out.at[:, columns(mi, g)],
                    osend.at[1], orecv, bi, source(k),
                ).start()

    def give_back(p):
        _, c = place(p)
        k, g = turn(1, c), c % pieces
        remote(
            fing.at[k, :, pl.ds(g * n * side, n * side)], out.at[:, columns(mi, g)],
            gsend, orecv, hosted, source(k),
        ).start()

    def pass_on(c):
        k, g = turn(0, c), c % pieces
        m = source(k)

        @pl.when(k == 0)
        def _():
            part = st.at[0, pl.ds(g * n, n)]
            go(edge, remote(part, x2g.at[blocks(mi, g)], fsem.at[0], fsem.at[1], hosting, mi))

        @pl.when(k > 0)
        def _():
            part = x2.at[blocks(m, g)]
            came(part, x2recv.at[c])
            go(edge, remote(part, x2g.at[blocks(m, g)], fsem.at[0], fsem.at[1], hosting, mi))

    def compute(layer, c, guest=False):
        k, g = turn(layer, c), c % pieces
        m = source(k)
        src = xin if layer == 0 else x2g if guest else x2
        for jj in range(n):
            j = g * n + jj
            column = m * cb + mi * per + j
            xparts, wparts = [], []
            for t in range(fan):
                at = lax.rem(ids[t, layer, column], cb)
                xparts.append(src[at])
                wparts.append(wl[layer, :, m, j, t].reshape(side, side))
            whole = jnp.dot(
                jnp.concatenate(xparts, axis=1),
                jnp.concatenate(wparts, axis=0),
                preferred_element_type=jnp.float32,
            )
            bias = bl[layer : layer + 1, pl.ds(pl.multiple_of((m * per + j) * side, side), side)]
            res = jnp.clip(whole + bias, 0.0, 32.0).astype(out.dtype)
            cols = pl.ds(pl.multiple_of(j * side, side), side)
            if layer == 0:
                st[k, j] = res
            elif guest:
                fing[k, :, cols] = res
                guests[...] += res.astype(jnp.float32)
            else:
                fin[k, :, cols] = res
                sums[...] += res.astype(jnp.float32)

    @pl.loop(0, every + depth + SLACK + LATER + 1)
    def _(t):
        flow(t)
        p = t - depth
        r = p - SLACK
        h = r - LATER

        @pl.when((p >= 1) & (p <= chunks))
        def _():
            hand_on(p - 1)

        @pl.when((r > chunks) & (r <= every))
        def _():
            hand_on(r - 1)

        @pl.when(host & (h > chunks))
        def _():
            pl.when(inside(h - 1))(lambda: give_back(h - 1))

        @pl.when((p >= LAG) & (p - LAG < chunks))
        def _():
            pass_on(p - LAG)

        steps(t)

        @pl.when(p == 0)
        def _():
            pltpu.make_async_copy(xin, xin, lsem.at[0]).wait()
            in_b.wait()
            came(bl.at[:, pl.ds(0, (shards - 1) * per * side)], bsem.at[1])

        @pl.when((p >= 0) & (p < chunks))
        def _():
            landing(p)
            compute(0, p)

        @pl.when(r == chunks)
        def _():
            pltpu.make_async_copy(st.at[0], st.at[0], okept.at[0]).wait()

        needed = (r >= chunks) & (r < every) & jnp.logical_not(edge & inside(r))

        @pl.when(needed)
        def _():
            landing(r)

        @pl.when(host & (h == chunks + FIRST))
        def _():
            came(x2g, fsem.at[1])

        @pl.when(host & (h >= chunks) & (h < every))
        def _():
            pl.when(inside(h))(lambda: compute(1, place(h)[1], True))

        @pl.when(needed)
        def _():
            compute(1, place(r)[1])

    own_line = jnp.sum(sums[...].T, axis=0, keepdims=True)
    guest_line = jnp.sum(guests[...].T, axis=0, keepdims=True)
    at_row = lax.broadcasted_iota(jnp.int32, line.shape, 0)
    line[...] = jnp.where(at_row < line.shape[0] // 2, own_line, guest_line)

    def gone(halves, ssem):
        if halves % 2 == 0:
            left(wl.at[0, pl.ds(0, halves // 2), 0], ssem)
        else:
            left(wl.at[0, pl.ds(0, halves), 0, pl.ds(0, per // 2)], ssem)

    wide, narrow = 2 * (shards + KEPT), 2 * (shards - KEPT)
    full = wide + narrow
    for d in range(nl):
        @pl.when((l - d >= 0) & (l < nl - 2))
        def _(d=d):
            gone(full, up.at[d])

        @pl.when((l - d >= 0) & (l == nl - 2))
        def _(d=d):
            gone(wide, up.at[d])

        @pl.when((l + d <= nl - 1) & (l > 1))
        def _(d=d):
            gone(full, dn.at[d])

        @pl.when((l + d <= nl - 1) & (l == 1))
        def _(d=d):
            gone(wide, dn.at[d])

    @pl.when(l == 0)
    def _():
        gone(full // 2, up.at[nl])

    @pl.when((l > 0) & (l < nl - 2))
    def _():
        gone(full // 2, up.at[nl])

    @pl.when(l == nl - 2)
    def _():
        gone(shards, up.at[nl])

    @pl.when(l == nl - 1)
    def _():
        gone(full // 2, dn.at[nl])

    @pl.when((l > 1) & (l < nl - 1))
    def _():
        gone(full // 2, dn.at[nl])

    @pl.when(l == 1)
    def _():
        gone(shards, dn.at[nl])

    for level in range(nl):
        close = abs(l - level) == 1
        outer = level in (0, nl - 1)

        @pl.when(l == level)
        def _(level=level):
            gone(full, xs.at[level])

        @pl.when(edge & (l != level))
        def _(level=level, close=close):
            @pl.when(close)
            def _():
                gone(wide - shards, xs.at[level])

            @pl.when(jnp.logical_not(close))
            def _():
                gone(wide, xs.at[level])

        @pl.when(jnp.logical_not(edge) & (l != level))
        def _(level=level, close=close, outer=outer):
            @pl.when(close)
            def _():
                gone(full // 2, xs.at[level])

            @pl.when(jnp.logical_not(close))
            def _():
                gone(full, xs.at[level])

    left(wl.at[:, bi, pl.ds(0, shards - 1)], qsend)
    left(bl.at[:, pl.ds(0, (shards - 1) * per * side)], bsem.at[0])
    left(st.at[pl.ds(0, shards - 1)], osend.at[0])

    @pl.when(edge)
    def _():
        left(x2g, fsem.at[0])

    def mcopy(d, slot):
        return remote(line, slots.at[slot], msem.at[0], msem.at[1], *peer(d))

    @pl.loop(1, total)
    def _(d):
        mcopy(d, me).start()

    slots[me] = line[...]

    @pl.when(edge)
    def _():
        left(fin.at[pl.ds(0, KEPT)], osend.at[1])

    @pl.when(jnp.logical_not(edge))
    def _():
        left(fin.at[pl.ds(0, shards - 1)], osend.at[1])

    @pl.when(host)
    def _():
        left(fing, gsend)

    lines = slots.at[pl.ds(0, total - 1)]
    came(lines, msem.at[1])
    low_half = line.shape[0] // 2
    whole = jnp.zeros((1, line.shape[1]), jnp.float32)
    for b in range(groups):
        one = slots[b * shards]
        for m in range(1, shards):
            one = one + slots[b * shards + m]
        whole = whole + (one[0:1] + one[low_half : low_half + 1]) / neurons
    mine = slots[bi * shards]
    help_ = slots[hosting * shards]
    for m in range(1, shards):
        mine = mine + slots[bi * shards + m]
        help_ = help_ + slots[hosting * shards + m]
    extra = jnp.where(edge, help_[low_half : low_half + 1], 0.0)
    rows_ref[...] = (mine[0:1] + extra) / neurons
    grand_ref[0, 0] = jnp.sum(whole) / total_rows

    @pl.when(edge)
    def _():
        came(fin, orecv)

    @pl.when(jnp.logical_not(edge))
    def _():
        pltpu.make_async_copy(fin.at[0], fin.at[0], okept.at[1]).wait()
        came(fin.at[pl.ds(0, shards - 1)], orecv)

    left(lines, msem.at[0])


def fused(geo, pieces, features, tiles, biases, in_block):
    nl, nq, _, nc = geo
    shards = lax.axis_size("mp")
    groups = lax.axis_size("batch")
    layers, cb, fan, depth, side = tiles.shape
    rows, width = features.shape
    per = cb // shards
    chunks = shards * pieces
    every = layers * chunks
    total = groups * shards
    dma = pltpu.SemaphoreType.DMA
    hbm = pl.BlockSpec(memory_space=pltpu.HBM)
    vmem = pl.BlockSpec(memory_space=pltpu.VMEM)
    smem = pl.BlockSpec(memory_space=pltpu.SMEM)
    blocks = pltpu.VMEM((cb, rows, side), features.dtype)
    sums = pltpu.VMEM((rows, side), jnp.float32)
    kept = [
        pltpu.with_memory_space_constraint(x, pltpu.HBM)
        for x in (features, tiles, biases)
    ]
    acts, row_means, grand = pl.pallas_call(
        functools.partial(
            fused_kernel, geo, pieces, cb * side * shards, rows * groups
        ),
        out_shape=(
            jax.ShapeDtypeStruct((rows, width), features.dtype),
            jax.ShapeDtypeStruct((1, rows), jnp.float32),
            jax.ShapeDtypeStruct((1, 1), jnp.float32),
        ),
        in_specs=[smem, hbm, hbm, hbm],
        out_specs=(pl.BlockSpec(memory_space=pl.ANY), vmem, smem),
        scratch_shapes=[
            pltpu.VMEM((layers, groups, shards, per, fan, depth, side), tiles.dtype),
            pltpu.VMEM(biases.shape, biases.dtype),
            blocks,
            blocks,
            blocks,
            pltpu.VMEM((shards, per, rows, side), features.dtype),
            pltpu.VMEM((shards, rows, per * side), features.dtype),
            pltpu.VMEM((shards - KEPT, rows, per * side), features.dtype),
            sums,
            sums,
            pltpu.VMEM((8, rows), jnp.float32),
            pltpu.VMEM((total, 8, rows), jnp.float32),
            dma((2 + layers,)),
            dma(()),
            dma((layers, shards)),
            dma((2,)),
            dma((nl + 1,)),
            dma((nl + 1,)),
            dma((nl,)),
            dma((nl, every)),
            dma((every,)),
            dma((every,)),
            dma((2,)),
            dma((2,)),
            dma(()),
            dma((chunks,)),
            dma((2,)),
            dma(()),
            dma((2,)),
        ],
        compiler_params=pltpu.CompilerParams(
            collective_id=3,
            has_side_effects=True,
            vmem_limit_bytes=48 * 1024 * 1024,
        ),
        name="net",
    )(in_block.transpose(2, 0, 1), *kept)
    return acts, row_means[0], grand[0, 0]


def suits(geo, shards, groups, features, tiles, biases):
    nl, nq, _, nc = geo
    kept = 6 * features.size + groups * tiles.size
    return (
        nq == 2
        and nl == 4
        and nc <= 2
        and shards == 2 * nc
        and groups >= 2 * shards
        and tiles.shape[0] == 2
        and tiles.shape[3] % 16 == 0
        and tiles.shape[1] // shards % PIECES == 0
        and 2 * kept < 54 * 1024 * 1024
    )


def on_device(geo, features, tiles, biases, in_block):
    shards = lax.axis_size("mp")
    groups = lax.axis_size("batch")
    me = lax.axis_index("mp")
    rows = features.shape[0]
    side = tiles.shape[4]
    cb = tiles.shape[1]
    fan = tiles.shape[2]
    if suits(geo, shards, groups, features, tiles, biases):
        return fused(geo, PIECES, features, tiles, biases, in_block)
    current = features
    mine = lax.dynamic_slice_in_dim(in_block, me * cb, cb, axis=1) % cb
    for layer in range(tiles.shape[0]):
        wall, xall = gather(geo, shards, groups, layer, tiles, current)
        current, sums = apply_layer(
            mine[layer].reshape(-1), xall, wall, biases[layer].reshape(1, -1)
        )
    row_means, whole = means(groups, shards, cb * side * shards, sums)
    grand = jnp.sum(whole) / (rows * groups)
    return (current, row_means, grand)


def solution(mesh):
    placed = (P("batch", "mp"), P(None, "mp", None, "batch", None), P(None, "mp"), P())
    return jax.shard_map(
        functools.partial(on_device, geometry(mesh)),
        mesh=mesh,
        in_specs=placed,
        out_specs=(P("batch", "mp"), P("batch"), P()),
        check_vma=False,
    )
```
